32 devices in a mesh: pair: 2 (over x), tp: 4 (over z), side: 4 (over y, core).
Axes of the slice: x: 2, y: 2, z: 4, core: 2. Of those that a mesh axis runs over, the one named last changes fastest.
Arguments:
- x_prompt: bfloat16 [8, 2048, 4096], P(('pair', 'side')), parts along dimension 0
- s_len: int32 [8], P(('pair', 'side')), parts along dimension 0
- y_tok: bfloat16 [16, 4096], P(('pair', 'side')), parts along dimension 0
- c_len: int32 [16], P(('pair', 'side')), parts along dimension 0
- k_cache: bfloat16 [1, 16, 1024, 32, 128], P(None, ('pair', 'side'), 'tp'), parts along dimension 1
- v_cache: bfloat16 [1, 16, 1024, 32, 128], P(None, ('pair', 'side'), 'tp'), parts along dimension 1
- attn_gain: bfloat16 [1, 4096], replicated
- w_qkv: bfloat16 [1, 4096, 32, 3, 128], P(None, None, 'tp')
- w_out: bfloat16 [1, 32, 1, 128, 4096], P(None, 'tp')
- mlp_gain: bfloat16 [1, 4096], replicated
- w_gate_up: bfloat16 [1, 4096, 2, 11008], P(None, None, None, 'tp')
- w_down: bfloat16 [1, 11008, 4096], P(None, 'tp')
Outputs:
- output 1: bfloat16 [8, 2048, 4096], P(('pair', 'side')), parts along dimension 0
- output 2: bfloat16 [16, 4096], P(('pair', 'side')), parts along dimension 0
- output 3: bfloat16 [1, 8, 2048, 32, 128], P(None, ('pair', 'side'), 'tp'), parts along dimension 1
- output 4: bfloat16 [1, 8, 2048, 32, 128], P(None, ('pair', 'side'), 'tp'), parts along dimension 1
- output 5: bfloat16 [1, 16, 1024, 32, 128], P(None, ('pair', 'side'), 'tp'), parts along dimension 1
- output 6: bfloat16 [1, 16, 1024, 32, 128], P(None, ('pair', 'side'), 'tp'), parts along dimension 1
There are 2 independent parts. The reference program is written for one: setup_inputs(seed, part) draws one part's arguments, and reference() takes and returns one part's arrays. A program takes and returns all parts, laid end to end along the dimension named above; an argument that names none is the same for every part.
All inputs are finite; a program needn't handle non-finite values.
Results may differ from the reference program's by a relative error of at most 0.00695739.
Values are sent between devices in bfloat16 or wider.
A program may use at most 1 GiB of HBM per device.

```python
import jax
import jax.numpy as jnp
from jax import lax

D = 4096
HEADS = 32
KV_HEADS = 32
HEAD = 128
FF = 11008
PROMPT_LEN = 2048
BATCH_DEC = 2
CACHE_LEN = 1024
LAYERS = 1
GROUPS = 4
Q_BLOCK = 128
GROUP_Q = HEADS // KV_HEADS
ROPE_BASE = 10000.0
NORM_EPS = 1e-5


def setup_inputs(seed: int = 0, part: int = 0) -> dict:
    rng_key = jax.random.fold_in(jax.random.key(seed), part)
    key_list = jax.random.split(rng_key, 6)
    shared = jax.random.split(jax.random.key(seed + 1), 6)
    cache_shape = (LAYERS, GROUPS * BATCH_DEC, CACHE_LEN, KV_HEADS, HEAD)
    x_prompt = jax.random.normal(key_list[0], (GROUPS, PROMPT_LEN, D), jnp.float32).astype(jnp.bfloat16)
    s_len = jax.random.randint(key_list[1], (GROUPS,), PROMPT_LEN // 2, PROMPT_LEN + 1, jnp.int32)
    s_len = s_len.at[0].set(PROMPT_LEN)
    y_tok = jax.random.normal(key_list[2], (GROUPS * BATCH_DEC, D), jnp.float32).astype(jnp.bfloat16)
    c_len = jax.random.randint(key_list[3], (GROUPS, BATCH_DEC), CACHE_LEN // 2, CACHE_LEN, jnp.int32)
    c_len = c_len.at[:, 0].set(CACHE_LEN - 1).reshape(GROUPS * BATCH_DEC)
    k_cache = (1.5 * jax.random.normal(key_list[4], cache_shape, jnp.float32)).astype(jnp.bfloat16)
    v_cache = jax.random.normal(key_list[5], cache_shape, jnp.float32).astype(jnp.bfloat16)
    attn_gain = (1.0 + 0.3 * jax.random.normal(shared[0], (LAYERS, D), jnp.float32)).astype(jnp.bfloat16)
    w_qkv = (jax.random.normal(shared[1], (LAYERS, D, KV_HEADS, GROUP_Q + 2, HEAD), jnp.float32) * D ** -0.5).astype(jnp.bfloat16)
    w_out = (jax.random.normal(shared[2], (LAYERS, KV_HEADS, GROUP_Q, HEAD, D), jnp.float32) * (HEADS * HEAD) ** -0.5).astype(jnp.bfloat16)
    mlp_gain = (1.0 + 0.3 * jax.random.normal(shared[3], (LAYERS, D), jnp.float32)).astype(jnp.bfloat16)
    w_gate_up = (jax.random.normal(shared[4], (LAYERS, D, 2, FF), jnp.float32) * D ** -0.5).astype(jnp.bfloat16)
    w_down = (jax.random.normal(shared[5], (LAYERS, FF, D), jnp.float32) * FF ** -0.5).astype(jnp.bfloat16)
    return {'x_prompt': x_prompt, 's_len': s_len, 'y_tok': y_tok, 'c_len': c_len, 'k_cache': k_cache, 'v_cache': v_cache, 'attn_gain': attn_gain, 'w_qkv': w_qkv, 'w_out': w_out, 'mlp_gain': mlp_gain, 'w_gate_up': w_gate_up, 'w_down': w_down}


def rms_norm(hidden, norm_gain):
    hidden_f32 = hidden.astype(jnp.float32)
    inv_rms = lax.rsqrt(jnp.mean(hidden_f32 * hidden_f32, axis=-1, keepdims=True) + NORM_EPS)
    return (hidden_f32 * inv_rms * norm_gain.astype(jnp.float32)).astype(jnp.bfloat16)


def rope_rotate(vals_f32, positions):
    half_dim = HEAD // 2
    inv_freq = ROPE_BASE ** (-2.0 * jnp.arange(half_dim, dtype=jnp.float32) / HEAD)
    angles = positions.astype(jnp.float32)[:, None] * inv_freq[None, :]
    cos_table = jnp.cos(angles)[:, None, None, :]
    sin_table = jnp.sin(angles)[:, None, None, :]
    first_half = vals_f32[..., :half_dim]
    second_half = vals_f32[..., half_dim:]
    return jnp.concatenate([first_half * cos_table - second_half * sin_table, second_half * cos_table + first_half * sin_table], axis=-1)


def mlp_sum(hidden, norm_gain, w_gate_up, w_down):
    normed = rms_norm(hidden, norm_gain)
    gate_up = jnp.einsum('nd,dcf->ncf', normed.astype(jnp.float32), w_gate_up.astype(jnp.float32))
    activated = (jax.nn.silu(gate_up[:, 0]) * gate_up[:, 1]).astype(jnp.bfloat16)
    return jnp.dot(activated, w_down, preferred_element_type=jnp.float32)


def prefill_context(queries, key_rows, value_rows, key_valid):
    positions = jnp.arange(PROMPT_LEN)
    query_blocks = queries.reshape(PROMPT_LEN // Q_BLOCK, Q_BLOCK, KV_HEADS, GROUP_Q, HEAD)
    block_starts = jnp.arange(PROMPT_LEN // Q_BLOCK) * Q_BLOCK
    key_f32 = key_rows.astype(jnp.float32)
    value_f32 = value_rows.astype(jnp.float32)

    def attend_block(block_args):
        query_block, block_start = block_args
        scores = jnp.einsum('qkgh,tkh->kgqt', query_block.astype(jnp.float32), key_f32) * HEAD ** -0.5
        query_pos = block_start + jnp.arange(Q_BLOCK)
        allowed = (positions[None, :] <= query_pos[:, None]) & key_valid[None, :]
        scores = jnp.where(allowed, scores, -1e30)
        weights = jnp.exp(scores - jnp.max(scores, axis=-1, keepdims=True))
        weight_sum = jnp.sum(weights, axis=-1, keepdims=True)
        mixed_sum = jnp.einsum('kgqt,tkh->kgqh', weights.astype(jnp.bfloat16).astype(jnp.float32), value_f32)
        return jnp.transpose(mixed_sum / weight_sum, (2, 0, 1, 3)).astype(jnp.bfloat16)

    context = lax.map(attend_block, (query_blocks, block_starts))
    return context.reshape(PROMPT_LEN, KV_HEADS, GROUP_Q, HEAD)


def prefill_group(prompt_one, slen_one, weight_stack):
    positions = jnp.arange(PROMPT_LEN)
    key_valid = positions < slen_one
    keep_mask = key_valid[:, None, None].astype(jnp.bfloat16)

    def layer_step(hidden, layer_weights):
        gain_attn, w_qkv, w_out, gain_mlp, w_gate_up, w_down = layer_weights
        normed = rms_norm(hidden, gain_attn)
        projected = jnp.einsum('sd,dkjh->skjh', normed.astype(jnp.float32), w_qkv.astype(jnp.float32))
        rotated = rope_rotate(projected[:, :, :GROUP_Q + 1], positions).astype(jnp.bfloat16)
        value_rows = projected[:, :, GROUP_Q + 1].astype(jnp.bfloat16)
        key_rows = rotated[:, :, GROUP_Q]
        context = prefill_context(rotated[:, :, :GROUP_Q], key_rows, value_rows, key_valid)
        attn_sum = jnp.einsum('skgh,kghd->sd', context.astype(jnp.float32), w_out.astype(jnp.float32))
        hidden = (hidden.astype(jnp.float32) + attn_sum).astype(jnp.bfloat16)
        down_sum = mlp_sum(hidden, gain_mlp, w_gate_up, w_down)
        hidden = (hidden.astype(jnp.float32) + down_sum).astype(jnp.bfloat16)
        return hidden, (key_rows * keep_mask, value_rows * keep_mask)

    hidden, (key_all, value_all) = lax.scan(layer_step, prompt_one, weight_stack)
    return hidden, key_all, value_all


def decode_group(tokens, cache_lens, key_cache, value_cache, weight_stack):
    cache_pos = jnp.arange(CACHE_LEN)
    write_mask = (cache_pos[None, :] == cache_lens[:, None])[:, :, None, None]
    allowed = (cache_pos[None, :] <= cache_lens[:, None])[:, None, None, :]

    def layer_step(hidden, layer_weights):
        gain_attn, w_qkv, w_out, gain_mlp, w_gate_up, w_down, key_old, value_old = layer_weights
        normed = rms_norm(hidden, gain_attn)
        projected = jnp.einsum('bd,dkjh->bkjh', normed.astype(jnp.float32), w_qkv.astype(jnp.float32))
        rotated = rope_rotate(projected[:, :, :GROUP_Q + 1], cache_lens).astype(jnp.bfloat16)
        value_new = projected[:, :, GROUP_Q + 1].astype(jnp.bfloat16)
        key_now = jnp.where(write_mask, rotated[:, None, :, GROUP_Q], key_old)
        value_now = jnp.where(write_mask, value_new[:, None], value_old)
        scores = jnp.einsum('bkgh,btkh->bkgt', rotated[:, :, :GROUP_Q].astype(jnp.float32), key_now.astype(jnp.float32)) * HEAD ** -0.5
        scores = jnp.where(allowed, scores, -1e30)
        weights = jnp.exp(scores - jnp.max(scores, axis=-1, keepdims=True))
        weight_sum = jnp.sum(weights, axis=-1)
        mixed_sum = jnp.einsum('bkgt,btkh->bkgh', weights.astype(jnp.bfloat16).astype(jnp.float32), value_now.astype(jnp.float32))
        context = (mixed_sum / weight_sum[..., None]).astype(jnp.bfloat16)
        attn_sum = jnp.einsum('bkgh,kghd->bd', context.astype(jnp.float32), w_out.astype(jnp.float32))
        hidden = (hidden.astype(jnp.float32) + attn_sum).astype(jnp.bfloat16)
        down_sum = mlp_sum(hidden, gain_mlp, w_gate_up, w_down)
        hidden = (hidden.astype(jnp.float32) + down_sum).astype(jnp.bfloat16)
        return hidden, (key_now, value_now)

    hidden, (key_all, value_all) = lax.scan(layer_step, tokens, weight_stack + (key_cache, value_cache))
    return hidden, key_all, value_all


def reference(x_prompt, s_len, y_tok, c_len, k_cache, v_cache, attn_gain, w_qkv, w_out, mlp_gain, w_gate_up, w_down):
    weight_stack = (attn_gain, w_qkv, w_out, mlp_gain, w_gate_up, w_down)

    def run_prefill(group_args):
        return prefill_group(group_args[0], group_args[1], weight_stack)

    hidden_out, key_pre, value_pre = lax.map(run_prefill, (x_prompt, s_len))
    k_prompt = jnp.moveaxis(jnp.roll(key_pre, 1, axis=0), 0, 1)
    v_prompt = jnp.moveaxis(jnp.roll(value_pre, 1, axis=0), 0, 1)
    cache_shape = (LAYERS, GROUPS, BATCH_DEC, CACHE_LEN, KV_HEADS, HEAD)

    def run_decode(group_args):
        return decode_group(group_args[0], group_args[1], group_args[2], group_args[3], weight_stack)

    decode_in = (y_tok.reshape(GROUPS, BATCH_DEC, D), c_len.reshape(GROUPS, BATCH_DEC), jnp.moveaxis(k_cache.reshape(cache_shape), 1, 0), jnp.moveaxis(v_cache.reshape(cache_shape), 1, 0))
    y_out, key_new, value_new = lax.map(run_decode, decode_in)
    k_cache_out = jnp.moveaxis(key_new, 0, 1).reshape(k_cache.shape)
    v_cache_out = jnp.moveaxis(value_new, 0, 1).reshape(v_cache.shape)
    return (hidden_out, y_out.reshape(GROUPS * BATCH_DEC, D), k_prompt, v_prompt, k_cache_out, v_cache_out)
```

```python
import functools

import jax
import jax.numpy as jnp
from jax import lax
from jax.experimental import pallas as pl
from jax.experimental.pallas import tpu as pltpu
from jax.sharding import PartitionSpec as P

ROPE_BASE = 10000.0
NORM_EPS = 1e-5
SUBS = 4

ORDER = (
    'Q0', 'T0', 'Q1', 'w1.2', 'T1', 'Q2', 'T2', 'w2.2', 'Q3', 'w1.3', 'T3', 'w3.2', 'K', 'c0.2', 'k0k', 'k0v', 'k1k',
    'D1', 'w2.3', 'c1.2', 'l0k', 'l0v', 'c2.2', 'w3.3', 'c0.3', 'c3.2', 'O0', 'c1.3', 'c2.3', 'k1v', 'k2k', 'l1k',
    'U0', 'c3.3', 'D2', 'W0', 's0', 's1', 'O1', 'U1', 'k2v', 'k3k', 'l1v', 'l2k', 'W1', 'a0', 's2', 'O2', 'a1', 's3',
    'U2', 'k3v', 'l2v', 'W2', 'O3', 'b0', 'a2', 's4', 'l3k', 'U3', 'f0', 'b1', 'a3', 's5', 'W3', 'b2', 'l3v', 'f1',
    'b3', 'a4', 's6', 'g0', 'f2', 'b4', 'a5', 's7', 'f3', 'h0', 'g1', 'f4', 'b5', 'a6', 's8', 'o0', 'h1', 'g2', 'f5',
    'b6', 'a7', 's9', 'o1', 'h2', 'g3', 'g4', 'f6', 'b7', 'o2', 'h3', 'a8', 's10', 'h4', 'g5', 'f7', 'o3', 'b8',
    'a9', 's11', 'o4', 'h5', 'g6', 'f8', 'b9', 'a10', 's12', 'o5', 'h6', 'g7', 'f9', 'b10', 'a11', 's13', 'o6', 'h7',
    'g8', 'f10', 'b11', 'a12', 's14', 'o7', 'h8', 'g9', 'f11', 'b12', 'a13', 's15', 'o8', 'h9', 'g10', 'f12', 'b13',
    'a14', 'o9', 'h10', 'g11', 'f13', 'b14', 'a15', 'o10', 'h11', 'g12', 'g13', 'f14', 'b15', 'o11', 'h12', 'g14',
    'h13', 'f15', 'h14', 'o12', 'g15', 'o13', 'h15', 'o14', 'o15',
)
MIDDLE = ()


def rms_scale(values_f32, gain_f32):
    inv_rms = lax.rsqrt(jnp.mean(values_f32 * values_f32, axis=-1, keepdims=True) + NORM_EPS)
    return (values_f32 * inv_rms * gain_f32).astype(jnp.bfloat16)


def rope_tables(positions, head_dim):
    half_dim = head_dim // 2
    inv_freq = ROPE_BASE ** (-2.0 * jnp.arange(half_dim, dtype=jnp.float32) / head_dim)
    angles = positions.astype(jnp.float32)[:, None] * inv_freq[None, :]
    cos_table = jnp.cos(angles)
    sin_table = jnp.sin(angles)
    return jnp.concatenate([cos_table, cos_table], axis=1), jnp.concatenate([-sin_table, sin_table], axis=1)


def qkv_kernel(head_dim, x_ref, gain_ref, w_ref, cos_ref, sin_ref, out_ref, normed_ref):
    part = pl.program_id(0)

    @pl.when((part == 0) & (pl.program_id(1) == 0))
    def _():
        normed_ref[...] = rms_scale(x_ref[...].astype(jnp.float32), gain_ref[...].astype(jnp.float32))

    acc = jnp.dot(normed_ref[...], w_ref[0], preferred_element_type=jnp.float32)

    @pl.when(part < 2)
    def _():
        for head in range(acc.shape[1] // head_dim):
            vals = acc[:, head * head_dim:(head + 1) * head_dim]
            turned = pltpu.roll(vals, head_dim // 2, 1)
            out_ref[0, :, head * head_dim:(head + 1) * head_dim] = (vals * cos_ref[...] + turned * sin_ref[...]).astype(out_ref.dtype)

    @pl.when(part == 2)
    def _():
        out_ref[0] = acc.astype(out_ref.dtype)


def project_qkv(chunk_in, gain, w_parts, cos_table, sin_table, head_dim):
    rows, depth = chunk_in.shape
    width = w_parts.shape[2]
    block = min(512, width)
    return pl.pallas_call(
        functools.partial(qkv_kernel, head_dim),
        out_shape=jax.ShapeDtypeStruct((3, rows, width), jnp.bfloat16),
        grid=(3, width // block),
        in_specs=[
            pl.BlockSpec((rows, depth), lambda j, n: (0, 0)),
            pl.BlockSpec((1, depth), lambda j, n: (0, 0)),
            pl.BlockSpec((1, depth, block), lambda j, n: (j, 0, n)),
            pl.BlockSpec((rows, head_dim), lambda j, n: (0, 0)),
            pl.BlockSpec((rows, head_dim), lambda j, n: (0, 0)),
        ],
        out_specs=pl.BlockSpec((1, rows, block), lambda j, n: (j, 0, n)),
        scratch_shapes=[pltpu.VMEM((rows, depth), jnp.bfloat16)],
        compiler_params=pltpu.CompilerParams(dimension_semantics=("arbitrary", "arbitrary"), vmem_limit_bytes=48 << 20),
        cost_estimate=pl.CostEstimate(flops=2 * rows * depth * 3 * width, bytes_accessed=2 * (rows * depth + 3 * depth * width + 3 * rows * width), transcendentals=0),
        name="project_qkv",
    )(chunk_in, gain, w_parts, cos_table, sin_table)


def attend_kernel(chunk, first_checked, q_rows, slen_ref, *refs):
    q_ref = refs[0]
    k_refs = refs[1:chunk + 2]
    v_refs = refs[chunk + 2:2 * chunk + 3]
    out_ref = refs[-1]
    rows, head_dim = q_ref.shape[1], q_ref.shape[2]
    scale = head_dim ** -0.5
    limit = slen_ref[0]
    for start in range(0, rows, q_rows):
        query = q_ref[0, start:start + q_rows, :]
        scores = []
        values = []
        for part in range(chunk + 1):
            keys = rows if part < chunk else start + q_rows
            score = lax.dot_general(query, k_refs[part][0, :keys, :], (((1,), (1,)), ((), ())), preferred_element_type=jnp.float32) * scale
            key_pos = lax.broadcasted_iota(jnp.int32, score.shape, 1)
            if part == chunk:
                allowed = key_pos <= lax.broadcasted_iota(jnp.int32, score.shape, 0) + start
                if part >= first_checked:
                    allowed = allowed & (key_pos < limit - part * rows)
                score = jnp.where(allowed, score, -1e30)
            elif part >= first_checked:
                score = jnp.where(key_pos < limit - part * rows, score, -1e30)
            scores.append(score)
            values.append(v_refs[part][0, :keys, :])
        peak = functools.reduce(jnp.maximum, [jnp.max(score, axis=-1, keepdims=True) for score in scores])
        total = jnp.zeros((q_rows, 1), jnp.float32)
        mixed = jnp.zeros((q_rows, head_dim), jnp.float32)
        for score, value in zip(scores, values):
            weight = jnp.exp(score - peak)
            total = total + jnp.sum(weight, axis=-1, keepdims=True)
            mixed = mixed + jnp.dot(weight.astype(jnp.bfloat16), value, preferred_element_type=jnp.float32)
        out_ref[start:start + q_rows, :] = (mixed / total).astype(out_ref.dtype)


def attend(chunk, chunks, rows, s_len, parts, head_dim):
    width = parts[0].shape[2]
    heads = width // head_dim

    def pick(which):
        return pl.BlockSpec((1, rows, head_dim), lambda h, slen: (which, 0, h))

    total_keys = rows * (chunk + 1)
    return pl.pallas_call(
        functools.partial(attend_kernel, chunk, chunks // 2, min(256, rows)),
        out_shape=jax.ShapeDtypeStruct((rows, width), jnp.bfloat16),
        grid_spec=pltpu.PrefetchScalarGridSpec(
            num_scalar_prefetch=1,
            grid=(heads,),
            in_specs=[pick(0)] + [pick(1)] * (chunk + 1) + [pick(2)] * (chunk + 1),
            out_specs=pl.BlockSpec((rows, head_dim), lambda h, slen: (0, h)),
        ),
        compiler_params=pltpu.CompilerParams(dimension_semantics=("arbitrary",), vmem_limit_bytes=48 << 20),
        cost_estimate=pl.CostEstimate(flops=8 * heads * rows * total_keys * head_dim, bytes_accessed=2 * width * (2 * total_keys + 2 * rows), transcendentals=heads * rows * total_keys),
        name=f"attend_{chunk}",
    )(s_len, parts[chunk], *parts, *parts)


def output_kernel(size, extra, where_ref, *refs):
    sources = refs[:2 * size - 1]
    refs = refs[2 * size - 1:]
    if extra:
        extra_ref, refs = refs[0], refs[1:]
    w_own_ref, refs = refs[0], refs[1:]
    heads, head_dim, block = w_own_ref.shape
    w_refs = refs[:(size - 1) * heads]
    x_ref, gain_ref, hidden_ref, normed_ref, full_ref, square_ref = refs[(size - 1) * heads:]
    rows, width = sources[0].shape
    step = pl.program_id(0)

    @pl.when(step == 0)
    def _():
        square_ref[...] = jnp.zeros_like(square_ref)
        for place in range(size):
            @pl.when(where_ref[0] == place)
            def _():
                for d in range(size):
                    source = sources[size - 1 - d] if place >= d else sources[2 * size - 1 - d]
                    if d == 0:
                        full_ref[d, :rows] = source[...]
                        if extra:
                            full_ref[d, rows:] = extra_ref[place]
                        continue
                    for r in range(heads):
                        columns = pl.ds(pl.multiple_of(lax.bitwise_xor(where_ref[1], r) * head_dim, head_dim), head_dim)
                        full_ref[d, :rows, r * head_dim:(r + 1) * head_dim] = source[:, columns]
                        if extra:
                            full_ref[d, rows:, r * head_dim:(r + 1) * head_dim] = extra_ref[(place - d) % size, :, columns]

    acc = jnp.dot(full_ref[0], w_own_ref[...].reshape(width, block), preferred_element_type=jnp.float32)
    for d in range(1, size):
        w_block = jnp.concatenate([w_ref[...] for w_ref in w_refs[(d - 1) * heads:d * heads]], axis=0)
        acc = acc + jnp.dot(full_ref[d], w_block, preferred_element_type=jnp.float32)
    hidden = (x_ref[...].astype(jnp.float32) + acc).astype(jnp.bfloat16)
    columns = pl.ds(pl.multiple_of(step * block, block), block)
    hidden_ref[:, columns] = hidden
    hidden_f32 = hidden.astype(jnp.float32)
    square_ref[...] += jnp.sum(hidden_f32 * hidden_f32, axis=-1, keepdims=True)

    @pl.when(step == pl.num_programs(0) - 1)
    def _():
        depth = hidden_ref.shape[1]
        inv_rms = lax.rsqrt(square_ref[...] / depth + NORM_EPS)
        for start in range(0, depth, block):
            normed_ref[:, start:start + block] = (hidden_ref[:, start:start + block].astype(jnp.float32) * inv_rms * gain_ref[:, start:start + block].astype(jnp.float32)).astype(jnp.bfloat16)


def project_out(where, sources, extra, w_own, w_others, residual, gain):
    total_rows, depth = residual.shape
    rows, width = sources[0].shape
    heads, head_dim = w_own.shape[:2]
    size = (len(sources) + 1) // 2
    block = min(512, depth)
    whole = lambda shape: pl.BlockSpec(shape, lambda n, where: (0,) * len(shape), pipeline_mode=pl.Buffered(1))
    extras = [] if extra is None else [extra]
    return pl.pallas_call(
        functools.partial(output_kernel, size, extra is not None),
        out_shape=[jax.ShapeDtypeStruct((total_rows, depth), jnp.bfloat16)] * 2,
        grid_spec=pltpu.PrefetchScalarGridSpec(
            num_scalar_prefetch=1,
            grid=(depth // block,),
            in_specs=[whole((rows, width))] * (2 * size - 1) + [whole(e.shape) for e in extras] + [
                pl.BlockSpec((heads, head_dim, block), lambda n, where: (0, 0, n)),
            ] + [pl.BlockSpec((head_dim, block), lambda n, where: (0, n))] * len(w_others) + [
                pl.BlockSpec((total_rows, block), lambda n, where: (0, n)),
                whole((1, depth)),
            ],
            out_specs=[whole((total_rows, depth))] * 2,
            scratch_shapes=[pltpu.VMEM((size, total_rows, width), jnp.bfloat16), pltpu.VMEM((total_rows, 1), jnp.float32)],
        ),
        compiler_params=pltpu.CompilerParams(dimension_semantics=("arbitrary",), vmem_limit_bytes=56 << 20),
        cost_estimate=pl.CostEstimate(flops=2 * total_rows * size * width * depth, bytes_accessed=2 * (size * width * depth + 7 * rows * width + 3 * total_rows * depth), transcendentals=0),
        name="project_out",
    )(where, *sources, *extras, w_own, *w_others, residual, gain)


def pick_by(index, options):
    result = options[0]
    for place in range(1, len(options)):
        result = jnp.where(index == place, options[place], result)
    return result


def solution(mesh):
    side_size = mesh.shape['side']
    tp_size = mesh.shape['tp']
    seats = mesh.shape['pair'] * side_size
    group_axes = ('pair', 'side')
    last = tp_size - 1

    def cyclic(value, d):
        return lax.ppermute(value, 'tp', [(t, (t + d) % tp_size) for t in range(tp_size)])

    def swap(value, mask):
        return lax.ppermute(value, group_axes, [(q, q ^ mask) for q in range(seats)])

    def in_order(me, copies):
        return [pick_by(me, [copies[(t - j) % tp_size] for t in range(tp_size)]) for j in range(tp_size)]

    def device_fn(x_prompt, s_len, y_tok, c_len, k_cache, v_cache, attn_gain, w_qkv, w_out, mlp_gain, w_gate_up, w_down):
        me = lax.axis_index('tp')
        seat = lax.axis_index('pair') * side_size + lax.axis_index('side')
        where = jnp.stack([me, seat]).astype(jnp.int32)
        seq_len, depth = x_prompt.shape[1:]
        heads_local = w_qkv.shape[2]
        head_dim = w_qkv.shape[4]
        width = heads_local * head_dim
        rows = seq_len // tp_size
        decodes = y_tok.shape[0]
        pad = 16
        half = rows // 2
        piece = half // SUBS
        cache_local = k_cache.shape[2]
        up_pairs = [(t, t + 1) for t in range(last)]
        down_pairs = [(t + 1, t) for t in range(last)]
        val = {}

        def tie(keys):
            keys = list(dict.fromkeys(keys))
            for key, value in zip(keys, lax.optimization_barrier(tuple(val[key] for key in keys))):
                val[key] = value

        def hop(value, chain, source, target):
            real = (lambda t: t) if chain == 0 else (lambda t: last - t)
            return lax.ppermute(value, 'tp', [(real(source), real(target))])

        def rows_of(name, m, chain):
            start = chain * half + (m % SUBS) * piece
            return val[name, m // SUBS][start:start + piece]

        w_own = w_out[0, :, 0]
        w_seat = lax.dynamic_index_in_dim(w_own, seat, 0, keepdims=False)
        for d in range(1, tp_size):
            val['w', d, 0] = cyclic(w_seat, d)

        w_parts = jnp.transpose(w_qkv[0], (2, 0, 1, 3)).reshape(3, depth, width)
        positions = jnp.concatenate([jnp.arange(seq_len, dtype=jnp.int32), c_len, jnp.zeros((pad - decodes,), jnp.int32)])
        cos_table, sin_table = rope_tables(positions, head_dim)
        y_pad = jnp.concatenate([y_tok, jnp.zeros((pad - decodes, depth), y_tok.dtype)])
        valid = (jnp.arange(seq_len) < s_len[0]).astype(jnp.bfloat16)
        val['w_parts'] = w_parts
        val['gain'], val['s_len'], val['mlp_gain'], val['valid'] = attn_gain, s_len, mlp_gain, valid
        val['out'] = jnp.zeros((seq_len, depth), jnp.bfloat16)
        for which in range(2):
            val['cache', which] = jnp.zeros((rows, tp_size, heads_local, head_dim), jnp.bfloat16)

        def compute(name):
            kind = name[0]
            c = int(name[1:]) if name[1:].isdigit() else 0
            lo, hi = c * rows, (c + 1) * rows
            if kind == 'Q':
                tie(thread + ['gain'])
                chunk_in = x_prompt[0, lo:hi]
                cos_c, sin_c = cos_table[lo:hi], sin_table[lo:hi]
                if c == 0:
                    chunk_in = jnp.concatenate([chunk_in, y_pad])
                    cos_c = jnp.concatenate([cos_c, cos_table[seq_len:]])
                    sin_c = jnp.concatenate([sin_c, sin_table[seq_len:]])
                made = project_qkv(chunk_in, val['gain'], val['w_parts'], cos_c, sin_c, head_dim)
                val['qkv', c] = made
                if c == 0:
                    val['dq', 0] = made[:, rows:rows + decodes].reshape(3, decodes, heads_local, head_dim)
                    for d in range(1, tp_size):
                        val['dq', d] = cyclic(val['dq', 0], d)
                return [('qkv', c)]
            if kind == 'T':
                tie(thread + ['s_len'])
                context = attend(c, tp_size, rows, val['s_len'], [val['qkv', i] for i in range(c + 1)], head_dim)
                val['L', c, 0] = val['R', c, 0] = context
                val['L', c, 1] = lax.ppermute(context, 'tp', up_pairs)
                val['R', c, 1] = lax.ppermute(context, 'tp', down_pairs)
                return [('L', c, 0)]
            if kind == 'K':
                tie(thread + ['valid'])
                made = []
                for d in range(tp_size):
                    for which in range(2):
                        rows_d = pick_by(me, [val['qkv', (t + d) % tp_size][which + 1, :rows] for t in range(tp_size)])
                        keep = pick_by(me, [val['valid'][((t + d) % tp_size) * rows:((t + d) % tp_size + 1) * rows] for t in range(tp_size)])
                        val['kv', d, which] = (rows_d * keep[:, None]).reshape(rows, heads_local, head_dim)
                        made.append(('kv', d, which))
                return made
            if name == 'D1':
                tie(thread + [('dq', d) for d in range(tp_size)])
                dec_full = jnp.concatenate(in_order(me, [val['dq', d] for d in range(tp_size)]), axis=2)
                cache_pos = me * cache_local + jnp.arange(cache_local)
                write_mask = (cache_pos[None, :] == c_len[:, None])[:, :, None, None]
                allowed = (cache_pos[None, :] <= c_len[:, None])[:, None, :]
                key_now = jnp.where(write_mask, dec_full[1][:, None], k_cache[0])
                value_now = jnp.where(write_mask, dec_full[2][:, None], v_cache[0])
                val['key_now'], val['value_now'] = key_now, value_now
                scores = jnp.einsum('bkh,btkh->bkt', dec_full[0], key_now, preferred_element_type=jnp.float32) * head_dim ** -0.5
                scores = jnp.where(allowed, scores, -1e30)
                peak = jnp.max(scores, axis=-1, keepdims=True)
                weights = jnp.exp(scores - peak)
                total = jnp.sum(weights, axis=-1, keepdims=True)
                mixed = jnp.einsum('bkt,btkh->bkh', weights.astype(jnp.bfloat16), value_now, preferred_element_type=jnp.float32)
                packed = jnp.stack([mixed, jnp.broadcast_to(peak, mixed.shape), jnp.broadcast_to(total, mixed.shape)])
                packed = packed.reshape(3, decodes, tp_size, heads_local, head_dim)
                for d in range(tp_size):
                    share = lax.dynamic_index_in_dim(packed, lax.rem(me + d, tp_size), 2, keepdims=False)
                    val['ds', d] = share if d == 0 else cyclic(share, d)
                return [('ds', 0)]
            if name == 'D2':
                tie(thread + [('ds', d) for d in range(tp_size)])
                shares = [val['ds', d] for d in range(tp_size)]
                top = functools.reduce(jnp.maximum, [share[1] for share in shares])
                factors = [jnp.exp(share[1] - top) for share in shares]
                dec_mixed = sum(share[0] * factor for share, factor in zip(shares, factors))
                dec_total = sum(share[2] * factor for share, factor in zip(shares, factors))
                val['dc', 0] = (dec_mixed / dec_total).astype(jnp.bfloat16).reshape(decodes, width)
                for d in range(1, tp_size):
                    val['dc', d] = cyclic(val['dc', 0], d)
                return [('dc', 0)]
            if kind == 'O':
                source_keys = [('L', c, d) for d in range(last, 0, -1)] + [('L', c, 0)] + [('R', c, d) for d in range(1, tp_size)]
                w_keys = [('w', d, r) for d in range(1, tp_size) for r in range(seats)]
                extra_keys = [('dc', d) for d in range(tp_size)] if c == last else []
                tie(thread + ['mlp_gain'] + source_keys + extra_keys + (w_keys if c == 0 else []))
                residual = x_prompt[0, lo:hi]
                extra = None
                if c == last:
                    extra = jnp.pad(jnp.stack(in_order(me, [val[key] for key in extra_keys])), ((0, 0), (0, pad - decodes), (0, 0)))
                    residual = jnp.concatenate([residual, y_pad])
                val['h', c], val['normed', c] = project_out(where, [val[key] for key in source_keys], extra, w_own, [val[key] for key in w_keys], residual, val['mlp_gain'])
                return [('h', c), ('normed', c)]
            if kind == 'U':
                tie(thread)
                gate_up = jnp.einsum('sd,dcf->scf', val['normed', c], w_gate_up[0], preferred_element_type=jnp.float32)
                val['act', c] = (jax.nn.silu(gate_up[:, 0]) * gate_up[:, 1]).astype(jnp.bfloat16)
                return [('act', c), ('h', c)]
            tie(thread)
            val['p', c] = jnp.dot(val['act', c], w_down[0], preferred_element_type=jnp.float32)
            if c == last:
                val['dp', 0] = val['p', c][rows:rows + decodes]
                for d in range(1, tp_size):
                    val['dp', d] = cyclic(val['dp', 0], d)
            return [('p', c), ('h', c)]

        def transfer(name):
            kind = name[0]
            if kind == 'c':
                c, step = map(int, name[1:].split('.'))
                tie(thread + [('L', c, step - 1), ('R', c, step - 1)])
                val['L', c, step] = lax.ppermute(val['L', c, step - 1], 'tp', [(a, b) for a, b in up_pairs if a >= step - 1])
                val['R', c, step] = lax.ppermute(val['R', c, step - 1], 'tp', [(a, b) for a, b in down_pairs if a <= last - step + 1])
                return
            if kind == 'w':
                d, step = map(int, name[1:].split('.'))
                masks = range(0, seats, 2) if step == 3 else [0]
                tie(thread + [('w', d, mask) for mask in masks])
                for mask in ([1] if step == 3 else range(2, seats, 2)):
                    for base in masks:
                        val['w', d, base ^ mask] = swap(val['w', d, base], mask)
                return
            if kind == 'k':
                d, which = int(name[1]), 'kv'.index(name[2])
                tie(thread + [('kv', d, which)])
                route = [(t * side_size + s, ((t + d) % tp_size) * side_size + (s + 1) % side_size) for t in range(tp_size) for s in range(side_size)]
                val['landed', d, which] = lax.ppermute(val['kv', d, which], ('tp', 'side'), route)
                return
            if kind == 'l':
                d, which = int(name[1]), 'kv'.index(name[2])
                tie(thread + [('landed', d, which), ('cache', which)])
                val['cache', which] = lax.dynamic_update_slice(val['cache', which], val['landed', d, which][:, None], (0, lax.rem(me - d + tp_size, tp_size), 0, 0))
                return
            m = int(name[1:])
            c = m // SUBS
            owner = 1 if m in MIDDLE else 0
            if kind == 's':
                tie(thread + [('p', c)])
            elif kind == 'o':
                tie(thread + ['out'] + [('g', m, chain, t) for chain in range(2) for t in range(tp_size)])
            else:
                reads = {'a': [('r', 3)], 'b': [('r', 2)], 'f': [('r', 2), ('r', 0)] if owner else [('r', 1)], 'g': [('g', owner + 1)], 'h': [('g', 2)]}[kind]
                tie(thread + [(table, m, chain, t) for chain in range(2) for table, t in reads] + ([('p', c)] if kind in 'abf' else []))
            for chain in range(2):
                if kind == 's':
                    part = rows_of('p', m, chain)
                    val['r', m, chain, 3] = hop(part, chain, 3, 2)
                    if owner:
                        val['r', m, chain, 0] = hop(part, chain, 0, 1)
                elif kind == 'a':
                    val['r', m, chain, 2] = hop(val['r', m, chain, 3] + rows_of('p', m, chain), chain, 2, 1)
                elif kind == 'b':
                    val['r', m, chain, 1] = hop(val['r', m, chain, 2] + rows_of('p', m, chain), chain, 1, 0)
                elif kind == 'f':
                    total = val['r', m, chain, 2] + val['r', m, chain, 0] if owner else val['r', m, chain, 1]
                    finished = (rows_of('h', m, chain).astype(jnp.float32) + (total + rows_of('p', m, chain))).astype(jnp.bfloat16)
                    val['g', m, chain, owner] = finished
                    val['g', m, chain, owner + 1] = hop(finished, chain, owner, owner + 1)
                    if owner:
                        val['g', m, chain, 0] = hop(finished, chain, 1, 0)
                elif kind == 'g':
                    val['g', m, chain, owner + 2] = hop(val['g', m, chain, owner + 1], chain, owner + 1, owner + 2)
                elif kind == 'h':
                    val['g', m, chain, 3] = hop(val['g', m, chain, 2], chain, 2, 3)
                elif kind == 'o':
                    place = me if chain == 0 else last - me
                    rows_m = pick_by(place, [val['g', m, chain, t] for t in range(tp_size)])
                    val['out'] = lax.dynamic_update_slice(val['out'], rows_m, (c * rows + chain * half + (m % SUBS) * piece, 0))

        thread = ['w_parts']
        for name in ORDER:
            if name[0] in 'QTKDOUW':
                made = compute(name)
                thread = thread + made if name in ('K', 'D1', 'D2') else made
            else:
                transfer(name)
                if name[0] == 'o':
                    thread = thread + ['out']

        dec_sum = functools.reduce(jnp.add, in_order(me, [val['dp', d] for d in range(tp_size)]))
        tokens = (val['h', last][rows:rows + decodes].astype(jnp.float32) + dec_sum).astype(jnp.bfloat16)
        caches = [val['cache', which].reshape(1, 1, rows, tp_size * heads_local, head_dim) for which in range(2)]
        return (val['out'][None], tokens, caches[0], caches[1], val['key_now'][None], val['value_now'][None])

    cache_spec = P(None, group_axes, 'tp', None, None)
    in_specs = (P(group_axes, None, None), P(group_axes), P(group_axes, None), P(group_axes), cache_spec, cache_spec, P(), P(None, None, 'tp', None, None), P(None, 'tp', None, None, None), P(), P(None, None, None, 'tp'), P(None, 'tp', None))
    out_specs = (P(group_axes, None, None), P(group_axes, None), cache_spec, cache_spec, cache_spec, cache_spec)
    return jax.shard_map(device_fn, mesh=mesh, in_specs=in_specs, out_specs=out_specs, check_vma=False)
```

```python
import functools

import jax
import jax.numpy as jnp
from jax import lax
from jax.experimental import pallas as pl
from jax.experimental.pallas import tpu as pltpu
from jax.sharding import PartitionSpec as P

ROPE_BASE = 10000.0
NORM_EPS = 1e-5

ORDER = (
    'Q0', 'T0', 'Q1', 'T1', 'c0.2', 'w2', 'Q2', 'T2', 'c0.3', 'c1.2', 'Q3', 'T3', 'c1.3', 'c2.2', 'K', 'D1',
    'c2.3', 'c3.2', 'D2', 'w3', 'O0', 'O1', 'c3.3', 'O2', 'k2k', 'k2v', 'k1k', 'k1v', 'k3k', 'k3v', 'k0k', 'k0v', 'O3', 'B',
    'l0k', 'l0v', 'l1k', 'l1v', 'l2k', 'l2v', 'l3k', 'l3v',
)


def rms_scale(values_f32, gain_f32):
    inv_rms = lax.rsqrt(jnp.mean(values_f32 * values_f32, axis=-1, keepdims=True) + NORM_EPS)
    return (values_f32 * inv_rms * gain_f32).astype(jnp.bfloat16)


def rope_tables(positions, head_dim):
    half_dim = head_dim // 2
    inv_freq = ROPE_BASE ** (-2.0 * jnp.arange(half_dim, dtype=jnp.float32) / head_dim)
    angles = positions.astype(jnp.float32)[:, None] * inv_freq[None, :]
    cos_table = jnp.cos(angles)
    sin_table = jnp.sin(angles)
    return jnp.concatenate([cos_table, cos_table], axis=1), jnp.concatenate([-sin_table, sin_table], axis=1)


def qkv_kernel(head_dim, extra, *refs):
    x_ref, gain_ref, wq_ref, wk_ref, wv_ref, cos_ref, sin_ref = refs[:7]
    extra_refs = refs[7:10] if extra else None
    q_ref, k_ref, v_ref, token_ref, normed_ref = refs[-5:]
    rows = x_ref.shape[0]

    @pl.when(pl.program_id(0) == 0)
    def _():
        gain = gain_ref[...].astype(jnp.float32)
        normed_ref[:rows] = rms_scale(x_ref[...].astype(jnp.float32), gain)
        if extra:
            normed_ref[rows:] = rms_scale(extra_refs[0][...].astype(jnp.float32), gain)
        token_ref[...] = jnp.zeros_like(token_ref)

    cos, sin = cos_ref[...], sin_ref[...]
    if extra:
        cos = jnp.concatenate([cos, extra_refs[1][...]], axis=0)
        sin = jnp.concatenate([sin, extra_refs[2][...]], axis=0)
    for w_ref, out_ref in ((wq_ref, q_ref), (wk_ref, k_ref), (wv_ref, v_ref)):
        acc = jnp.dot(normed_ref[...], w_ref[...], preferred_element_type=jnp.float32)
        for start in range(0, acc.shape[1], head_dim):
            vals = acc[:, start:start + head_dim]
            if out_ref is not v_ref:
                vals = vals * cos + pltpu.roll(vals, head_dim // 2, 1) * sin
            out_ref[:, start:start + head_dim] = vals.astype(out_ref.dtype)


TOKEN = jax.ShapeDtypeStruct((8, 128), jnp.float32)


def project_qkv(chunk, rows, token, x, extra_rows, gain, w_all, tables, extra_tables, head_dim):
    depth = x.shape[1]
    width = w_all.shape[1] // 3
    block = 2 * head_dim
    steps = width // block
    extras = [] if extra_rows is None else [extra_rows, *extra_tables]
    total = rows + (0 if extra_rows is None else extra_rows.shape[0])
    whole = lambda shape: pl.BlockSpec(shape, lambda n: (0, 0), pipeline_mode=pl.Buffered(1))
    columns = lambda part: pl.BlockSpec((depth, block), lambda n: (0, part * steps + n))
    return pl.pallas_call(
        functools.partial(qkv_kernel, head_dim, extra_rows is not None),
        out_shape=[jax.ShapeDtypeStruct((total, width), jnp.bfloat16)] * 3 + [TOKEN],
        grid=(steps,),
        in_specs=[
            pl.BlockSpec((rows, depth), lambda n: (chunk, 0), pipeline_mode=pl.Buffered(1)),
            whole((1, depth)),
            columns(0),
            columns(1),
            columns(2),
            pl.BlockSpec((rows, head_dim), lambda n: (chunk, 0), pipeline_mode=pl.Buffered(1)),
            pl.BlockSpec((rows, head_dim), lambda n: (chunk, 0), pipeline_mode=pl.Buffered(1)),
        ] + [whole(e.shape) for e in extras] + [pl.BlockSpec(memory_space=pl.ANY)],
        out_specs=[pl.BlockSpec((total, block), lambda n: (0, n))] * 3 + [whole(TOKEN.shape)],
        scratch_shapes=[pltpu.VMEM((total, depth), jnp.bfloat16)],
        compiler_params=pltpu.CompilerParams(dimension_semantics=("arbitrary",), vmem_limit_bytes=48 << 20),
        cost_estimate=pl.CostEstimate(flops=6 * total * depth * width, bytes_accessed=2 * (total * depth + 3 * depth * width + 3 * total * width), transcendentals=0),
        name="project_qkv",
    )(x, gain, w_all, w_all, w_all, *tables, *extras, token)


def attend_kernel(chunk, first_checked, q_rows, slen_ref, *refs):
    q_ref = refs[0]
    k_refs = refs[1:chunk + 2]
    v_refs = refs[chunk + 2:2 * chunk + 3]
    out_ref, token_ref = refs[-2:]
    token_ref[...] = jnp.zeros_like(token_ref)
    rows, head_dim = q_ref.shape
    scale = head_dim ** -0.5
    limit = slen_ref[0]
    for start in range(0, rows, q_rows):
        query = q_ref[start:start + q_rows, :]
        scores = []
        values = []
        for part in range(chunk + 1):
            keys = rows if part < chunk else start + q_rows
            score = lax.dot_general(query, k_refs[part][:keys, :], (((1,), (1,)), ((), ())), preferred_element_type=jnp.float32) * scale
            key_pos = lax.broadcasted_iota(jnp.int32, score.shape, 1)
            if part == chunk:
                allowed = key_pos <= lax.broadcasted_iota(jnp.int32, score.shape, 0) + start
                if part >= first_checked:
                    allowed = allowed & (key_pos < limit - part * rows)
                score = jnp.where(allowed, score, -1e30)
            elif part >= first_checked:
                score = jnp.where(key_pos < limit - part * rows, score, -1e30)
            scores.append(score)
            values.append(v_refs[part][:keys, :])
        peak = functools.reduce(jnp.maximum, [jnp.max(score, axis=-1, keepdims=True) for score in scores])
        total = jnp.zeros((q_rows, 1), jnp.float32)
        mixed = jnp.zeros((q_rows, head_dim), jnp.float32)
        for score, value in zip(scores, values):
            weight = jnp.exp(score - peak)
            total = total + jnp.sum(weight, axis=-1, keepdims=True)
            mixed = mixed + jnp.dot(weight.astype(jnp.bfloat16), value, preferred_element_type=jnp.float32)
        out_ref[start:start + q_rows, :] = (mixed / total).astype(out_ref.dtype)


def attend(chunk, chunks, rows, token, s_len, queries, keys, values, head_dim):
    width = queries.shape[1]
    heads = width // head_dim

    pick = pl.BlockSpec((rows, head_dim), lambda h, slen: (0, h))
    total_keys = rows * (chunk + 1)
    return pl.pallas_call(
        functools.partial(attend_kernel, chunk, chunks // 2, min(256, rows)),
        out_shape=[jax.ShapeDtypeStruct((rows, width), jnp.bfloat16), TOKEN],
        grid_spec=pltpu.PrefetchScalarGridSpec(
            num_scalar_prefetch=1,
            grid=(heads,),
            in_specs=[pick] * (2 * chunk + 3) + [pl.BlockSpec(memory_space=pl.ANY)],
            out_specs=[pick, pl.BlockSpec(TOKEN.shape, lambda h, slen: (0, 0))],
        ),
        compiler_params=pltpu.CompilerParams(dimension_semantics=("arbitrary",), vmem_limit_bytes=48 << 20),
        cost_estimate=pl.CostEstimate(flops=8 * heads * rows * total_keys * head_dim, bytes_accessed=2 * width * (2 * total_keys + 2 * rows), transcendentals=heads * rows * total_keys),
        name=f"attend_{chunk}",
    )(s_len, queries, *keys, *values, token)


def output_kernel(size, heads, extra, aliased, where_ref, *refs):
    sources, refs = refs[:2 * size - 1], refs[2 * size - 1:]
    w_refs, refs = refs[:heads], refs[heads:]
    x_ref, gain_ref, refs = refs[0], refs[1], refs[2:]
    if extra:
        context_x_ref, x_x_ref, refs = refs[0], refs[1], refs[2:]
    refs = refs[1:]
    if aliased:
        refs = refs[2:]
    normed_ref, hidden_ref, refs = refs[0], refs[1], refs[2:]
    if extra:
        hidden_x_ref, refs = refs[0], refs[1:]
    token_ref, full_ref, square_ref = refs
    rows = sources[0].shape[0]
    head_dim, block = w_refs[0].shape[1:]
    depth = hidden_ref.shape[1]
    step = pl.program_id(0)

    @pl.when(step == 0)
    def _():
        square_ref[...] = jnp.zeros_like(square_ref)
        token_ref[...] = jnp.zeros_like(token_ref)
        for place in range(size):
            @pl.when(where_ref[0] == place)
            def _():
                for r in range(heads):
                    columns = pl.ds(pl.multiple_of(lax.bitwise_xor(where_ref[1], r) * head_dim, head_dim), head_dim)
                    for t in range(size):
                        there = (r * size + t) * head_dim
                        full_ref[:rows, there:there + head_dim] = sources[t - place + size - 1][:, columns]
        if extra:
            for r in range(heads):
                columns = pl.ds(pl.multiple_of(lax.bitwise_xor(where_ref[1], r) * head_dim, head_dim), head_dim)
                for t in range(size):
                    there = (r * size + t) * head_dim
                    full_ref[rows:, there:there + head_dim] = context_x_ref[t, :, columns]

    w_block = jnp.concatenate([w_ref[...].reshape(size * head_dim, block) for w_ref in w_refs], axis=0)
    acc = jnp.dot(full_ref[...], w_block, preferred_element_type=jnp.float32)
    columns = pl.ds(pl.multiple_of(step * block, block), block)
    hidden = (x_ref[...].astype(jnp.float32) + acc[:rows]).astype(jnp.bfloat16)
    hidden_ref[:, columns] = hidden
    hidden_f32 = hidden.astype(jnp.float32)
    square_ref[:rows] += jnp.sum(hidden_f32 * hidden_f32, axis=-1, keepdims=True)
    if extra:
        hidden = (x_x_ref[...].astype(jnp.float32) + acc[rows:]).astype(jnp.bfloat16)
        hidden_x_ref[:, columns] = hidden
        hidden_f32 = hidden.astype(jnp.float32)
        square_ref[rows:] += jnp.sum(hidden_f32 * hidden_f32, axis=-1, keepdims=True)

    @pl.when(step == pl.num_programs(0) - 1)
    def _():
        half = rows // 2
        inv_rms = lax.rsqrt(square_ref[...] / depth + NORM_EPS)
        for start in range(0, depth, block):
            gain = gain_ref[:, start:start + block].astype(jnp.float32)
            for part in range(2):
                lo, hi = part * half, (part + 1) * half
                normed_ref[part, :half, start:start + block] = (hidden_ref[lo:hi, start:start + block].astype(jnp.float32) * inv_rms[lo:hi] * gain).astype(jnp.bfloat16)
                if extra and part == 1:
                    normed_ref[part, half:, start:start + block] = (hidden_x_ref[:, start:start + block].astype(jnp.float32) * inv_rms[rows:] * gain).astype(jnp.bfloat16)
                else:
                    normed_ref[part, half:, start:start + block] = jnp.zeros((normed_ref.shape[1] - half, block), jnp.bfloat16)


def project_out(chunk, chunks, pad, token, where, sources, w_heads, x, gain, extras, buffers):
    rows, width = sources[0].shape
    depth = x.shape[1]
    heads = len(w_heads)
    size, head_dim = w_heads[0].shape[:2]
    block = min(512, depth)
    total = rows + (pad if extras else 0)
    whole = lambda shape: pl.BlockSpec(shape, lambda n, where: (0,) * len(shape), pipeline_mode=pl.Buffered(1))
    in_specs = [whole((rows, width))] * (2 * size - 1)
    in_specs += [pl.BlockSpec((size, head_dim, block), lambda n, where: (0, 0, n))] * heads
    in_specs += [pl.BlockSpec((rows, block), lambda n, where: (chunk, n)), whole((1, depth))]
    out_shape = [jax.ShapeDtypeStruct((2 * chunks, rows // 2 + pad, depth), jnp.bfloat16), jax.ShapeDtypeStruct((rows * chunks, depth), jnp.bfloat16)]
    out_specs = [
        pl.BlockSpec((2, rows // 2 + pad, depth), lambda n, where: (chunk, 0, 0), pipeline_mode=pl.Buffered(1)),
        pl.BlockSpec((rows, depth), lambda n, where: (chunk, 0), pipeline_mode=pl.Buffered(1)),
    ]
    if extras:
        in_specs += [whole(extras[0].shape), pl.BlockSpec((pad, block), lambda n, where: (0, n))]
        out_shape.append(jax.ShapeDtypeStruct((pad, depth), jnp.bfloat16))
        out_specs.append(whole((pad, depth)))
    in_specs.append(pl.BlockSpec(memory_space=pl.ANY))
    out_shape.append(TOKEN)
    out_specs.append(whole(TOKEN.shape))
    aliases = {}
    if buffers:
        aliases = {1 + len(in_specs): 0, 2 + len(in_specs): 1}
        in_specs += [pl.BlockSpec(memory_space=pl.ANY)] * 2
    return pl.pallas_call(
        functools.partial(output_kernel, size, heads, bool(extras), bool(buffers)),
        out_shape=out_shape,
        grid_spec=pltpu.PrefetchScalarGridSpec(
            num_scalar_prefetch=1,
            grid=(depth // block,),
            in_specs=in_specs,
            out_specs=out_specs,
            scratch_shapes=[pltpu.VMEM((total, size * width), jnp.bfloat16), pltpu.VMEM((total, 1), jnp.float32)],
        ),
        input_output_aliases=aliases,
        compiler_params=pltpu.CompilerParams(dimension_semantics=("arbitrary",), vmem_limit_bytes=60 << 20),
        cost_estimate=pl.CostEstimate(flops=2 * total * size * width * depth, bytes_accessed=2 * (size * width * depth + 7 * rows * width + 3 * total * depth), transcendentals=0),
        name="project_out",
    )(where, *sources, *w_heads, x, gain, *extras, token, *buffers)


def mlp_kernel(size, chunk_rows, extra, ff_steps, slots, token_ref, normed_ref, hextra_ref, wgu_ref, wd_ref, h_ref, out_ref, y_ref,
               acc, landed, outgoing, finished, residual, others,
               rs_send, rs_recv, ag_send, ag_recv, keep_sem, h_sem, x_send, x_recv, credit):
    step = pl.program_id(0)
    me = lax.axis_index('tp')
    depth = wd_ref.shape[1]
    chunks = (out_ref.shape[0] // chunk_rows)
    piece = outgoing.shape[2]
    per_chunk = chunk_rows // (2 * piece)
    pieces = chunks * per_chunk
    slot = step - ff_steps
    last = size - 1

    @pl.when(step == 0)
    def _():
        barrier = pltpu.get_barrier_semaphore()
        for d in range(1, size):
            pl.semaphore_signal(barrier, inc=1, device_id={'tp': lax.rem(me + d, size)}, device_id_type=pl.DeviceIdType.MESH)
        pl.semaphore_wait(barrier, size - 1)

    def own_part(chain, m):
        start = pl.multiple_of(chain * (chunk_rows // 2) + lax.rem(m, per_chunk) * piece, piece)
        return acc.at[lax.rem(lax.div(m, per_chunk), 3), pl.ds(start, piece)]

    def out_rows(chain, m):
        start = pl.multiple_of(lax.div(m, per_chunk) * chunk_rows + chain * (chunk_rows // 2) + lax.rem(m, per_chunk) * piece, piece)
        return pl.ds(start, piece)

    for chain in range(2):
        place = me if chain == 0 else last - me
        nearer = me - 1 if chain == 0 else me + 1
        farther = me + 1 if chain == 0 else me - 1

        def sum_copy(source, m):
            return pltpu.make_async_remote_copy(
                src_ref=source, dst_ref=landed.at[chain, lax.rem(m, slots)], send_sem=rs_send.at[chain, lax.rem(m, 4)],
                recv_sem=rs_recv.at[chain, lax.rem(m, slots)], device_id={'tp': nearer}, device_id_type=pl.DeviceIdType.MESH)

        def keep_copy(m):
            return pltpu.make_async_copy(finished.at[chain, lax.rem(m, 2)], out_ref.at[out_rows(chain, m)], keep_sem.at[chain, lax.rem(m, 2)])

        def h_copy(m):
            return pltpu.make_async_copy(h_ref.at[out_rows(chain, m)], residual.at[chain, lax.rem(m, 2)], h_sem.at[chain, lax.rem(m, 2)])

        def back_copy(source, m):
            return pltpu.make_async_remote_copy(
                src_ref=source, dst_ref=out_ref.at[out_rows(chain, m)], send_sem=ag_send.at[chain, lax.rem(m, 4)],
                recv_sem=ag_recv.at[chain, lax.rem(m, 8)], device_id={'tp': farther}, device_id_type=pl.DeviceIdType.MESH)

        @pl.when((place == last) & (slot >= 0) & (slot < pieces))
        def _():
            @pl.when(slot >= 4)
            def _():
                sum_copy(own_part(chain, slot - 4), slot - 4).wait_send()

            @pl.when(slot >= slots)
            def _():
                pl.semaphore_wait(credit.at[chain], 1)
            sum_copy(own_part(chain, slot), slot).start()

        for hops in range(1, last):
            m = slot - (last - hops)

            @pl.when((place == hops) & (m >= 0) & (m < pieces))
            def _():
                @pl.when(m >= 2)
                def _():
                    sum_copy(outgoing.at[chain, lax.rem(m, 2)], m - 2).wait_send()
                sum_copy(outgoing.at[chain, lax.rem(m, 2)], m).wait_recv()
                outgoing[chain, lax.rem(m, 2)] = landed[chain, lax.rem(m, slots)] + own_part(chain, m)[...]

                @pl.when(m + slots < pieces)
                def _():
                    pl.semaphore_signal(credit.at[chain], inc=1, device_id={'tp': farther}, device_id_type=pl.DeviceIdType.MESH)

                @pl.when(m >= slots)
                def _():
                    pl.semaphore_wait(credit.at[chain], 1)
                sum_copy(outgoing.at[chain, lax.rem(m, 2)], m).start()

        m = slot - last

        @pl.when((place == 0) & (slot == 0))
        def _():
            h_copy(0).start()

        @pl.when((place == 0) & (m >= 0) & (m < pieces))
        def _():
            @pl.when(m + 1 < pieces)
            def _():
                h_copy(m + 1).start()

            @pl.when(m >= 2)
            def _():
                keep_copy(m - 2).wait()
                back_copy(finished.at[chain, lax.rem(m, 2)], m - 2).wait_send()
            h_copy(m).wait()
            sum_copy(outgoing.at[chain, lax.rem(m, 2)], m).wait_recv()
            total = landed[chain, lax.rem(m, slots)] + own_part(chain, m)[...]
            finished[chain, lax.rem(m, 2)] = (residual[chain, lax.rem(m, 2)].astype(jnp.float32) + total).astype(jnp.bfloat16)

            @pl.when(m + slots < pieces)
            def _():
                pl.semaphore_signal(credit.at[chain], inc=1, device_id={'tp': farther}, device_id_type=pl.DeviceIdType.MESH)
            keep_copy(m).start()
            back_copy(finished.at[chain, lax.rem(m, 2)], m).start()

    for chain in range(2):
        place = me if chain == 0 else last - me
        farther = me + 1 if chain == 0 else me - 1

        def relay_copy(m):
            return pltpu.make_async_remote_copy(
                src_ref=out_ref.at[out_rows(chain, m)], dst_ref=out_ref.at[out_rows(chain, m)], send_sem=ag_send.at[chain, lax.rem(m, 4)],
                recv_sem=ag_recv.at[chain, lax.rem(m, 8)], device_id={'tp': farther}, device_id_type=pl.DeviceIdType.MESH)

        for hops in range(1, size):
            m = slot - last - 2 * hops

            @pl.when((place == hops) & (m >= 0) & (m < pieces))
            def _():
                relay_copy(m).wait_recv()
                if hops < last:
                    @pl.when(m >= 4)
                    def _():
                        relay_copy(m - 4).wait_send()
                    relay_copy(m).start()

    def extra_copy(d):
        return pltpu.make_async_remote_copy(
            src_ref=acc.at[(chunks - 1) % 3, pl.ds(chunk_rows, others.shape[1])], dst_ref=others.at[d], send_sem=x_send.at[d - 1],
            recv_sem=x_recv.at[d - 1], device_id={'tp': lax.rem(me + d, size)}, device_id_type=pl.DeviceIdType.MESH)

    @pl.when(step == chunks * ff_steps)
    def _():
        others[0] = acc[(chunks - 1) % 3, chunk_rows:chunk_rows + others.shape[1]]
        for d in range(1, size):
            extra_copy(d).start()

    @pl.when(step == chunks * ff_steps + 4)
    def _():
        for d in range(1, size):
            extra_copy(d).wait()
        total = others[lax.rem(me, size)]
        for j in range(1, size):
            total = total + others[lax.rem(me + size - j, size)]
        y_ref[...] = (hextra_ref[:others.shape[1]].astype(jnp.float32) + total).astype(jnp.bfloat16)

    @pl.when(step < chunks * ff_steps)
    def _():
        chunk = lax.div(step, ff_steps)
        rows_in = normed_ref[0]
        dims = (((1,), (1,)), ((), ()))
        gate = lax.dot_general(rows_in, wgu_ref[0], dims, preferred_element_type=jnp.float32)
        up = lax.dot_general(rows_in, wgu_ref[1], dims, preferred_element_type=jnp.float32)
        activated = (gate * jax.nn.sigmoid(gate) * up).astype(jnp.bfloat16)
        block = min(1024, depth)
        first = lax.rem(step, ff_steps) == 0
        for start in range(0, depth, block):
            part = jnp.dot(activated, wd_ref[:, start:start + block], preferred_element_type=jnp.float32)

            @pl.when(first)
            def _():
                acc[lax.rem(chunk, 3), :, start:start + block] = part

            @pl.when(jnp.logical_not(first))
            def _():
                acc[lax.rem(chunk, 3), :, start:start + block] += part

    @pl.when(step == pl.num_programs(0) - 1)
    def _():
        for chain in range(2):
            place = me if chain == 0 else last - me
            nearer = me - 1 if chain == 0 else me + 1
            farther = me + 1 if chain == 0 else me - 1

            def sent(m):
                return pltpu.make_async_remote_copy(
                    src_ref=outgoing.at[chain, m % 2], dst_ref=landed.at[chain, m % slots], send_sem=rs_send.at[chain, m % 4],
                    recv_sem=rs_recv.at[chain, m % slots], device_id={'tp': nearer}, device_id_type=pl.DeviceIdType.MESH)

            def returned(m):
                return pltpu.make_async_remote_copy(
                    src_ref=finished.at[chain, m % 2], dst_ref=out_ref.at[pl.ds(0, piece)], send_sem=ag_send.at[chain, m % 4],
                    recv_sem=ag_recv.at[chain, m % 8], device_id={'tp': farther}, device_id_type=pl.DeviceIdType.MESH)

            @pl.when(place == last)
            def _():
                for m in range(pieces - 4, pieces):
                    sent(m).wait_send()

            @pl.when((place > 0) & (place < last))
            def _():
                for m in range(pieces - 2, pieces):
                    sent(m).wait_send()
                for m in range(pieces - 4, pieces):
                    returned(m).wait_send()

            @pl.when(place == 0)
            def _():
                for m in range(pieces - 2, pieces):
                    pltpu.make_async_copy(finished.at[chain, m % 2], out_ref.at[pl.ds(0, piece)], keep_sem.at[chain, m % 2]).wait()
                    returned(m).wait_send()


def mlp(token, normed, hextra, w_gate_up, w_down, hidden, size):
    chunks, lines, depth = normed.shape
    rows = hidden.shape[0]
    chunk_rows = rows // chunks
    ff = w_down.shape[0]
    ff_steps = 4
    piece = chunk_rows // 8
    slots = 4
    pieces = chunks * 4
    extra = lines - chunk_rows
    seen = min(8, extra)
    steps = chunks * ff_steps
    total_steps = ff_steps + pieces + (size - 1) + 2 * (size - 1)
    ff_block = ff // ff_steps
    at_ff = lambda g: lax.select(g < steps, lax.rem(g, ff_steps), ff_steps - 1)
    at_chunk = lambda g: lax.min(lax.div(g, ff_steps), chunks - 1)
    f32, bf16 = jnp.float32, jnp.bfloat16
    return pl.pallas_call(
        functools.partial(mlp_kernel, size, chunk_rows, extra, ff_steps, slots),
        out_shape=[jax.ShapeDtypeStruct((rows, depth), bf16), jax.ShapeDtypeStruct((seen, depth), bf16)],
        grid=(total_steps,),
        in_specs=[
            pl.BlockSpec(memory_space=pl.ANY),
            pl.BlockSpec((1, lines, depth), lambda g: (at_chunk(g), 0, 0)),
            pl.BlockSpec((extra, depth), lambda g: (0, 0), pipeline_mode=pl.Buffered(1)),
            pl.BlockSpec((2, ff_block, depth), lambda g: (0, at_ff(g), 0)),
            pl.BlockSpec((ff_block, depth), lambda g: (at_ff(g), 0)),
            pl.BlockSpec(memory_space=pl.ANY),
        ],
        out_specs=[pl.BlockSpec(memory_space=pl.ANY), pl.BlockSpec((seen, depth), lambda g: (0, 0), pipeline_mode=pl.Buffered(1))],
        scratch_shapes=[
            pltpu.VMEM((3, lines, depth), f32),
            pltpu.VMEM((2, slots, piece, depth), f32),
            pltpu.VMEM((2, 2, piece, depth), f32),
            pltpu.VMEM((2, 2, piece, depth), bf16),
            pltpu.VMEM((2, 2, piece, depth), bf16),
            pltpu.VMEM((size, seen, depth), f32),
            pltpu.SemaphoreType.DMA((2, 4)),
            pltpu.SemaphoreType.DMA((2, slots)),
            pltpu.SemaphoreType.DMA((2, 4)),
            pltpu.SemaphoreType.DMA((2, 8)),
            pltpu.SemaphoreType.DMA((2, 2)),
            pltpu.SemaphoreType.DMA((2, 2)),
            pltpu.SemaphoreType.DMA((size - 1,)),
            pltpu.SemaphoreType.DMA((size - 1,)),
            pltpu.SemaphoreType.REGULAR((2,)),
        ],
        compiler_params=pltpu.CompilerParams(dimension_semantics=("arbitrary",), vmem_limit_bytes=63 << 20, collective_id=0, has_side_effects=True),
        cost_estimate=pl.CostEstimate(flops=6 * rows * depth * ff, bytes_accessed=6 * chunks * depth * ff, transcendentals=rows * ff),
        name="mlp",
    )(token, normed, hextra, w_gate_up, w_down, hidden)


def pick_by(index, options):
    result = options[0]
    for place in range(1, len(options)):
        result = jnp.where(index == place, options[place], result)
    return result


def solution(mesh):
    side_size = mesh.shape['side']
    tp_size = mesh.shape['tp']
    seats = mesh.shape['pair'] * side_size
    group_axes = ('pair', 'side')
    last = tp_size - 1

    def cyclic(value, d):
        return lax.ppermute(value, 'tp', [(t, (t + d) % tp_size) for t in range(tp_size)])

    def swap(value, mask):
        return lax.ppermute(value, group_axes, [(q, q ^ mask) for q in range(seats)])

    def in_order(me, copies):
        return [pick_by(me, [copies[(t - j) % tp_size] for t in range(tp_size)]) for j in range(tp_size)]

    def device_fn(x_prompt, s_len, y_tok, c_len, k_cache, v_cache, attn_gain, w_qkv, w_out, mlp_gain, w_gate_up, w_down):
        me = lax.axis_index('tp')
        seat = lax.axis_index('pair') * side_size + lax.axis_index('side')
        where = jnp.stack([me, seat]).astype(jnp.int32)
        seq_len, depth = x_prompt.shape[1:]
        heads_local = w_qkv.shape[2]
        head_dim = w_qkv.shape[4]
        width = heads_local * head_dim
        rows = seq_len // tp_size
        decodes = y_tok.shape[0]
        pad = 16
        cache_local = k_cache.shape[2]
        up_pairs = [(t, t + 1) for t in range(last)]
        down_pairs = [(t + 1, t) for t in range(last)]
        val = {}

        def tie(keys):
            keys = list(dict.fromkeys(keys))
            for key, value in zip(keys, lax.optimization_barrier(tuple(val[key] for key in keys))):
                val[key] = value

        val['w', 0] = lax.all_gather(lax.dynamic_index_in_dim(w_out[0, :, 0], seat, 0, keepdims=False), 'tp', axis=0, tiled=False)

        val['w_all'] = jnp.swapaxes(w_qkv[0], 1, 2).reshape(depth, 3 * width)
        tables = rope_tables(jnp.arange(seq_len, dtype=jnp.int32), head_dim)
        extra_tables = rope_tables(jnp.concatenate([c_len, jnp.zeros((pad - decodes,), jnp.int32)]), head_dim)
        y_pad = jnp.concatenate([y_tok, jnp.zeros((pad - decodes, depth), y_tok.dtype)])
        val['gain'], val['s_len'], val['mlp_gain'] = attn_gain, s_len, mlp_gain
        val['valid'] = (jnp.arange(seq_len) < s_len[0]).astype(jnp.bfloat16)
        for which in range(2):
            val['cache', which] = jnp.zeros((rows, tp_size, heads_local, head_dim), jnp.bfloat16)
        buffers = []
        qkv = []

        def compute(name):
            kind = name[0]
            c = int(name[1:]) if name[1:].isdigit() else 0
            if kind == 'Q':
                tie(thread + ['gain'])
                *made, val['token'] = project_qkv(c, rows, val['token'], x_prompt[0], y_pad if c == 0 else None, val['gain'], val['w_all'], tables, extra_tables, head_dim)
                qkv.append(made)
                if c == 0:
                    val['dq', 0] = jnp.stack([part[rows:rows + decodes].reshape(decodes, heads_local, head_dim) for part in made])
                    for d in range(1, tp_size):
                        val['dq', d] = cyclic(val['dq', 0], d)
                return ['token']
            if kind == 'T':
                tie(thread + ['s_len'])
                context, val['token'] = attend(c, tp_size, rows, val['token'], val['s_len'], qkv[c][0], [part[1] for part in qkv], [part[2] for part in qkv], head_dim)
                val['L', c, 0] = val['R', c, 0] = context
                val['L', c, 1] = lax.ppermute(context, 'tp', up_pairs)
                val['R', c, 1] = lax.ppermute(context, 'tp', down_pairs)
                return ['token']
            if kind == 'K':
                tie(thread + ['valid'])
                for d in range(tp_size):
                    for which in range(2):
                        rows_d = pick_by(me, [qkv[(t + d) % tp_size][which + 1][:rows].reshape(rows, heads_local, head_dim) for t in range(tp_size)])
                        keep = pick_by(me, [val['valid'][((t + d) % tp_size) * rows:((t + d) % tp_size + 1) * rows] for t in range(tp_size)])
                        val['kv', d, which] = rows_d * keep[:, None, None]
                return []
            if name == 'D1':
                tie(thread + [('dq', d) for d in range(tp_size)])
                dec_full = jnp.concatenate(in_order(me, [val['dq', d] for d in range(tp_size)]), axis=2)
                cache_pos = me * cache_local + jnp.arange(cache_local)
                write_mask = (cache_pos[None, :] == c_len[:, None])[:, :, None, None]
                allowed = (cache_pos[None, :] <= c_len[:, None])[:, None, :]
                key_now = jnp.where(write_mask, dec_full[1][:, None], k_cache[0])
                value_now = jnp.where(write_mask, dec_full[2][:, None], v_cache[0])
                val['key_now'], val['value_now'] = key_now, value_now
                scores = jnp.einsum('bkh,btkh->bkt', dec_full[0], key_now, preferred_element_type=jnp.float32) * head_dim ** -0.5
                scores = jnp.where(allowed, scores, -1e30)
                peak = jnp.max(scores, axis=-1, keepdims=True)
                weights = jnp.exp(scores - peak)
                total = jnp.sum(weights, axis=-1, keepdims=True)
                mixed = jnp.einsum('bkt,btkh->bkh', weights.astype(jnp.bfloat16), value_now, preferred_element_type=jnp.float32)
                packed = jnp.stack([mixed, jnp.broadcast_to(peak, mixed.shape), jnp.broadcast_to(total, mixed.shape)])
                packed = packed.reshape(3, decodes, tp_size, heads_local, head_dim)
                for d in range(tp_size):
                    share = lax.dynamic_index_in_dim(packed, lax.rem(me + d, tp_size), 2, keepdims=False)
                    val['ds', d] = share if d == 0 else cyclic(share, d)
                return [('ds', 0)]
            if name == 'D2':
                tie(thread + [('ds', d) for d in range(tp_size)])
                shares = [val['ds', d] for d in range(tp_size)]
                top = functools.reduce(jnp.maximum, [share[1] for share in shares])
                factors = [jnp.exp(share[1] - top) for share in shares]
                dec_mixed = sum(share[0] * factor for share, factor in zip(shares, factors))
                dec_total = sum(share[2] * factor for share, factor in zip(shares, factors))
                val['dc', 0] = (dec_mixed / dec_total).astype(jnp.bfloat16).reshape(decodes, width)
                for d in range(1, tp_size):
                    val['dc', d] = cyclic(val['dc', 0], d)
                return [('dc', 0)]
            if kind == 'O':
                source_keys = [('L', c, d) for d in range(last, 0, -1)] + [('L', c, 0)] + [('R', c, d) for d in range(1, tp_size)]
                w_keys = [('w', r) for r in range(seats)]
                extra_keys = [('dc', d) for d in range(tp_size)] if c == last else []
                tie(thread + ['mlp_gain'] + source_keys + extra_keys + (w_keys if c == 0 else []))
                extras = []
                if c == last:
                    extras = [jnp.pad(jnp.stack(in_order(me, [val[key] for key in extra_keys])), ((0, 0), (0, pad - decodes), (0, 0))), y_pad]
                made = project_out(c, tp_size, pad, val['token'], where, [val[key] for key in source_keys], [val[key] for key in w_keys], x_prompt[0], val['mlp_gain'], extras, [val[key] for key in buffers])
                buffers[:] = ['normed', 'h']
                val['normed'], val['h'], val['token'] = made[0], made[1], made[-1]
                if c == last:
                    val['hx'] = made[2]
                return ['token']
            val['out'], val['y'] = mlp(val['token'], val['normed'], val['hx'], jnp.transpose(w_gate_up[0], (1, 2, 0)), w_down[0], val['h'], tp_size)
            return ['y']

        def transfer(name):
            kind = name[0]
            if kind == 'c':
                c, step = map(int, name[1:].split('.'))
                tie(thread + [('L', c, step - 1), ('R', c, step - 1)])
                val['L', c, step] = lax.ppermute(val['L', c, step - 1], 'tp', [(a, b) for a, b in up_pairs if a >= step - 1])
                val['R', c, step] = lax.ppermute(val['R', c, step - 1], 'tp', [(a, b) for a, b in down_pairs if a <= last - step + 1])
            elif kind == 'w':
                bases = [0] if name == 'w2' else list(range(0, seats, 2))
                tie(thread + [('w', base) for base in bases])
                for mask in (range(2, seats, 2) if name == 'w2' else [1]):
                    for base in bases:
                        val['w', base ^ mask] = swap(val['w', base], mask)
            elif kind == 'k':
                d, which = int(name[1]), 'kv'.index(name[2])
                tie(thread + [('kv', d, which)])
                route = [(t * side_size + s, ((t + d) % tp_size) * side_size + (s + 1) % side_size) for t in range(tp_size) for s in range(side_size)]
                val['landed', d, which] = lax.ppermute(val['kv', d, which], ('tp', 'side'), route)
            else:
                d, which = int(name[1]), 'kv'.index(name[2])
                tie(thread + [('landed', d, which), ('cache', which)])
                val['cache', which] = lax.dynamic_update_slice(val['cache', which], val['landed', d, which][:, None], (0, lax.rem(me - d + tp_size, tp_size), 0, 0))

        val['token'] = jnp.zeros(TOKEN.shape, TOKEN.dtype)
        thread = ['token']
        for name in ORDER:
            if name[0] in 'QTKDOB':
                made = compute(name)
                thread = thread + made if name in ('K', 'D1', 'D2') else made
            else:
                transfer(name)

        caches = [val['cache', which].reshape(1, 1, rows, tp_size * heads_local, head_dim) for which in range(2)]
        return (val['out'][None], val['y'][:decodes], caches[0], caches[1], val['key_now'][None], val['value_now'][None])

    cache_spec = P(None, group_axes, 'tp', None, None)
    in_specs = (P(group_axes, None, None), P(group_axes), P(group_axes, None), P(group_axes), cache_spec, cache_spec, P(), P(None, None, 'tp', None, None), P(None, 'tp', None, None, None), P(), P(None, None, None, 'tp'), P(None, 'tp', None))
    out_specs = (P(group_axes, None, None), P(group_axes, None), cache_spec, cache_spec, cache_spec, cache_spec)
    return jax.shard_map(device_fn, mesh=mesh, in_specs=in_specs, out_specs=out_specs, check_vma=False)
```

```python
import functools

import jax
import jax.numpy as jnp
from jax import lax
from jax.experimental import pallas as pl
from jax.experimental.pallas import tpu as pltpu
from jax.sharding import PartitionSpec as P

ROPE_BASE = 10000.0
NORM_EPS = 1e-5

ORDER = ('Q0', 'T0', 'Q1', 'T1', 'w2', 'Q2', 'T2', 'Q3', 'T3', 'D1', 'K', 'D2', 'w3', 'O0', 'O1', 'O2', 'O3', 'B')


def rms_scale(values_f32, gain_f32):
    inv_rms = lax.rsqrt(jnp.mean(values_f32 * values_f32, axis=-1, keepdims=True) + NORM_EPS)
    return (values_f32 * inv_rms * gain_f32).astype(jnp.bfloat16)


def rope_tables(positions, head_dim):
    half_dim = head_dim // 2
    inv_freq = ROPE_BASE ** (-2.0 * jnp.arange(half_dim, dtype=jnp.float32) / head_dim)
    angles = positions.astype(jnp.float32)[:, None] * inv_freq[None, :]
    cos_table = jnp.cos(angles)
    sin_table = jnp.sin(angles)
    return jnp.concatenate([cos_table, cos_table], axis=1), jnp.concatenate([-sin_table, sin_table], axis=1)


def qkv_kernel(head_dim, extra, *refs):
    x_ref, gain_ref, wq_ref, wk_ref, wv_ref, cos_ref, sin_ref = refs[:7]
    extra_refs = refs[7:10] if extra else None
    q_ref, k_ref, v_ref, token_ref, normed_ref = refs[-5:]
    rows = x_ref.shape[0]

    @pl.when(pl.program_id(0) == 0)
    def _():
        gain = gain_ref[...].astype(jnp.float32)
        normed_ref[:rows] = rms_scale(x_ref[...].astype(jnp.float32), gain)
        if extra:
            normed_ref[rows:] = rms_scale(extra_refs[0][...].astype(jnp.float32), gain)
        token_ref[...] = jnp.zeros_like(token_ref)

    cos, sin = cos_ref[...], sin_ref[...]
    if extra:
        cos = jnp.concatenate([cos, extra_refs[1][...]], axis=0)
        sin = jnp.concatenate([sin, extra_refs[2][...]], axis=0)
    for w_ref, out_ref in ((wq_ref, q_ref), (wk_ref, k_ref), (wv_ref, v_ref)):
        acc = jnp.dot(normed_ref[...], w_ref[...], preferred_element_type=jnp.float32)
        for start in range(0, acc.shape[1], head_dim):
            vals = acc[:, start:start + head_dim]
            if out_ref is not v_ref:
                vals = vals * cos + pltpu.roll(vals, head_dim // 2, 1) * sin
            out_ref[:, start:start + head_dim] = vals.astype(out_ref.dtype)


TOKEN = jax.ShapeDtypeStruct((8, 128), jnp.float32)


def project_qkv(chunk, rows, token, x, extra_rows, gain, w_all, tables, extra_tables, head_dim):
    depth = x.shape[1]
    width = w_all.shape[1] // 3
    block = 2 * head_dim
    steps = width // block
    extras = [] if extra_rows is None else [extra_rows, *extra_tables]
    total = rows + (0 if extra_rows is None else extra_rows.shape[0])
    whole = lambda shape: pl.BlockSpec(shape, lambda n: (0, 0), pipeline_mode=pl.Buffered(1))
    columns = lambda part: pl.BlockSpec((depth, block), lambda n: (0, part * steps + n))
    return pl.pallas_call(
        functools.partial(qkv_kernel, head_dim, extra_rows is not None),
        out_shape=[jax.ShapeDtypeStruct((total, width), jnp.bfloat16)] * 3 + [TOKEN],
        grid=(steps,),
        in_specs=[
            pl.BlockSpec((rows, depth), lambda n: (chunk, 0), pipeline_mode=pl.Buffered(1)),
            whole((1, depth)),
            columns(0),
            columns(1),
            columns(2),
            pl.BlockSpec((rows, head_dim), lambda n: (chunk, 0), pipeline_mode=pl.Buffered(1)),
            pl.BlockSpec((rows, head_dim), lambda n: (chunk, 0), pipeline_mode=pl.Buffered(1)),
        ] + [whole(e.shape) for e in extras] + [pl.BlockSpec(memory_space=pl.ANY)],
        out_specs=[pl.BlockSpec((total, block), lambda n: (0, n))] * 3 + [whole(TOKEN.shape)],
        scratch_shapes=[pltpu.VMEM((total, depth), jnp.bfloat16)],
        compiler_params=pltpu.CompilerParams(dimension_semantics=("arbitrary",), vmem_limit_bytes=48 << 20),
        cost_estimate=pl.CostEstimate(flops=6 * total * depth * width, bytes_accessed=2 * (total * depth + 3 * depth * width + 3 * total * width), transcendentals=0),
        name="project_qkv",
    )(x, gain, w_all, w_all, w_all, *tables, *extras, token)


def attend_kernel(chunk, first_checked, q_rows, slen_ref, *refs):
    q_ref = refs[0]
    k_refs = refs[1:chunk + 2]
    v_refs = refs[chunk + 2:2 * chunk + 3]
    out_ref, token_ref = refs[-2:]
    token_ref[...] = jnp.zeros_like(token_ref)
    rows, head_dim = q_ref.shape
    scale = head_dim ** -0.5
    limit = slen_ref[0]
    for start in range(0, rows, q_rows):
        query = q_ref[start:start + q_rows, :]
        scores = []
        values = []
        for part in range(chunk + 1):
            keys = rows if part < chunk else start + q_rows
            score = lax.dot_general(query, k_refs[part][:keys, :], (((1,), (1,)), ((), ())), preferred_element_type=jnp.float32) * scale
            key_pos = lax.broadcasted_iota(jnp.int32, score.shape, 1)
            if part == chunk:
                allowed = key_pos <= lax.broadcasted_iota(jnp.int32, score.shape, 0) + start
                if part >= first_checked:
                    allowed = allowed & (key_pos < limit - part * rows)
                score = jnp.where(allowed, score, -1e30)
            elif part >= first_checked:
                score = jnp.where(key_pos < limit - part * rows, score, -1e30)
            scores.append(score)
            values.append(v_refs[part][:keys, :])
        peak = functools.reduce(jnp.maximum, [jnp.max(score, axis=-1, keepdims=True) for score in scores])
        total = jnp.zeros((q_rows, 1), jnp.float32)
        mixed = jnp.zeros((q_rows, head_dim), jnp.float32)
        for score, value in zip(scores, values):
            weight = jnp.exp(score - peak)
            total = total + jnp.sum(weight, axis=-1, keepdims=True)
            mixed = mixed + jnp.dot(weight.astype(jnp.bfloat16), value, preferred_element_type=jnp.float32)
        out_ref[start:start + q_rows, :] = (mixed / total).astype(out_ref.dtype)


def attend(chunk, chunks, rows, token, s_len, queries, keys, values, head_dim):
    width = queries.shape[1]
    heads = width // head_dim

    pick = pl.BlockSpec((rows, head_dim), lambda h, slen: (0, h))
    total_keys = rows * (chunk + 1)
    return pl.pallas_call(
        functools.partial(attend_kernel, chunk, chunks // 2, min(256, rows)),
        out_shape=[jax.ShapeDtypeStruct((rows, width), jnp.bfloat16), TOKEN],
        grid_spec=pltpu.PrefetchScalarGridSpec(
            num_scalar_prefetch=1,
            grid=(heads,),
            in_specs=[pick] * (2 * chunk + 3) + [pl.BlockSpec(memory_space=pl.ANY)],
            out_specs=[pick, pl.BlockSpec(TOKEN.shape, lambda h, slen: (0, 0))],
        ),
        compiler_params=pltpu.CompilerParams(dimension_semantics=("arbitrary",), vmem_limit_bytes=48 << 20),
        cost_estimate=pl.CostEstimate(flops=8 * heads * rows * total_keys * head_dim, bytes_accessed=2 * width * (2 * total_keys + 2 * rows), transcendentals=heads * rows * total_keys),
        name=f"attend_{chunk}",
    )(s_len, queries, *keys, *values, token)


def output_kernel(size, heads, extra, aliased, where_ref, *refs):
    context_ref, refs = refs[0], refs[1:]
    w_refs, refs = refs[:heads], refs[heads:]
    x_ref, gain_ref, refs = refs[0], refs[1], refs[2:]
    if extra:
        context_x_ref, x_x_ref, refs = refs[0], refs[1], refs[2:]
    refs = refs[1:]
    if aliased:
        refs = refs[2:]
    normed_ref, hidden_ref, refs = refs[0], refs[1], refs[2:]
    if extra:
        hidden_x_ref, refs = refs[0], refs[1:]
    token_ref, full_ref, square_ref = refs
    rows = context_ref.shape[1]
    head_dim, block = w_refs[0].shape[1:]
    depth = hidden_ref.shape[1]
    step = pl.program_id(0)

    @pl.when(step == 0)
    def _():
        square_ref[...] = jnp.zeros_like(square_ref)
        token_ref[...] = jnp.zeros_like(token_ref)
        for r in range(heads):
            columns = pl.ds(pl.multiple_of(lax.bitwise_xor(where_ref[0], r) * head_dim, head_dim), head_dim)
            for t in range(size):
                there = (r * size + t) * head_dim
                full_ref[:rows, there:there + head_dim] = context_ref[t, :, columns]
                if extra:
                    full_ref[rows:, there:there + head_dim] = context_x_ref[t, :, columns]

    w_block = jnp.concatenate([w_ref[...].reshape(size * head_dim, block) for w_ref in w_refs], axis=0)
    acc = jnp.dot(full_ref[...], w_block, preferred_element_type=jnp.float32)
    columns = pl.ds(pl.multiple_of(step * block, block), block)
    hidden = (x_ref[...].astype(jnp.float32) + acc[:rows]).astype(jnp.bfloat16)
    hidden_ref[:, columns] = hidden
    hidden_f32 = hidden.astype(jnp.float32)
    square_ref[:rows] += jnp.sum(hidden_f32 * hidden_f32, axis=-1, keepdims=True)
    if extra:
        hidden = (x_x_ref[...].astype(jnp.float32) + acc[rows:]).astype(jnp.bfloat16)
        hidden_x_ref[:, columns] = hidden
        hidden_f32 = hidden.astype(jnp.float32)
        square_ref[rows:] += jnp.sum(hidden_f32 * hidden_f32, axis=-1, keepdims=True)

    @pl.when(step == pl.num_programs(0) - 1)
    def _():
        half = rows // 2
        inv_rms = lax.rsqrt(square_ref[...] / depth + NORM_EPS)
        for start in range(0, depth, block):
            gain = gain_ref[:, start:start + block].astype(jnp.float32)
            for part in range(2):
                lo, hi = part * half, (part + 1) * half
                normed_ref[part, :half, start:start + block] = (hidden_ref[lo:hi, start:start + block].astype(jnp.float32) * inv_rms[lo:hi] * gain).astype(jnp.bfloat16)
                if extra and part == 1:
                    normed_ref[part, half:, start:start + block] = (hidden_x_ref[:, start:start + block].astype(jnp.float32) * inv_rms[rows:] * gain).astype(jnp.bfloat16)
                else:
                    normed_ref[part, half:, start:start + block] = jnp.zeros((normed_ref.shape[1] - half, block), jnp.bfloat16)


def project_out(chunk, chunks, pad, token, where, context, w_heads, x, gain, extras, buffers):
    rows, width = context.shape[1:]
    depth = x.shape[1]
    heads = len(w_heads)
    size, head_dim = w_heads[0].shape[:2]
    block = min(512, depth)
    total = rows + (pad if extras else 0)
    whole = lambda shape: pl.BlockSpec(shape, lambda n, where: (0,) * len(shape), pipeline_mode=pl.Buffered(1))
    in_specs = [whole(context.shape)]
    in_specs += [pl.BlockSpec((size, head_dim, block), lambda n, where: (0, 0, n))] * heads
    in_specs += [pl.BlockSpec((rows, block), lambda n, where: (chunk, n)), whole((1, depth))]
    out_shape = [jax.ShapeDtypeStruct((2 * chunks, rows // 2 + pad, depth), jnp.bfloat16), jax.ShapeDtypeStruct((rows * chunks, depth), jnp.bfloat16)]
    out_specs = [
        pl.BlockSpec((2, rows // 2 + pad, depth), lambda n, where: (chunk, 0, 0), pipeline_mode=pl.Buffered(1)),
        pl.BlockSpec((rows, depth), lambda n, where: (chunk, 0), pipeline_mode=pl.Buffered(1)),
    ]
    if extras:
        in_specs += [whole(extras[0].shape), pl.BlockSpec((pad, block), lambda n, where: (0, n))]
        out_shape.append(jax.ShapeDtypeStruct((pad, depth), jnp.bfloat16))
        out_specs.append(whole((pad, depth)))
    in_specs.append(pl.BlockSpec(memory_space=pl.ANY))
    out_shape.append(TOKEN)
    out_specs.append(whole(TOKEN.shape))
    aliases = {}
    if buffers:
        aliases = {1 + len(in_specs): 0, 2 + len(in_specs): 1}
        in_specs += [pl.BlockSpec(memory_space=pl.ANY)] * 2
    return pl.pallas_call(
        functools.partial(output_kernel, size, heads, bool(extras), bool(buffers)),
        out_shape=out_shape,
        grid_spec=pltpu.PrefetchScalarGridSpec(
            num_scalar_prefetch=1,
            grid=(depth // block,),
            in_specs=in_specs,
            out_specs=out_specs,
            scratch_shapes=[pltpu.VMEM((total, size * width), jnp.bfloat16), pltpu.VMEM((total, 1), jnp.float32)],
        ),
        input_output_aliases=aliases,
        compiler_params=pltpu.CompilerParams(dimension_semantics=("arbitrary",), vmem_limit_bytes=60 << 20),
        cost_estimate=pl.CostEstimate(flops=2 * total * size * width * depth, bytes_accessed=2 * (size * width * depth + 4 * rows * width + 3 * total * depth), transcendentals=0),
        name="project_out",
    )(where, context, *w_heads, x, gain, *extras, token, *buffers)


def mlp_kernel(size, sides, chunk_rows, extra, ff_steps, slots, token_ref, normed_ref, hextra_ref, wgu_ref, wd_ref, h_ref, kv_ref,
               out_ref, y_ref, k_ref, v_ref, acc, landed, outgoing, finished, residual, others,
               rs_send, rs_recv, ag_send, ag_recv, keep_sem, h_sem, x_send, x_recv, kv_send, kv_recv, credit):
    step = pl.program_id(0)
    me = lax.axis_index('tp')
    side = lax.axis_index('side')
    depth = wd_ref.shape[1]
    chunks = (out_ref.shape[0] // chunk_rows)
    piece = outgoing.shape[2]
    per_chunk = chunk_rows // (2 * piece)
    pieces = chunks * per_chunk
    slot = step - ff_steps
    last = size - 1

    @pl.when(step == 0)
    def _():
        barrier = pltpu.get_barrier_semaphore()
        for d in range(1, size):
            pl.semaphore_signal(barrier, inc=1, device_id={'tp': lax.rem(me + d, size)}, device_id_type=pl.DeviceIdType.MESH)
        for d in range(size):
            for turn in (1, sides - 1):
                pl.semaphore_signal(barrier, inc=1, device_id={'tp': lax.rem(me + d, size), 'side': lax.rem(side + turn, sides)}, device_id_type=pl.DeviceIdType.MESH)
        pl.semaphore_wait(barrier, 3 * size - 1)

    def own_part(chain, m):
        start = pl.multiple_of(chain * (chunk_rows // 2) + lax.rem(m, per_chunk) * piece, piece)
        return acc.at[lax.rem(lax.div(m, per_chunk), 3), pl.ds(start, piece)]

    def out_rows(chain, m):
        start = pl.multiple_of(lax.div(m, per_chunk) * chunk_rows + chain * (chunk_rows // 2) + lax.rem(m, per_chunk) * piece, piece)
        return pl.ds(start, piece)

    heads = kv_ref.shape[3]
    kv_rows = kv_ref.shape[2] // 32

    def kv_copy(d, which, rows):
        return pltpu.make_async_remote_copy(
            src_ref=kv_ref.at[d, which, rows], dst_ref=(k_ref, v_ref)[which].at[rows, pl.ds(pl.multiple_of(me * heads, heads), heads)],
            send_sem=kv_send.at[d, which], recv_sem=kv_recv.at[d, which],
            device_id={'tp': lax.rem(me + d, size), 'side': lax.rem(side + 1, sides)}, device_id_type=pl.DeviceIdType.MESH)

    def kv_start(first, count):
        for d in range(size):
            for which in range(2):
                kv_copy(d, which, pl.ds(pl.multiple_of(first, kv_rows), count)).start()

    @pl.when(step < KV_HEAD)
    def _():
        kv_start(step * KV_BULK * kv_rows, KV_BULK * kv_rows)

    @pl.when((step >= ff_steps) & (step < ff_steps + 32 - KV_HEAD * KV_BULK))
    def _():
        kv_start((step - ff_steps + KV_HEAD * KV_BULK) * kv_rows, kv_rows)

    for chain in range(2):
        place = me if chain == 0 else last - me
        nearer = me - 1 if chain == 0 else me + 1
        farther = me + 1 if chain == 0 else me - 1

        def sum_copy(source, m):
            return pltpu.make_async_remote_copy(
                src_ref=source, dst_ref=landed.at[chain, lax.rem(m, slots)], send_sem=rs_send.at[chain, lax.rem(m, 4)],
                recv_sem=rs_recv.at[chain, lax.rem(m, slots)], device_id={'tp': nearer}, device_id_type=pl.DeviceIdType.MESH)

        def keep_copy(m):
            return pltpu.make_async_copy(finished.at[chain, lax.rem(m, 2)], out_ref.at[out_rows(chain, m)], keep_sem.at[chain, lax.rem(m, 2)])

        def h_copy(m):
            return pltpu.make_async_copy(h_ref.at[out_rows(chain, m)], residual.at[chain, lax.rem(m, 2)], h_sem.at[chain, lax.rem(m, 2)])

        def back_copy(source, m):
            return pltpu.make_async_remote_copy(
                src_ref=source, dst_ref=out_ref.at[out_rows(chain, m)], send_sem=ag_send.at[chain, lax.rem(m, 4)],
                recv_sem=ag_recv.at[chain, lax.rem(m, 8)], device_id={'tp': farther}, device_id_type=pl.DeviceIdType.MESH)

        @pl.when((place == last) & (slot >= 0) & (slot < pieces))
        def _():
            @pl.when(slot >= 4)
            def _():
                sum_copy(own_part(chain, slot - 4), slot - 4).wait_send()

            @pl.when(slot >= slots)
            def _():
                pl.semaphore_wait(credit.at[chain], 1)
            sum_copy(own_part(chain, slot), slot).start()

        for hops in range(1, last):
            m = slot - (last - hops)

            @pl.when((place == hops) & (m >= 0) & (m < pieces))
            def _():
                @pl.when(m >= 2)
                def _():
                    sum_copy(outgoing.at[chain, lax.rem(m, 2)], m - 2).wait_send()
                sum_copy(outgoing.at[chain, lax.rem(m, 2)], m).wait_recv()
                outgoing[chain, lax.rem(m, 2)] = landed[chain, lax.rem(m, slots)] + own_part(chain, m)[...]

                @pl.when(m + slots < pieces)
                def _():
                    pl.semaphore_signal(credit.at[chain], inc=1, device_id={'tp': farther}, device_id_type=pl.DeviceIdType.MESH)

                @pl.when(m >= slots)
                def _():
                    pl.semaphore_wait(credit.at[chain], 1)
                sum_copy(outgoing.at[chain, lax.rem(m, 2)], m).start()

        m = slot - last

        @pl.when((place == 0) & (slot == 0))
        def _():
            h_copy(0).start()

        @pl.when((place == 0) & (m >= 0) & (m < pieces))
        def _():
            @pl.when(m + 1 < pieces)
            def _():
                h_copy(m + 1).start()

            @pl.when(m >= 2)
            def _():
                keep_copy(m - 2).wait()
                back_copy(finished.at[chain, lax.rem(m, 2)], m - 2).wait_send()
            h_copy(m).wait()
            sum_copy(outgoing.at[chain, lax.rem(m, 2)], m).wait_recv()
            total = landed[chain, lax.rem(m, slots)] + own_part(chain, m)[...]
            finished[chain, lax.rem(m, 2)] = (residual[chain, lax.rem(m, 2)].astype(jnp.float32) + total).astype(jnp.bfloat16)

            @pl.when(m + slots < pieces)
            def _():
                pl.semaphore_signal(credit.at[chain], inc=1, device_id={'tp': farther}, device_id_type=pl.DeviceIdType.MESH)
            keep_copy(m).start()
            back_copy(finished.at[chain, lax.rem(m, 2)], m).start()

    for chain in range(2):
        place = me if chain == 0 else last - me
        farther = me + 1 if chain == 0 else me - 1

        def relay_copy(m):
            return pltpu.make_async_remote_copy(
                src_ref=out_ref.at[out_rows(chain, m)], dst_ref=out_ref.at[out_rows(chain, m)], send_sem=ag_send.at[chain, lax.rem(m, 4)],
                recv_sem=ag_recv.at[chain, lax.rem(m, 8)], device_id={'tp': farther}, device_id_type=pl.DeviceIdType.MESH)

        for hops in range(1, size):
            m = slot - last - 2 * hops

            @pl.when((place == hops) & (m >= 0) & (m < pieces))
            def _():
                relay_copy(m).wait_recv()
                if hops < last:
                    @pl.when(m >= 4)
                    def _():
                        relay_copy(m - 4).wait_send()
                    relay_copy(m).start()

    def extra_copy(d):
        return pltpu.make_async_remote_copy(
            src_ref=acc.at[(chunks - 1) % 3, pl.ds(chunk_rows, others.shape[1])], dst_ref=others.at[d], send_sem=x_send.at[d - 1],
            recv_sem=x_recv.at[d - 1], device_id={'tp': lax.rem(me + d, size)}, device_id_type=pl.DeviceIdType.MESH)

    @pl.when(step == chunks * ff_steps)
    def _():
        others[0] = acc[(chunks - 1) % 3, chunk_rows:chunk_rows + others.shape[1]]
        for d in range(1, size):
            extra_copy(d).start()

    @pl.when(step == chunks * ff_steps + 4)
    def _():
        for d in range(1, size):
            extra_copy(d).wait()
        total = others[lax.rem(me, size)]
        for j in range(1, size):
            total = total + others[lax.rem(me + size - j, size)]
        y_ref[...] = (hextra_ref[:others.shape[1]].astype(jnp.float32) + total).astype(jnp.bfloat16)

    @pl.when(step < chunks * ff_steps)
    def _():
        chunk = lax.div(step, ff_steps)
        rows_in = normed_ref[0]
        dims = (((1,), (1,)), ((), ()))
        gate = lax.dot_general(rows_in, wgu_ref[0], dims, preferred_element_type=jnp.float32)
        up = lax.dot_general(rows_in, wgu_ref[1], dims, preferred_element_type=jnp.float32)
        activated = (gate * jax.nn.sigmoid(gate) * up).astype(jnp.bfloat16)
        block = min(1024, depth)
        first = lax.rem(step, ff_steps) == 0
        for start in range(0, depth, block):
            part = jnp.dot(activated, wd_ref[:, start:start + block], preferred_element_type=jnp.float32)

            @pl.when(first)
            def _():
                acc[lax.rem(chunk, 3), :, start:start + block] = part

            @pl.when(jnp.logical_not(first))
            def _():
                acc[lax.rem(chunk, 3), :, start:start + block] += part

    @pl.when(step == pl.num_programs(0) - 1)
    def _():
        for d in range(size):
            for which in range(2):
                kv_copy(d, which, pl.ds(0, kv_ref.shape[2])).wait()
        for chain in range(2):
            place = me if chain == 0 else last - me
            nearer = me - 1 if chain == 0 else me + 1
            farther = me + 1 if chain == 0 else me - 1

            def sent(m):
                return pltpu.make_async_remote_copy(
                    src_ref=outgoing.at[chain, m % 2], dst_ref=landed.at[chain, m % slots], send_sem=rs_send.at[chain, m % 4],
                    recv_sem=rs_recv.at[chain, m % slots], device_id={'tp': nearer}, device_id_type=pl.DeviceIdType.MESH)

            def returned(m):
                return pltpu.make_async_remote_copy(
                    src_ref=finished.at[chain, m % 2], dst_ref=out_ref.at[pl.ds(0, piece)], send_sem=ag_send.at[chain, m % 4],
                    recv_sem=ag_recv.at[chain, m % 8], device_id={'tp': farther}, device_id_type=pl.DeviceIdType.MESH)

            @pl.when(place == last)
            def _():
                for m in range(pieces - 4, pieces):
                    sent(m).wait_send()

            @pl.when((place > 0) & (place < last))
            def _():
                for m in range(pieces - 2, pieces):
                    sent(m).wait_send()
                for m in range(pieces - 4, pieces):
                    returned(m).wait_send()

            @pl.when(place == 0)
            def _():
                for m in range(pieces - 2, pieces):
                    pltpu.make_async_copy(finished.at[chain, m % 2], out_ref.at[pl.ds(0, piece)], keep_sem.at[chain, m % 2]).wait()
                    returned(m).wait_send()


KV_HEAD, KV_BULK = 4, 2


def mlp(token, normed, hextra, w_gate_up, w_down, hidden, kv, size, sides):
    chunks, lines, depth = normed.shape
    rows = hidden.shape[0]
    chunk_rows = rows // chunks
    ff = w_down.shape[0]
    ff_steps = 4
    piece = chunk_rows // 8
    slots = 4
    pieces = chunks * 4
    extra = lines - chunk_rows
    seen = min(8, extra)
    steps = chunks * ff_steps
    total_steps = ff_steps + pieces + (size - 1) + 2 * (size - 1)
    ff_block = ff // ff_steps
    at_ff = lambda g: lax.select(g < steps, lax.rem(g, ff_steps), ff_steps - 1)
    at_chunk = lambda g: lax.min(lax.div(g, ff_steps), chunks - 1)
    f32, bf16 = jnp.float32, jnp.bfloat16
    cache = jax.ShapeDtypeStruct((kv.shape[2], size * kv.shape[3], kv.shape[4]), bf16)
    return pl.pallas_call(
        functools.partial(mlp_kernel, size, sides, chunk_rows, extra, ff_steps, slots),
        out_shape=[jax.ShapeDtypeStruct((rows, depth), bf16), jax.ShapeDtypeStruct((seen, depth), bf16)] + [cache] * 2,
        grid=(total_steps,),
        in_specs=[
            pl.BlockSpec(memory_space=pl.ANY),
            pl.BlockSpec((1, lines, depth), lambda g: (at_chunk(g), 0, 0)),
            pl.BlockSpec((extra, depth), lambda g: (0, 0), pipeline_mode=pl.Buffered(1)),
            pl.BlockSpec((2, ff_block, depth), lambda g: (0, at_ff(g), 0)),
            pl.BlockSpec((ff_block, depth), lambda g: (at_ff(g), 0)),
            pl.BlockSpec(memory_space=pl.ANY),
            pl.BlockSpec(memory_space=pl.ANY),
        ],
        out_specs=[pl.BlockSpec(memory_space=pl.ANY), pl.BlockSpec((seen, depth), lambda g: (0, 0), pipeline_mode=pl.Buffered(1))] + [pl.BlockSpec(memory_space=pl.ANY)] * 2,
        scratch_shapes=[
            pltpu.VMEM((3, lines, depth), f32),
            pltpu.VMEM((2, slots, piece, depth), f32),
            pltpu.VMEM((2, 2, piece, depth), f32),
            pltpu.VMEM((2, 2, piece, depth), bf16),
            pltpu.VMEM((2, 2, piece, depth), bf16),
            pltpu.VMEM((size, seen, depth), f32),
            pltpu.SemaphoreType.DMA((2, 4)),
            pltpu.SemaphoreType.DMA((2, slots)),
            pltpu.SemaphoreType.DMA((2, 4)),
            pltpu.SemaphoreType.DMA((2, 8)),
            pltpu.SemaphoreType.DMA((2, 2)),
            pltpu.SemaphoreType.DMA((2, 2)),
            pltpu.SemaphoreType.DMA((size - 1,)),
            pltpu.SemaphoreType.DMA((size - 1,)),
            pltpu.SemaphoreType.DMA((size, 2)),
            pltpu.SemaphoreType.DMA((size, 2)),
            pltpu.SemaphoreType.REGULAR((2,)),
        ],
        compiler_params=pltpu.CompilerParams(dimension_semantics=("arbitrary",), vmem_limit_bytes=63 << 20, collective_id=0, has_side_effects=True),
        cost_estimate=pl.CostEstimate(flops=6 * rows * depth * ff, bytes_accessed=6 * chunks * depth * ff, transcendentals=rows * ff),
        name="mlp",
    )(token, normed, hextra, w_gate_up, w_down, hidden, kv)


def pick_by(index, options):
    result = options[0]
    for place in range(1, len(options)):
        result = jnp.where(index == place, options[place], result)
    return result


def solution(mesh):
    side_size = mesh.shape['side']
    tp_size = mesh.shape['tp']
    seats = mesh.shape['pair'] * side_size
    group_axes = ('pair', 'side')
    last = tp_size - 1

    def cyclic(value, d):
        return lax.ppermute(value, 'tp', [(t, (t + d) % tp_size) for t in range(tp_size)])

    def swap(value, mask):
        return lax.ppermute(value, group_axes, [(q, q ^ mask) for q in range(seats)])

    def in_order(me, copies):
        return [pick_by(me, [copies[(t - j) % tp_size] for t in range(tp_size)]) for j in range(tp_size)]

    def device_fn(x_prompt, s_len, y_tok, c_len, k_cache, v_cache, attn_gain, w_qkv, w_out, mlp_gain, w_gate_up, w_down):
        me = lax.axis_index('tp')
        seat = lax.axis_index('pair') * side_size + lax.axis_index('side')
        where = seat.reshape(1).astype(jnp.int32)
        seq_len, depth = x_prompt.shape[1:]
        heads_local = w_qkv.shape[2]
        head_dim = w_qkv.shape[4]
        width = heads_local * head_dim
        rows = seq_len // tp_size
        decodes = y_tok.shape[0]
        pad = 16
        cache_local = k_cache.shape[2]
        val = {}

        def tie(keys):
            keys = list(dict.fromkeys(keys))
            for key, value in zip(keys, lax.optimization_barrier(tuple(val[key] for key in keys))):
                val[key] = value

        val['w', 0] = lax.all_gather(lax.dynamic_index_in_dim(w_out[0, :, 0], seat, 0, keepdims=False), 'tp', axis=0, tiled=False)

        val['w_all'] = jnp.swapaxes(w_qkv[0], 1, 2).reshape(depth, 3 * width)
        tables = rope_tables(jnp.arange(seq_len, dtype=jnp.int32), head_dim)
        extra_tables = rope_tables(jnp.concatenate([c_len, jnp.zeros((pad - decodes,), jnp.int32)]), head_dim)
        y_pad = jnp.concatenate([y_tok, jnp.zeros((pad - decodes, depth), y_tok.dtype)])
        val['gain'], val['s_len'], val['mlp_gain'] = attn_gain, s_len, mlp_gain
        val['valid'] = (jnp.arange(seq_len) < s_len[0]).astype(jnp.bfloat16)
        buffers = []
        qkv = []

        def compute(name):
            kind = name[0]
            c = int(name[1:]) if name[1:].isdigit() else 0
            if kind == 'Q':
                tie(thread + ['gain'])
                *made, val['token'] = project_qkv(c, rows, val['token'], x_prompt[0], y_pad if c == 0 else None, val['gain'], val['w_all'], tables, extra_tables, head_dim)
                qkv.append(made)
                if c == 0:
                    val['dq', 0] = jnp.stack([part[rows:rows + decodes].reshape(decodes, heads_local, head_dim) for part in made])
                    for d in range(1, tp_size):
                        val['dq', d] = cyclic(val['dq', 0], d)
                return ['token']
            if kind == 'T':
                tie(thread + ['s_len'])
                context, val['token'] = attend(c, tp_size, rows, val['token'], val['s_len'], qkv[c][0], [part[1] for part in qkv], [part[2] for part in qkv], head_dim)
                val['c', c] = lax.all_gather(context, 'tp', axis=0, tiled=False)
                return ['token']
            if kind == 'K':
                tie(thread + ['valid'])
                made = []
                for d in range(tp_size):
                    keep = pick_by(me, [val['valid'][((t + d) % tp_size) * rows:((t + d) % tp_size + 1) * rows] for t in range(tp_size)])
                    for which in (1, 2):
                        rows_d = pick_by(me, [qkv[(t + d) % tp_size][which][:rows].reshape(rows, heads_local, head_dim) for t in range(tp_size)])
                        made.append(rows_d * keep[:, None, None])
                val['kv'] = jnp.stack(made).reshape(tp_size, 2, rows, heads_local, head_dim)
                return []
            if name == 'D1':
                tie(thread + [('dq', d) for d in range(tp_size)])
                dec_full = jnp.concatenate(in_order(me, [val['dq', d] for d in range(tp_size)]), axis=2)
                cache_pos = me * cache_local + jnp.arange(cache_local)
                write_mask = (cache_pos[None, :] == c_len[:, None])[:, :, None, None]
                allowed = (cache_pos[None, :] <= c_len[:, None])[:, None, :]
                key_now = jnp.where(write_mask, dec_full[1][:, None], k_cache[0])
                value_now = jnp.where(write_mask, dec_full[2][:, None], v_cache[0])
                val['key_now'], val['value_now'] = key_now, value_now
                scores = jnp.einsum('bkh,btkh->bkt', dec_full[0], key_now, preferred_element_type=jnp.float32) * head_dim ** -0.5
                scores = jnp.where(allowed, scores, -1e30)
                peak = jnp.max(scores, axis=-1, keepdims=True)
                weights = jnp.exp(scores - peak)
                total = jnp.sum(weights, axis=-1, keepdims=True)
                mixed = jnp.einsum('bkt,btkh->bkh', weights.astype(jnp.bfloat16), value_now, preferred_element_type=jnp.float32)
                packed = jnp.stack([mixed, jnp.broadcast_to(peak, mixed.shape), jnp.broadcast_to(total, mixed.shape)])
                packed = packed.reshape(3, decodes, tp_size, heads_local, head_dim)
                for d in range(tp_size):
                    share = lax.dynamic_index_in_dim(packed, lax.rem(me + d, tp_size), 2, keepdims=False)
                    val['ds', d] = share if d == 0 else cyclic(share, d)
                return [('ds', 0)]
            if name == 'D2':
                tie(thread + [('ds', d) for d in range(tp_size)])
                shares = [val['ds', d] for d in range(tp_size)]
                top = functools.reduce(jnp.maximum, [share[1] for share in shares])
                factors = [jnp.exp(share[1] - top) for share in shares]
                dec_mixed = sum(share[0] * factor for share, factor in zip(shares, factors))
                dec_total = sum(share[2] * factor for share, factor in zip(shares, factors))
                val['dc', 0] = (dec_mixed / dec_total).astype(jnp.bfloat16).reshape(decodes, width)
                for d in range(1, tp_size):
                    val['dc', d] = cyclic(val['dc', 0], d)
                return [('dc', 0)]
            if kind == 'O':
                w_keys = [('w', r) for r in range(seats)]
                extra_keys = [('dc', d) for d in range(tp_size)] if c == last else []
                tie(thread + ['mlp_gain', ('c', c)] + extra_keys + (w_keys if c == 0 else []))
                extras = []
                if c == last:
                    extras = [jnp.pad(jnp.stack(in_order(me, [val[key] for key in extra_keys])), ((0, 0), (0, pad - decodes), (0, 0))), y_pad]
                made = project_out(c, tp_size, pad, val['token'], where, val['c', c], [val[key] for key in w_keys], x_prompt[0], val['mlp_gain'], extras, [val[key] for key in buffers])
                buffers[:] = ['normed', 'h']
                val['normed'], val['h'], val['token'] = made[0], made[1], made[-1]
                if c == last:
                    val['hx'] = made[2]
                return ['token']
            val['out'], val['y'], val['k'], val['v'] = mlp(val['token'], val['normed'], val['hx'], jnp.transpose(w_gate_up[0], (1, 2, 0)), w_down[0], val['h'], val['kv'], tp_size, side_size)
            return ['y']

        def transfer(name):
            bases = [0] if name == 'w2' else list(range(0, seats, 2))
            tie(thread + [('w', base) for base in bases])
            for mask in (range(2, seats, 2) if name == 'w2' else [1]):
                for base in bases:
                    val['w', base ^ mask] = swap(val['w', base], mask)

        val['token'] = jnp.zeros(TOKEN.shape, TOKEN.dtype)
        thread = ['token']
        for name in ORDER:
            if name[0] in 'QTKDOB':
                made = compute(name)
                thread = thread + made if name in ('K', 'D1', 'D2') else made
            else:
                transfer(name)

        return (val['out'][None], val['y'][:decodes], val['k'][None, None], val['v'][None, None], val['key_now'][None], val['value_now'][None])

    cache_spec = P(None, group_axes, 'tp', None, None)
    in_specs = (P(group_axes, None, None), P(group_axes), P(group_axes, None), P(group_axes), cache_spec, cache_spec, P(), P(None, None, 'tp', None, None), P(None, 'tp', None, None, None), P(), P(None, None, None, 'tp'), P(None, 'tp', None))
    out_specs = (P(group_axes, None, None), P(group_axes, None), cache_spec, cache_spec, cache_spec, cache_spec)
    return jax.shard_map(device_fn, mesh=mesh, in_specs=in_specs, out_specs=out_specs, check_vma=False)
```

```python
import functools

import jax
import jax.numpy as jnp
from jax import lax
from jax.experimental import pallas as pl
from jax.experimental.pallas import tpu as pltpu
from jax.sharding import PartitionSpec as P

ROPE_BASE = 10000.0
NORM_EPS = 1e-5

ORDER = (
    'Q0', 'T0', 'Q1', 'T1', 'w2', 'Q2', 'T2', 'Q3', 'T3', 'D1', 'K', 'D2', 'w3', 'k2', 'k1', 'k3', 'k0',
    'O0', 'O1', 'O2', 'O3', 'B', 'l0', 'l2', 'l1', 'l3',
)


def rms_scale(values_f32, gain_f32):
    inv_rms = lax.rsqrt(jnp.mean(values_f32 * values_f32, axis=-1, keepdims=True) + NORM_EPS)
    return (values_f32 * inv_rms * gain_f32).astype(jnp.bfloat16)


def rope_tables(positions, head_dim):
    half_dim = head_dim // 2
    inv_freq = ROPE_BASE ** (-2.0 * jnp.arange(half_dim, dtype=jnp.float32) / head_dim)
    angles = positions.astype(jnp.float32)[:, None] * inv_freq[None, :]
    cos_table = jnp.cos(angles)
    sin_table = jnp.sin(angles)
    return jnp.concatenate([cos_table, cos_table], axis=1), jnp.concatenate([-sin_table, sin_table], axis=1)


def qkv_kernel(head_dim, extra, *refs):
    x_ref, gain_ref, wq_ref, wk_ref, wv_ref, cos_ref, sin_ref = refs[:7]
    extra_refs = refs[7:10] if extra else None
    q_ref, k_ref, v_ref, token_ref, normed_ref = refs[-5:]
    rows = x_ref.shape[0]

    @pl.when(pl.program_id(0) == 0)
    def _():
        gain = gain_ref[...].astype(jnp.float32)
        normed_ref[:rows] = rms_scale(x_ref[...].astype(jnp.float32), gain)
        if extra:
            normed_ref[rows:] = rms_scale(extra_refs[0][...].astype(jnp.float32), gain)
        token_ref[...] = jnp.zeros_like(token_ref)

    cos, sin = cos_ref[...], sin_ref[...]
    if extra:
        cos = jnp.concatenate([cos, extra_refs[1][...]], axis=0)
        sin = jnp.concatenate([sin, extra_refs[2][...]], axis=0)
    for w_ref, out_ref in ((wq_ref, q_ref), (wk_ref, k_ref), (wv_ref, v_ref)):
        acc = jnp.dot(normed_ref[...], w_ref[...], preferred_element_type=jnp.float32)
        for start in range(0, acc.shape[1], head_dim):
            vals = acc[:, start:start + head_dim]
            if out_ref is not v_ref:
                vals = vals * cos + pltpu.roll(vals, head_dim // 2, 1) * sin
            out_ref[:, start:start + head_dim] = vals.astype(out_ref.dtype)


TOKEN = jax.ShapeDtypeStruct((8, 128), jnp.float32)


def project_qkv(chunk, rows, token, x, extra_rows, gain, w_all, tables, extra_tables, head_dim):
    depth = x.shape[1]
    width = w_all.shape[1] // 3
    block = 2 * head_dim
    steps = width // block
    extras = [] if extra_rows is None else [extra_rows, *extra_tables]
    total = rows + (0 if extra_rows is None else extra_rows.shape[0])
    whole = lambda shape: pl.BlockSpec(shape, lambda n: (0, 0), pipeline_mode=pl.Buffered(1))
    columns = lambda part: pl.BlockSpec((depth, block), lambda n: (0, part * steps + n))
    return pl.pallas_call(
        functools.partial(qkv_kernel, head_dim, extra_rows is not None),
        out_shape=[jax.ShapeDtypeStruct((total, width), jnp.bfloat16)] * 3 + [TOKEN],
        grid=(steps,),
        in_specs=[
            pl.BlockSpec((rows, depth), lambda n: (chunk, 0), pipeline_mode=pl.Buffered(1)),
            whole((1, depth)),
            columns(0),
            columns(1),
            columns(2),
            pl.BlockSpec((rows, head_dim), lambda n: (chunk, 0), pipeline_mode=pl.Buffered(1)),
            pl.BlockSpec((rows, head_dim), lambda n: (chunk, 0), pipeline_mode=pl.Buffered(1)),
        ] + [whole(e.shape) for e in extras] + [pl.BlockSpec(memory_space=pl.ANY)],
        out_specs=[pl.BlockSpec((total, block), lambda n: (0, n))] * 3 + [whole(TOKEN.shape)],
        scratch_shapes=[pltpu.VMEM((total, depth), jnp.bfloat16)],
        compiler_params=pltpu.CompilerParams(dimension_semantics=("arbitrary",), vmem_limit_bytes=48 << 20),
        cost_estimate=pl.CostEstimate(flops=6 * total * depth * width, bytes_accessed=2 * (total * depth + 3 * depth * width + 3 * total * width), transcendentals=0),
        name="project_qkv",
    )(x, gain, w_all, w_all, w_all, *tables, *extras, token)


def attend_kernel(chunk, first_checked, q_rows, slen_ref, *refs):
    q_ref = refs[0]
    k_refs = refs[1:chunk + 2]
    v_refs = refs[chunk + 2:2 * chunk + 3]
    out_ref, token_ref = refs[-2:]
    token_ref[...] = jnp.zeros_like(token_ref)
    rows, head_dim = q_ref.shape
    scale = head_dim ** -0.5
    limit = slen_ref[0]
    for start in range(0, rows, q_rows):
        query = q_ref[start:start + q_rows, :]
        scores = []
        values = []
        for part in range(chunk + 1):
            keys = rows if part < chunk else start + q_rows
            score = lax.dot_general(query, k_refs[part][:keys, :], (((1,), (1,)), ((), ())), preferred_element_type=jnp.float32) * scale
            key_pos = lax.broadcasted_iota(jnp.int32, score.shape, 1)
            if part == chunk:
                allowed = key_pos <= lax.broadcasted_iota(jnp.int32, score.shape, 0) + start
                if part >= first_checked:
                    allowed = allowed & (key_pos < limit - part * rows)
                score = jnp.where(allowed, score, -1e30)
            elif part >= first_checked:
                score = jnp.where(key_pos < limit - part * rows, score, -1e30)
            scores.append(score)
            values.append(v_refs[part][:keys, :])
        peak = functools.reduce(jnp.maximum, [jnp.max(score, axis=-1, keepdims=True) for score in scores])
        total = jnp.zeros((q_rows, 1), jnp.float32)
        mixed = jnp.zeros((q_rows, head_dim), jnp.float32)
        for score, value in zip(scores, values):
            weight = jnp.exp(score - peak)
            total = total + jnp.sum(weight, axis=-1, keepdims=True)
            mixed = mixed + jnp.dot(weight.astype(jnp.bfloat16), value, preferred_element_type=jnp.float32)
        out_ref[start:start + q_rows, :] = (mixed / total).astype(out_ref.dtype)


def attend(chunk, chunks, rows, token, s_len, queries, keys, values, head_dim):
    width = queries.shape[1]
    heads = width // head_dim

    pick = pl.BlockSpec((rows, head_dim), lambda h, slen: (0, h))
    total_keys = rows * (chunk + 1)
    return pl.pallas_call(
        functools.partial(attend_kernel, chunk, chunks // 2, min(256, rows)),
        out_shape=[jax.ShapeDtypeStruct((rows, width), jnp.bfloat16), TOKEN],
        grid_spec=pltpu.PrefetchScalarGridSpec(
            num_scalar_prefetch=1,
            grid=(heads,),
            in_specs=[pick] * (2 * chunk + 3) + [pl.BlockSpec(memory_space=pl.ANY)],
            out_specs=[pick, pl.BlockSpec(TOKEN.shape, lambda h, slen: (0, 0))],
        ),
        compiler_params=pltpu.CompilerParams(dimension_semantics=("arbitrary",), vmem_limit_bytes=48 << 20),
        cost_estimate=pl.CostEstimate(flops=8 * heads * rows * total_keys * head_dim, bytes_accessed=2 * width * (2 * total_keys + 2 * rows), transcendentals=heads * rows * total_keys),
        name=f"attend_{chunk}",
    )(s_len, queries, *keys, *values, token)


def output_kernel(size, heads, extra, aliased, where_ref, *refs):
    context_ref, refs = refs[0], refs[1:]
    w_refs, refs = refs[:heads], refs[heads:]
    x_ref, gain_ref, refs = refs[0], refs[1], refs[2:]
    if extra:
        context_x_ref, x_x_ref, refs = refs[0], refs[1], refs[2:]
    refs = refs[1:]
    if aliased:
        refs = refs[2:]
    normed_ref, hidden_ref, refs = refs[0], refs[1], refs[2:]
    if extra:
        hidden_x_ref, refs = refs[0], refs[1:]
    token_ref, full_ref, square_ref = refs
    rows = context_ref.shape[1]
    head_dim, block = w_refs[0].shape[1:]
    depth = hidden_ref.shape[1]
    step = pl.program_id(0)

    @pl.when(step == 0)
    def _():
        square_ref[...] = jnp.zeros_like(square_ref)
        token_ref[...] = jnp.zeros_like(token_ref)
        for r in range(heads):
            columns = pl.ds(pl.multiple_of(lax.bitwise_xor(where_ref[0], r) * head_dim, head_dim), head_dim)
            for t in range(size):
                there = (r * size + t) * head_dim
                full_ref[:rows, there:there + head_dim] = context_ref[t, :, columns]
                if extra:
                    full_ref[rows:, there:there + head_dim] = context_x_ref[t, :, columns]

    w_block = jnp.concatenate([w_ref[...].reshape(size * head_dim, block) for w_ref in w_refs], axis=0)
    acc = jnp.dot(full_ref[...], w_block, preferred_element_type=jnp.float32)
    columns = pl.ds(pl.multiple_of(step * block, block), block)
    hidden = (x_ref[...].astype(jnp.float32) + acc[:rows]).astype(jnp.bfloat16)
    hidden_ref[:, columns] = hidden
    hidden_f32 = hidden.astype(jnp.float32)
    square_ref[:rows] += jnp.sum(hidden_f32 * hidden_f32, axis=-1, keepdims=True)
    if extra:
        hidden = (x_x_ref[...].astype(jnp.float32) + acc[rows:]).astype(jnp.bfloat16)
        hidden_x_ref[:, columns] = hidden
        hidden_f32 = hidden.astype(jnp.float32)
        square_ref[rows:] += jnp.sum(hidden_f32 * hidden_f32, axis=-1, keepdims=True)

    @pl.when(step == pl.num_programs(0) - 1)
    def _():
        half = rows // 2
        inv_rms = lax.rsqrt(square_ref[...] / depth + NORM_EPS)
        for start in range(0, depth, block):
            gain = gain_ref[:, start:start + block].astype(jnp.float32)
            for part in range(2):
                lo, hi = part * half, (part + 1) * half
                normed_ref[part, :half, start:start + block] = (hidden_ref[lo:hi, start:start + block].astype(jnp.float32) * inv_rms[lo:hi] * gain).astype(jnp.bfloat16)
                if extra and part == 1:
                    normed_ref[part, half:, start:start + block] = (hidden_x_ref[:, start:start + block].astype(jnp.float32) * inv_rms[rows:] * gain).astype(jnp.bfloat16)
                else:
                    normed_ref[part, half:, start:start + block] = jnp.zeros((normed_ref.shape[1] - half, block), jnp.bfloat16)


def project_out(chunk, chunks, pad, token, where, context, w_heads, x, gain, extras, buffers):
    rows, width = context.shape[1:]
    depth = x.shape[1]
    heads = len(w_heads)
    size, head_dim = w_heads[0].shape[:2]
    block = min(512, depth)
    total = rows + (pad if extras else 0)
    whole = lambda shape: pl.BlockSpec(shape, lambda n, where: (0,) * len(shape), pipeline_mode=pl.Buffered(1))
    in_specs = [whole(context.shape)]
    in_specs += [pl.BlockSpec((size, head_dim, block), lambda n, where: (0, 0, n))] * heads
    in_specs += [pl.BlockSpec((rows, block), lambda n, where: (chunk, n)), whole((1, depth))]
    out_shape = [jax.ShapeDtypeStruct((2 * chunks, rows // 2 + pad, depth), jnp.bfloat16), jax.ShapeDtypeStruct((rows * chunks, depth), jnp.bfloat16)]
    out_specs = [
        pl.BlockSpec((2, rows // 2 + pad, depth), lambda n, where: (chunk, 0, 0), pipeline_mode=pl.Buffered(1)),
        pl.BlockSpec((rows, depth), lambda n, where: (chunk, 0), pipeline_mode=pl.Buffered(1)),
    ]
    if extras:
        in_specs += [whole(extras[0].shape), pl.BlockSpec((pad, block), lambda n, where: (0, n))]
        out_shape.append(jax.ShapeDtypeStruct((pad, depth), jnp.bfloat16))
        out_specs.append(whole((pad, depth)))
    in_specs.append(pl.BlockSpec(memory_space=pl.ANY))
    out_shape.append(TOKEN)
    out_specs.append(whole(TOKEN.shape))
    aliases = {}
    if buffers:
        aliases = {1 + len(in_specs): 0, 2 + len(in_specs): 1}
        in_specs += [pl.BlockSpec(memory_space=pl.ANY)] * 2
    return pl.pallas_call(
        functools.partial(output_kernel, size, heads, bool(extras), bool(buffers)),
        out_shape=out_shape,
        grid_spec=pltpu.PrefetchScalarGridSpec(
            num_scalar_prefetch=1,
            grid=(depth // block,),
            in_specs=in_specs,
            out_specs=out_specs,
            scratch_shapes=[pltpu.VMEM((total, size * width), jnp.bfloat16), pltpu.VMEM((total, 1), jnp.float32)],
        ),
        input_output_aliases=aliases,
        compiler_params=pltpu.CompilerParams(dimension_semantics=("arbitrary",), vmem_limit_bytes=60 << 20),
        cost_estimate=pl.CostEstimate(flops=2 * total * size * width * depth, bytes_accessed=2 * (size * width * depth + 4 * rows * width + 3 * total * depth), transcendentals=0),
        name="project_out",
    )(where, context, *w_heads, x, gain, *extras, token, *buffers)


def mlp_kernel(size, chunk_rows, extra, ff_steps, slots, token_ref, normed_ref, hextra_ref, wgu_ref, wd_ref, h_ref, out_ref, y_ref,
               acc, landed, outgoing, finished, residual, others, activated,
               rs_send, rs_recv, ag_send, ag_recv, keep_sem, h_sem, x_send, x_recv, credit):
    step = pl.program_id(0)
    me = lax.axis_index('tp')
    depth = wd_ref.shape[1]
    chunks = (out_ref.shape[0] // chunk_rows)
    piece = outgoing.shape[2]
    per_chunk = chunk_rows // (2 * piece)
    pieces = chunks * per_chunk
    subs = per_chunk // ff_steps
    last = size - 1

    @pl.when(step == 0)
    def _():
        barrier = pltpu.get_barrier_semaphore()
        for d in range(1, size):
            pl.semaphore_signal(barrier, inc=1, device_id={'tp': lax.rem(me + d, size)}, device_id_type=pl.DeviceIdType.MESH)
        pl.semaphore_wait(barrier, size - 1)

    def own_part(chain, m):
        start = pl.multiple_of(chain * (chunk_rows // 2) + lax.rem(m, per_chunk) * piece, piece)
        return acc.at[lax.rem(lax.div(m, per_chunk), 3), pl.ds(start, piece)]

    def out_rows(chain, m):
        start = pl.multiple_of(lax.div(m, per_chunk) * chunk_rows + chain * (chunk_rows // 2) + lax.rem(m, per_chunk) * piece, piece)
        return pl.ds(start, piece)

    def exchange(slot):
        for chain in range(2):
            place = me if chain == 0 else last - me
            nearer = me - 1 if chain == 0 else me + 1
            farther = me + 1 if chain == 0 else me - 1

            def sum_copy(source, m):
                return pltpu.make_async_remote_copy(
                    src_ref=source, dst_ref=landed.at[chain, lax.rem(m, slots)], send_sem=rs_send.at[chain, lax.rem(m, 4)],
                    recv_sem=rs_recv.at[chain, lax.rem(m, slots)], device_id={'tp': nearer}, device_id_type=pl.DeviceIdType.MESH)

            def keep_copy(m):
                return pltpu.make_async_copy(finished.at[chain, lax.rem(m, 2)], out_ref.at[out_rows(chain, m)], keep_sem.at[chain, lax.rem(m, 2)])

            def h_copy(m):
                return pltpu.make_async_copy(h_ref.at[out_rows(chain, m)], residual.at[chain, lax.rem(m, 2)], h_sem.at[chain, lax.rem(m, 2)])

            def back_copy(source, m):
                return pltpu.make_async_remote_copy(
                    src_ref=source, dst_ref=out_ref.at[out_rows(chain, m)], send_sem=ag_send.at[chain, lax.rem(m, 4)],
                    recv_sem=ag_recv.at[chain, lax.rem(m, 8)], device_id={'tp': farther}, device_id_type=pl.DeviceIdType.MESH)

            @pl.when((place == last) & (slot >= 0) & (slot < pieces))
            def _():
                @pl.when(slot >= 4)
                def _():
                    sum_copy(own_part(chain, slot - 4), slot - 4).wait_send()

                @pl.when(slot >= slots)
                def _():
                    pl.semaphore_wait(credit.at[chain], 1)
                sum_copy(own_part(chain, slot), slot).start()

            for hops in range(1, last):
                m = slot - (last - hops)

                @pl.when((place == hops) & (m >= 0) & (m < pieces))
                def _():
                    @pl.when(m >= 2)
                    def _():
                        sum_copy(outgoing.at[chain, lax.rem(m, 2)], m - 2).wait_send()
                    sum_copy(outgoing.at[chain, lax.rem(m, 2)], m).wait_recv()
                    outgoing[chain, lax.rem(m, 2)] = landed[chain, lax.rem(m, slots)] + own_part(chain, m)[...]

                    @pl.when(m + slots < pieces)
                    def _():
                        pl.semaphore_signal(credit.at[chain], inc=1, device_id={'tp': farther}, device_id_type=pl.DeviceIdType.MESH)

                    @pl.when(m >= slots)
                    def _():
                        pl.semaphore_wait(credit.at[chain], 1)
                    sum_copy(outgoing.at[chain, lax.rem(m, 2)], m).start()

            m = slot - last

            @pl.when((place == 0) & (slot == 0))
            def _():
                h_copy(0).start()

            @pl.when((place == 0) & (m >= 0) & (m < pieces))
            def _():
                @pl.when(m + 1 < pieces)
                def _():
                    h_copy(m + 1).start()

                @pl.when(m >= 2)
                def _():
                    keep_copy(m - 2).wait()
                    back_copy(finished.at[chain, lax.rem(m, 2)], m - 2).wait_send()
                h_copy(m).wait()
                sum_copy(outgoing.at[chain, lax.rem(m, 2)], m).wait_recv()
                total = landed[chain, lax.rem(m, slots)] + own_part(chain, m)[...]
                finished[chain, lax.rem(m, 2)] = (residual[chain, lax.rem(m, 2)].astype(jnp.float32) + total).astype(jnp.bfloat16)

                @pl.when(m + slots < pieces)
                def _():
                    pl.semaphore_signal(credit.at[chain], inc=1, device_id={'tp': farther}, device_id_type=pl.DeviceIdType.MESH)
                keep_copy(m).start()
                back_copy(finished.at[chain, lax.rem(m, 2)], m).start()

        for chain in range(2):
            place = me if chain == 0 else last - me
            farther = me + 1 if chain == 0 else me - 1

            def relay_copy(m):
                return pltpu.make_async_remote_copy(
                    src_ref=out_ref.at[out_rows(chain, m)], dst_ref=out_ref.at[out_rows(chain, m)], send_sem=ag_send.at[chain, lax.rem(m, 4)],
                    recv_sem=ag_recv.at[chain, lax.rem(m, 8)], device_id={'tp': farther}, device_id_type=pl.DeviceIdType.MESH)

            for hops in range(1, size):
                m = slot - last - 2 * hops

                @pl.when((place == hops) & (m >= 0) & (m < pieces))
                def _():
                    relay_copy(m).wait_recv()
                    if hops < last:
                        @pl.when(m >= 4)
                        def _():
                            relay_copy(m - 4).wait_send()
                        relay_copy(m).start()

    def extra_copy(d):
        return pltpu.make_async_remote_copy(
            src_ref=acc.at[(chunks - 1) % 3, pl.ds(chunk_rows, others.shape[1])], dst_ref=others.at[d], send_sem=x_send.at[d - 1],
            recv_sem=x_recv.at[d - 1], device_id={'tp': lax.rem(me + d, size)}, device_id_type=pl.DeviceIdType.MESH)

    @pl.when(step == chunks * ff_steps)
    def _():
        others[0] = acc[(chunks - 1) % 3, chunk_rows:chunk_rows + others.shape[1]]
        for d in range(1, size):
            extra_copy(d).start()

    @pl.when(step == chunks * ff_steps + 4)
    def _():
        for d in range(1, size):
            extra_copy(d).wait()
        total = others[lax.rem(me, size)]
        for j in range(1, size):
            total = total + others[lax.rem(me + size - j, size)]
        y_ref[...] = (hextra_ref[:others.shape[1]].astype(jnp.float32) + total).astype(jnp.bfloat16)

    chunk = lax.div(step, ff_steps)
    block = min(1024, depth)

    def compute_gate():
        rows_in = normed_ref[0]
        dims = (((1,), (1,)), ((), ()))
        gate = lax.dot_general(rows_in, wgu_ref[0], dims, preferred_element_type=jnp.float32)
        up = lax.dot_general(rows_in, wgu_ref[1], dims, preferred_element_type=jnp.float32)
        activated[...] = (gate * jax.nn.sigmoid(gate) * up).astype(jnp.bfloat16)

    def compute_down():
        first = lax.rem(step, ff_steps) == 0
        for start in range(0, depth, block):
            part = jnp.dot(activated[...], wd_ref[:, start:start + block], preferred_element_type=jnp.float32)

            @pl.when(first)
            def _():
                acc[lax.rem(chunk, 3), :, start:start + block] = part

            @pl.when(jnp.logical_not(first))
            def _():
                acc[lax.rem(chunk, 3), :, start:start + block] += part

    for sub in range(subs):
        exchange((step - ff_steps) * subs + sub)
        for part in range(2):
            if part * subs // 2 == sub:
                pl.when(step < chunks * ff_steps)((compute_gate, compute_down)[part])

    @pl.when(step == pl.num_programs(0) - 1)
    def _():
        for chain in range(2):
            place = me if chain == 0 else last - me
            nearer = me - 1 if chain == 0 else me + 1
            farther = me + 1 if chain == 0 else me - 1

            def sent(m):
                return pltpu.make_async_remote_copy(
                    src_ref=outgoing.at[chain, m % 2], dst_ref=landed.at[chain, m % slots], send_sem=rs_send.at[chain, m % 4],
                    recv_sem=rs_recv.at[chain, m % slots], device_id={'tp': nearer}, device_id_type=pl.DeviceIdType.MESH)

            def returned(m):
                return pltpu.make_async_remote_copy(
                    src_ref=finished.at[chain, m % 2], dst_ref=out_ref.at[pl.ds(0, piece)], send_sem=ag_send.at[chain, m % 4],
                    recv_sem=ag_recv.at[chain, m % 8], device_id={'tp': farther}, device_id_type=pl.DeviceIdType.MESH)

            @pl.when(place == last)
            def _():
                for m in range(pieces - 4, pieces):
                    sent(m).wait_send()

            @pl.when((place > 0) & (place < last))
            def _():
                for m in range(pieces - 2, pieces):
                    sent(m).wait_send()
                for m in range(pieces - 4, pieces):
                    returned(m).wait_send()

            @pl.when(place == 0)
            def _():
                for m in range(pieces - 2, pieces):
                    pltpu.make_async_copy(finished.at[chain, m % 2], out_ref.at[pl.ds(0, piece)], keep_sem.at[chain, m % 2]).wait()
                    returned(m).wait_send()


SUBSLOTS = 2


def mlp(token, normed, hextra, w_gate_up, w_down, hidden, size):
    chunks, lines, depth = normed.shape
    rows = hidden.shape[0]
    chunk_rows = rows // chunks
    ff = w_down.shape[0]
    ff_steps = 4
    piece = chunk_rows // (8 * SUBSLOTS)
    slots = 4
    pieces = chunks * 4 * SUBSLOTS
    extra = lines - chunk_rows
    seen = min(8, extra)
    steps = chunks * ff_steps
    total_steps = ff_steps + -(-(pieces + 3 * (size - 1)) // SUBSLOTS)
    ff_block = ff // ff_steps
    at_ff = lambda g: lax.select(g < steps, lax.rem(g, ff_steps), ff_steps - 1)
    at_chunk = lambda g: lax.min(lax.div(g, ff_steps), chunks - 1)
    f32, bf16 = jnp.float32, jnp.bfloat16
    return pl.pallas_call(
        functools.partial(mlp_kernel, size, chunk_rows, extra, ff_steps, slots),
        out_shape=[jax.ShapeDtypeStruct((rows, depth), bf16), jax.ShapeDtypeStruct((seen, depth), bf16)],
        grid=(total_steps,),
        in_specs=[
            pl.BlockSpec(memory_space=pl.ANY),
            pl.BlockSpec((1, lines, depth), lambda g: (at_chunk(g), 0, 0)),
            pl.BlockSpec((extra, depth), lambda g: (0, 0), pipeline_mode=pl.Buffered(1)),
            pl.BlockSpec((2, ff_block, depth), lambda g: (0, at_ff(g), 0)),
            pl.BlockSpec((ff_block, depth), lambda g: (at_ff(g), 0)),
            pl.BlockSpec(memory_space=pl.ANY),
        ],
        out_specs=[pl.BlockSpec(memory_space=pl.ANY), pl.BlockSpec((seen, depth), lambda g: (0, 0), pipeline_mode=pl.Buffered(1))],
        scratch_shapes=[
            pltpu.VMEM((3, lines, depth), f32),
            pltpu.VMEM((2, slots, piece, depth), f32),
            pltpu.VMEM((2, 2, piece, depth), f32),
            pltpu.VMEM((2, 2, piece, depth), bf16),
            pltpu.VMEM((2, 2, piece, depth), bf16),
            pltpu.VMEM((size, seen, depth), f32),
            pltpu.VMEM((lines, ff_block), bf16),
            pltpu.SemaphoreType.DMA((2, 4)),
            pltpu.SemaphoreType.DMA((2, slots)),
            pltpu.SemaphoreType.DMA((2, 4)),
            pltpu.SemaphoreType.DMA((2, 8)),
            pltpu.SemaphoreType.DMA((2, 2)),
            pltpu.SemaphoreType.DMA((2, 2)),
            pltpu.SemaphoreType.DMA((size - 1,)),
            pltpu.SemaphoreType.DMA((size - 1,)),
            pltpu.SemaphoreType.REGULAR((2,)),
        ],
        compiler_params=pltpu.CompilerParams(dimension_semantics=("arbitrary",), vmem_limit_bytes=63 << 20, collective_id=0, has_side_effects=True),
        cost_estimate=pl.CostEstimate(flops=6 * rows * depth * ff, bytes_accessed=6 * chunks * depth * ff, transcendentals=rows * ff),
        name="mlp",
    )(token, normed, hextra, w_gate_up, w_down, hidden)


def pick_by(index, options):
    result = options[0]
    for place in range(1, len(options)):
        result = jnp.where(index == place, options[place], result)
    return result


def solution(mesh):
    side_size = mesh.shape['side']
    tp_size = mesh.shape['tp']
    seats = mesh.shape['pair'] * side_size
    group_axes = ('pair', 'side')
    last = tp_size - 1

    def cyclic(value, d):
        return lax.ppermute(value, 'tp', [(t, (t + d) % tp_size) for t in range(tp_size)])

    def swap(value, mask):
        return lax.ppermute(value, group_axes, [(q, q ^ mask) for q in range(seats)])

    def in_order(me, copies):
        return [pick_by(me, [copies[(t - j) % tp_size] for t in range(tp_size)]) for j in range(tp_size)]

    def device_fn(x_prompt, s_len, y_tok, c_len, k_cache, v_cache, attn_gain, w_qkv, w_out, mlp_gain, w_gate_up, w_down):
        me = lax.axis_index('tp')
        seat = lax.axis_index('pair') * side_size + lax.axis_index('side')
        where = seat.reshape(1).astype(jnp.int32)
        seq_len, depth = x_prompt.shape[1:]
        heads_local = w_qkv.shape[2]
        head_dim = w_qkv.shape[4]
        width = heads_local * head_dim
        rows = seq_len // tp_size
        decodes = y_tok.shape[0]
        pad = 16
        cache_local = k_cache.shape[2]
        val = {}

        def tie(keys):
            keys = list(dict.fromkeys(keys))
            for key, value in zip(keys, lax.optimization_barrier(tuple(val[key] for key in keys))):
                val[key] = value

        val['w', 0] = lax.all_gather(lax.dynamic_index_in_dim(w_out[0, :, 0], seat, 0, keepdims=False), 'tp', axis=0, tiled=False)

        val['w_all'] = jnp.swapaxes(w_qkv[0], 1, 2).reshape(depth, 3 * width)
        tables = rope_tables(jnp.arange(seq_len, dtype=jnp.int32), head_dim)
        extra_tables = rope_tables(jnp.concatenate([c_len, jnp.zeros((pad - decodes,), jnp.int32)]), head_dim)
        y_pad = jnp.concatenate([y_tok, jnp.zeros((pad - decodes, depth), y_tok.dtype)])
        val['gain'], val['s_len'], val['mlp_gain'] = attn_gain, s_len, mlp_gain
        val['valid'] = (jnp.arange(seq_len) < s_len[0]).astype(jnp.bfloat16)
        for which in range(2):
            val['cache', which] = jnp.zeros((rows, tp_size, heads_local, head_dim), jnp.bfloat16)
        buffers = []
        qkv = []

        def compute(name):
            kind = name[0]
            c = int(name[1:]) if name[1:].isdigit() else 0
            if kind == 'Q':
                tie(thread + ['gain'])
                *made, val['token'] = project_qkv(c, rows, val['token'], x_prompt[0], y_pad if c == 0 else None, val['gain'], val['w_all'], tables, extra_tables, head_dim)
                qkv.append(made)
                if c == 0:
                    val['dq', 0] = jnp.stack([part[rows:rows + decodes].reshape(decodes, heads_local, head_dim) for part in made])
                    for d in range(1, tp_size):
                        val['dq', d] = cyclic(val['dq', 0], d)
                return ['token']
            if kind == 'T':
                tie(thread + ['s_len'])
                context, val['token'] = attend(c, tp_size, rows, val['token'], val['s_len'], qkv[c][0], [part[1] for part in qkv], [part[2] for part in qkv], head_dim)
                val['c', c] = lax.all_gather(context, 'tp', axis=0, tiled=False)
                return ['token']
            if kind == 'K':
                tie(thread + ['valid'])
                for d in range(tp_size):
                    made = []
                    keep = pick_by(me, [val['valid'][((t + d) % tp_size) * rows:((t + d) % tp_size + 1) * rows] for t in range(tp_size)])
                    for which in (1, 2):
                        rows_d = pick_by(me, [qkv[(t + d) % tp_size][which][:rows].reshape(rows, heads_local, head_dim) for t in range(tp_size)])
                        made.append(rows_d * keep[:, None, None])
                    val['kv', d] = jnp.stack(made)
                return []
            if name == 'D1':
                tie(thread + [('dq', d) for d in range(tp_size)])
                dec_full = jnp.concatenate(in_order(me, [val['dq', d] for d in range(tp_size)]), axis=2)
                cache_pos = me * cache_local + jnp.arange(cache_local)
                write_mask = (cache_pos[None, :] == c_len[:, None])[:, :, None, None]
                allowed = (cache_pos[None, :] <= c_len[:, None])[:, None, :]
                key_now = jnp.where(write_mask, dec_full[1][:, None], k_cache[0])
                value_now = jnp.where(write_mask, dec_full[2][:, None], v_cache[0])
                val['key_now'], val['value_now'] = key_now, value_now
                scores = jnp.einsum('bkh,btkh->bkt', dec_full[0], key_now, preferred_element_type=jnp.float32) * head_dim ** -0.5
                scores = jnp.where(allowed, scores, -1e30)
                peak = jnp.max(scores, axis=-1, keepdims=True)
                weights = jnp.exp(scores - peak)
                total = jnp.sum(weights, axis=-1, keepdims=True)
                mixed = jnp.einsum('bkt,btkh->bkh', weights.astype(jnp.bfloat16), value_now, preferred_element_type=jnp.float32)
                packed = jnp.stack([mixed, jnp.broadcast_to(peak, mixed.shape), jnp.broadcast_to(total, mixed.shape)])
                packed = packed.reshape(3, decodes, tp_size, heads_local, head_dim)
                for d in range(tp_size):
                    share = lax.dynamic_index_in_dim(packed, lax.rem(me + d, tp_size), 2, keepdims=False)
                    val['ds', d] = share if d == 0 else cyclic(share, d)
                return [('ds', 0)]
            if name == 'D2':
                tie(thread + [('ds', d) for d in range(tp_size)])
                shares = [val['ds', d] for d in range(tp_size)]
                top = functools.reduce(jnp.maximum, [share[1] for share in shares])
                factors = [jnp.exp(share[1] - top) for share in shares]
                dec_mixed = sum(share[0] * factor for share, factor in zip(shares, factors))
                dec_total = sum(share[2] * factor for share, factor in zip(shares, factors))
                val['dc', 0] = (dec_mixed / dec_total).astype(jnp.bfloat16).reshape(decodes, width)
                for d in range(1, tp_size):
                    val['dc', d] = cyclic(val['dc', 0], d)
                return [('dc', 0)]
            if kind == 'O':
                w_keys = [('w', r) for r in range(seats)]
                extra_keys = [('dc', d) for d in range(tp_size)] if c == last else []
                tie(thread + ['mlp_gain', ('c', c)] + extra_keys + (w_keys if c == 0 else []))
                extras = []
                if c == last:
                    extras = [jnp.pad(jnp.stack(in_order(me, [val[key] for key in extra_keys])), ((0, 0), (0, pad - decodes), (0, 0))), y_pad]
                made = project_out(c, tp_size, pad, val['token'], where, val['c', c], [val[key] for key in w_keys], x_prompt[0], val['mlp_gain'], extras, [val[key] for key in buffers])
                buffers[:] = ['normed', 'h']
                val['normed'], val['h'], val['token'] = made[0], made[1], made[-1]
                if c == last:
                    val['hx'] = made[2]
                return ['token']
            val['out'], val['y'] = mlp(val['token'], val['normed'], val['hx'], jnp.transpose(w_gate_up[0], (1, 2, 0)), w_down[0], val['h'], tp_size)
            return ['y']

        def transfer(name):
            if name[0] == 'k':
                d = int(name[1])
                tie(thread + [('kv', d)])
                route = [(t * side_size + s, ((t + d) % tp_size) * side_size + (s + 1) % side_size) for t in range(tp_size) for s in range(side_size)]
                val['landed', d] = lax.ppermute(val['kv', d], ('tp', 'side'), route)
                return
            if name[0] == 'l':
                d = int(name[1])
                tie(thread + [('landed', d)])
                for which in range(2):
                    val['cache', which] = lax.dynamic_update_slice(val['cache', which], val['landed', d][which][:, None], (0, lax.rem(me - d + tp_size, tp_size), 0, 0))
                return
            bases = [0] if name == 'w2' else list(range(0, seats, 2))
            tie(thread + [('w', base) for base in bases])
            for mask in (range(2, seats, 2) if name == 'w2' else [1]):
                for base in bases:
                    val['w', base ^ mask] = swap(val['w', base], mask)

        val['token'] = jnp.zeros(TOKEN.shape, TOKEN.dtype)
        thread = ['token']
        for name in ORDER:
            if name[0] in 'QTKDOB':
                made = compute(name)
                thread = thread + made if name in ('K', 'D1', 'D2') else made
            else:
                transfer(name)

        caches = [val['cache', which].reshape(1, 1, rows, tp_size * heads_local, head_dim) for which in range(2)]
        return (val['out'][None], val['y'][:decodes], caches[0], caches[1], val['key_now'][None], val['value_now'][None])

    cache_spec = P(None, group_axes, 'tp', None, None)
    in_specs = (P(group_axes, None, None), P(group_axes), P(group_axes, None), P(group_axes), cache_spec, cache_spec, P(), P(None, None, 'tp', None, None), P(None, 'tp', None, None, None), P(), P(None, None, None, 'tp'), P(None, 'tp', None))
    out_specs = (P(group_axes, None, None), P(group_axes, None), cache_spec, cache_spec, cache_spec, cache_spec)
    return jax.shard_map(device_fn, mesh=mesh, in_specs=in_specs, out_specs=out_specs, check_vma=False)
```

```python
import functools

import jax
import jax.numpy as jnp
from jax import lax
from jax.experimental import pallas as pl
from jax.experimental.pallas import tpu as pltpu
from jax.sharding import PartitionSpec as P


ROPE_BASE = 10000.0
NORM_EPS = 1e-5

ORDER = (
    'Q0', 'T0', 'G0', 'T1', 'w2', 'Q1', 'T2', 'G12', 'T3', 'G3', 'D1', 'K', 'D2', 'w3', 'O012', 'k2', 'k1', 'k3', 'k0',
    'O3', 'B', 'l0', 'l2', 'l1', 'l3',
)


def rms_scale(values_f32, gain_f32):
    inv_rms = lax.rsqrt(jnp.mean(values_f32 * values_f32, axis=-1, keepdims=True) + NORM_EPS)
    return (values_f32 * inv_rms * gain_f32).astype(jnp.bfloat16)


def rope_tables(positions, head_dim):
    half_dim = head_dim // 2
    inv_freq = ROPE_BASE ** (-2.0 * jnp.arange(half_dim, dtype=jnp.float32) / head_dim)
    angles = positions.astype(jnp.float32)[:, None] * inv_freq[None, :]
    cos_table = jnp.cos(angles)
    sin_table = jnp.sin(angles)
    return jnp.concatenate([cos_table, cos_table], axis=1), jnp.concatenate([-sin_table, sin_table], axis=1)


def qkv_kernel(head_dim, extra, *refs):
    x_ref, gain_ref, wq_ref, wk_ref, wv_ref, cos_ref, sin_ref = refs[:7]
    extra_refs = refs[7:10] if extra else None
    normed_ref = refs[-1]
    q_ref, k_ref, v_ref, token_ref = refs[-5 - 3 * extra:-1 - 3 * extra]
    extra_outs = refs[-4:-1] if extra else (None,) * 3
    rows = x_ref.shape[0]
    chunk = pl.program_id(1)

    @pl.when(pl.program_id(0) == 0)
    def _():
        gain = gain_ref[...].astype(jnp.float32)
        normed_ref[chunk, :rows] = rms_scale(x_ref[...].astype(jnp.float32), gain)
        if extra:
            normed_ref[chunk, rows:] = rms_scale(extra_refs[0][...].astype(jnp.float32), gain)
        token_ref[...] = jnp.zeros_like(token_ref)

    cos, sin = cos_ref[...], sin_ref[...]
    if extra:
        cos = jnp.concatenate([cos, extra_refs[1][...]], axis=0)
        sin = jnp.concatenate([sin, extra_refs[2][...]], axis=0)
    for w_ref, out_ref, extra_out in zip((wq_ref, wk_ref, wv_ref), (q_ref, k_ref, v_ref), extra_outs):
        acc = jnp.dot(normed_ref[chunk], w_ref[...], preferred_element_type=jnp.float32)
        for start in range(0, acc.shape[1], head_dim):
            vals = acc[:, start:start + head_dim]
            if out_ref is not v_ref:
                vals = vals * cos + pltpu.roll(vals, head_dim // 2, 1) * sin
            out_ref[:, start:start + head_dim] = vals[:rows].astype(out_ref.dtype)
            if extra:
                extra_out[:, start:start + head_dim] = vals[rows:].astype(out_ref.dtype)


TOKEN = jax.ShapeDtypeStruct((8, 128), jnp.float32)


def project_qkv(half, rows, token, x, extra_rows, gain, w_all, tables, extra_tables, head_dim):
    depth = x.shape[1]
    width = w_all.shape[1] // 3
    block = 2 * head_dim
    steps = width // block
    extra = extra_rows is not None
    extras = [extra_rows, *extra_tables] if extra else []
    pad = extra_rows.shape[0] if extra else 0
    bf16 = jnp.bfloat16
    whole = lambda shape: pl.BlockSpec(shape, lambda n, c: (0, 0), pipeline_mode=pl.Buffered(1))
    columns = lambda part: pl.BlockSpec((depth, block), lambda n, c: (0, part * steps + n))
    table = pl.BlockSpec((rows, head_dim), lambda n, c: (2 * half + c, 0))
    extra_outs = [jax.ShapeDtypeStruct((pad, width), bf16)] * 3 if extra else []
    return pl.pallas_call(
        functools.partial(qkv_kernel, head_dim, extra),
        out_shape=[jax.ShapeDtypeStruct((2 * rows, width), bf16)] * 3 + [TOKEN] + extra_outs,
        grid=(steps, 2),
        in_specs=[
            pl.BlockSpec((rows, depth), lambda n, c: (2 * half + lax.select(n == 0, c, 1), 0)),
            whole((1, depth)),
            columns(0),
            columns(1),
            columns(2),
            table,
            table,
        ] + [whole(e.shape) for e in extras] + [pl.BlockSpec(memory_space=pl.ANY)],
        out_specs=[pl.BlockSpec((rows, block), lambda n, c: (c, n))] * 3 + [whole(TOKEN.shape)] + [pl.BlockSpec((pad, block), lambda n, c: (0, n))] * len(extra_outs),
        scratch_shapes=[pltpu.VMEM((2, rows + pad, depth), bf16)],
        compiler_params=pltpu.CompilerParams(dimension_semantics=("arbitrary", "arbitrary"), vmem_limit_bytes=56 << 20),
        cost_estimate=pl.CostEstimate(flops=12 * rows * depth * width, bytes_accessed=2 * (2 * rows * depth + 3 * depth * width + 6 * rows * width), transcendentals=0),
        name="project_qkv",
    )(x, gain, w_all, w_all, w_all, *tables, *extras, token)


def attend_kernel(chunk, first_checked, q_rows, slen_ref, *refs):
    q_ref = refs[0]
    k_refs = refs[1:chunk + 2]
    v_refs = refs[chunk + 2:2 * chunk + 3]
    out_ref, token_ref = refs[-2:]
    token_ref[...] = jnp.zeros_like(token_ref)
    rows, head_dim = q_ref.shape
    scale = head_dim ** -0.5
    limit = slen_ref[0]
    for start in range(0, rows, q_rows):
        query = q_ref[start:start + q_rows, :]
        scores = []
        values = []
        for part in range(chunk + 1):
            keys = rows if part < chunk else start + q_rows
            score = lax.dot_general(query, k_refs[part][:keys, :], (((1,), (1,)), ((), ())), preferred_element_type=jnp.float32) * scale
            key_pos = lax.broadcasted_iota(jnp.int32, score.shape, 1)
            if part == chunk:
                allowed = key_pos <= lax.broadcasted_iota(jnp.int32, score.shape, 0) + start
                if part >= first_checked:
                    allowed = allowed & (key_pos < limit - part * rows)
                score = jnp.where(allowed, score, -1e30)
            elif part >= first_checked:
                score = jnp.where(key_pos < limit - part * rows, score, -1e30)
            scores.append(score)
            values.append(v_refs[part][:keys, :])
        peak = functools.reduce(jnp.maximum, [jnp.max(score, axis=-1, keepdims=True) for score in scores])
        total = jnp.zeros((q_rows, 1), jnp.float32)
        mixed = jnp.zeros((q_rows, head_dim), jnp.float32)
        for score, value in zip(scores, values):
            weight = jnp.exp(score - peak)
            total = total + jnp.sum(weight, axis=-1, keepdims=True)
            mixed = mixed + jnp.dot(weight.astype(jnp.bfloat16), value, preferred_element_type=jnp.float32)
        out_ref[start:start + q_rows, :] = (mixed / total).astype(out_ref.dtype)


def attend(chunk, chunks, rows, token, s_len, queries, keys, values, head_dim):
    width = queries[0].shape[1]
    heads = width // head_dim

    pick = lambda c: pl.BlockSpec((rows, head_dim), lambda h, slen: (c % 2, h))
    every = range(chunk + 1)
    total_keys = rows * (chunk + 1)
    return pl.pallas_call(
        functools.partial(attend_kernel, chunk, chunks // 2, min(256, rows)),
        out_shape=[jax.ShapeDtypeStruct((rows, width), jnp.bfloat16), TOKEN],
        grid_spec=pltpu.PrefetchScalarGridSpec(
            num_scalar_prefetch=1,
            grid=(heads,),
            in_specs=[pick(c) for c in (chunk, *every, *every)] + [pl.BlockSpec(memory_space=pl.ANY)],
            out_specs=[pick(0), pl.BlockSpec(TOKEN.shape, lambda h, slen: (0, 0))],
        ),
        compiler_params=pltpu.CompilerParams(dimension_semantics=("arbitrary",), vmem_limit_bytes=48 << 20),
        cost_estimate=pl.CostEstimate(flops=8 * heads * rows * total_keys * head_dim, bytes_accessed=2 * width * (2 * total_keys + 2 * rows), transcendentals=heads * rows * total_keys),
    )(s_len, queries[chunk // 2], *[keys[c // 2] for c in every], *[values[c // 2] for c in every], token)


def output_kernel(size, heads, contexts, extra, aliased, where_ref, *refs):
    context_refs, refs = refs[:contexts], refs[contexts:]
    w_refs, refs = refs[:heads], refs[heads:]
    x_ref, gain_ref, refs = refs[0], refs[1], refs[2:]
    if extra:
        context_x_ref, x_x_ref, refs = refs[0], refs[1], refs[2:]
    refs = refs[1:]
    if aliased:
        refs = refs[2:]
    normed_ref, hidden_ref, refs = refs[0], refs[1], refs[2:]
    if extra:
        hidden_x_ref, refs = refs[0], refs[1:]
    token_ref, full_ref, square_ref = refs
    rows, depth = hidden_ref.shape
    head_dim, block = w_refs[0].shape[1:]
    chunk, step = pl.program_id(0), pl.program_id(1)

    @pl.when(step == 0)
    def _():
        square_ref[...] = jnp.zeros_like(square_ref)
        token_ref[...] = jnp.zeros_like(token_ref)
        for number, context_ref in enumerate(context_refs):
            @pl.when((chunk == 0) if number == 0 else (chunk > 0))
            def _():
                for r in range(heads):
                    columns = pl.ds(pl.multiple_of(lax.bitwise_xor(where_ref[0], r) * head_dim, head_dim), head_dim)
                    for t in range(size):
                        there = (r * size + t) * head_dim
                        full_ref[:rows, there:there + head_dim] = context_ref[t, 0, :, columns]
                        if extra:
                            full_ref[rows:, there:there + head_dim] = context_x_ref[t, :, columns]

    w_block = jnp.concatenate([w_ref[...].reshape(size * head_dim, block) for w_ref in w_refs], axis=0)
    acc = jnp.dot(full_ref[...], w_block, preferred_element_type=jnp.float32)
    columns = pl.ds(pl.multiple_of(step * block, block), block)
    hidden = (x_ref[...].astype(jnp.float32) + acc[:rows]).astype(jnp.bfloat16)
    hidden_ref[:, columns] = hidden
    hidden_f32 = hidden.astype(jnp.float32)
    square_ref[:rows] += jnp.sum(hidden_f32 * hidden_f32, axis=-1, keepdims=True)
    if extra:
        hidden = (x_x_ref[...].astype(jnp.float32) + acc[rows:]).astype(jnp.bfloat16)
        hidden_x_ref[:, columns] = hidden
        hidden_f32 = hidden.astype(jnp.float32)
        square_ref[rows:] += jnp.sum(hidden_f32 * hidden_f32, axis=-1, keepdims=True)

    @pl.when(step == pl.num_programs(1) - 1)
    def _():
        half = rows // 2
        inv_rms = lax.rsqrt(square_ref[...] / depth + NORM_EPS)
        for start in range(0, depth, block):
            gain = gain_ref[:, start:start + block].astype(jnp.float32)
            for part in range(2):
                lo, hi = part * half, (part + 1) * half
                normed_ref[part, :half, start:start + block] = (hidden_ref[lo:hi, start:start + block].astype(jnp.float32) * inv_rms[lo:hi] * gain).astype(jnp.bfloat16)
                if extra and part == 1:
                    normed_ref[part, half:, start:start + block] = (hidden_x_ref[:, start:start + block].astype(jnp.float32) * inv_rms[rows:] * gain).astype(jnp.bfloat16)
                else:
                    normed_ref[part, half:, start:start + block] = jnp.zeros((normed_ref.shape[1] - half, block), jnp.bfloat16)


def project_out(first, count, chunks, pad, token, where, contexts, w_heads, x, gain, extras, buffers):
    rows, width = contexts[0].shape[2:]
    depth = x.shape[1]
    heads = len(w_heads)
    size, head_dim = w_heads[0].shape[:2]
    block = min(512, depth)
    total = rows + (pad if extras else 0)
    whole = lambda shape: pl.BlockSpec(shape, lambda c, n, where: (0,) * len(shape), pipeline_mode=pl.Buffered(1))
    in_specs = [whole(contexts[0].shape)]
    if count > 1:
        in_specs.append(pl.BlockSpec((size, 1, rows, width), lambda c, n, where: (0, lax.max(c - 1, 0), 0, 0)))
    in_specs += [pl.BlockSpec((size, head_dim, block), lambda c, n, where: (0, 0, n))] * heads
    in_specs += [pl.BlockSpec((rows, block), lambda c, n, where: (first + c, n)), whole((1, depth))]
    out_shape = [jax.ShapeDtypeStruct((2 * chunks, rows // 2 + pad, depth), jnp.bfloat16), jax.ShapeDtypeStruct((rows * chunks, depth), jnp.bfloat16)]
    mode = {} if count > 1 else dict(pipeline_mode=pl.Buffered(1))
    out_specs = [
        pl.BlockSpec((2, rows // 2 + pad, depth), lambda c, n, where: (first + c, 0, 0), **mode),
        pl.BlockSpec((rows, depth), lambda c, n, where: (first + c, 0), **mode),
    ]
    if extras:
        in_specs += [whole(extras[0].shape), pl.BlockSpec((pad, block), lambda c, n, where: (0, n))]
        out_shape.append(jax.ShapeDtypeStruct((pad, depth), jnp.bfloat16))
        out_specs.append(whole((pad, depth)))
    in_specs.append(pl.BlockSpec(memory_space=pl.ANY))
    out_shape.append(TOKEN)
    out_specs.append(whole(TOKEN.shape))
    aliases = {}
    if buffers:
        aliases = {1 + len(in_specs): 0, 2 + len(in_specs): 1}
        in_specs += [pl.BlockSpec(memory_space=pl.ANY)] * 2
    return pl.pallas_call(
        functools.partial(output_kernel, size, heads, len(contexts), bool(extras), bool(buffers)),
        out_shape=out_shape,
        grid_spec=pltpu.PrefetchScalarGridSpec(
            num_scalar_prefetch=1,
            grid=(count, depth // block),
            in_specs=in_specs,
            out_specs=out_specs,
            scratch_shapes=[pltpu.VMEM((total, size * width), jnp.bfloat16), pltpu.VMEM((total, 1), jnp.float32)],
        ),
        input_output_aliases=aliases,
        compiler_params=pltpu.CompilerParams(dimension_semantics=("arbitrary", "arbitrary"), vmem_limit_bytes=60 << 20),
        cost_estimate=pl.CostEstimate(flops=2 * count * total * size * width * depth, bytes_accessed=2 * count * (size * width * depth + 4 * rows * width + 3 * total * depth), transcendentals=0),
        name="project_out",
    )(where, *contexts, *w_heads, x, gain, *extras, token, *buffers)


def mlp_kernel(size, chunk_rows, ff_steps, slots, token_ref, normed_ref, hextra_ref, wgu_ref, wd_ref, h_ref, out_ref, y_ref,
               acc, landed, outgoing, finished, residual, others, activated,
               rs_send, rs_recv, ag_send, ag_recv, keep_sem, h_sem, x_send, x_recv, credit):
    step = pl.program_id(0)
    me = lax.axis_index('tp')
    depth = wd_ref.shape[1]
    chunks = (out_ref.shape[0] // chunk_rows)
    piece = outgoing.shape[2]
    per_chunk = chunk_rows // (2 * piece)
    pieces = chunks * per_chunk
    subs = per_chunk // ff_steps
    last = size - 1

    @pl.when(step == 0)
    def _():
        barrier = pltpu.get_barrier_semaphore()
        for d in range(1, size):
            pl.semaphore_signal(barrier, inc=1, device_id={'tp': lax.rem(me + d, size)}, device_id_type=pl.DeviceIdType.MESH)
        pl.semaphore_wait(barrier, size - 1)

    def own_part(chain, m):
        start = pl.multiple_of(chain * (chunk_rows // 2) + lax.rem(m, per_chunk) * piece, piece)
        return acc.at[lax.rem(lax.div(m, per_chunk), 3), pl.ds(start, piece)]

    def out_rows(chain, m):
        start = pl.multiple_of(lax.div(m, per_chunk) * chunk_rows + chain * (chunk_rows // 2) + lax.rem(m, per_chunk) * piece, piece)
        return pl.ds(start, piece)

    def exchange(slot):
        for chain in range(2):
            place = me if chain == 0 else last - me
            nearer = me - 1 if chain == 0 else me + 1
            farther = me + 1 if chain == 0 else me - 1

            def sum_copy(source, m):
                return pltpu.make_async_remote_copy(
                    src_ref=source, dst_ref=landed.at[chain, lax.rem(m, slots)], send_sem=rs_send.at[chain, lax.rem(m, 4)],
                    recv_sem=rs_recv.at[chain, lax.rem(m, slots)], device_id={'tp': nearer}, device_id_type=pl.DeviceIdType.MESH)

            def keep_copy(m):
                return pltpu.make_async_copy(finished.at[chain, lax.rem(m, 2)], out_ref.at[out_rows(chain, m)], keep_sem.at[chain, lax.rem(m, 2)])

            def h_copy(m):
                return pltpu.make_async_copy(h_ref.at[out_rows(chain, m)], residual.at[chain, lax.rem(m, 2)], h_sem.at[chain, lax.rem(m, 2)])

            def back_copy(source, m):
                return pltpu.make_async_remote_copy(
                    src_ref=source, dst_ref=out_ref.at[out_rows(chain, m)], send_sem=ag_send.at[chain, lax.rem(m, 4)],
                    recv_sem=ag_recv.at[chain, lax.rem(m, 8)], device_id={'tp': farther}, device_id_type=pl.DeviceIdType.MESH)

            @pl.when((place == last) & (slot >= 0) & (slot < pieces))
            def _():
                @pl.when(slot >= 4)
                def _():
                    sum_copy(own_part(chain, slot - 4), slot - 4).wait_send()

                @pl.when(slot >= slots)
                def _():
                    pl.semaphore_wait(credit.at[chain], 1)

                sum_copy(own_part(chain, slot), slot).start()

            for hops in range(1, last):
                m = slot - (last - hops)

                @pl.when((place == hops) & (m >= 0) & (m < pieces))
                def _():
                    @pl.when(m >= 2)
                    def _():
                        sum_copy(outgoing.at[chain, lax.rem(m, 2)], m - 2).wait_send()

                    sum_copy(outgoing.at[chain, lax.rem(m, 2)], m).wait_recv()
                    outgoing[chain, lax.rem(m, 2)] = landed[chain, lax.rem(m, slots)] + own_part(chain, m)[...]

                    @pl.when(m + slots < pieces)
                    def _():
                        pl.semaphore_signal(credit.at[chain], inc=1, device_id={'tp': farther}, device_id_type=pl.DeviceIdType.MESH)

                    @pl.when(m >= slots)
                    def _():
                        pl.semaphore_wait(credit.at[chain], 1)

                    sum_copy(outgoing.at[chain, lax.rem(m, 2)], m).start()

            m = slot - last

            @pl.when((place == 0) & (slot == 0))
            def _():
                h_copy(0).start()

            @pl.when((place == 0) & (m >= 0) & (m < pieces))
            def _():
                @pl.when(m + 1 < pieces)
                def _():
                    h_copy(m + 1).start()

                @pl.when(m >= 2)
                def _():
                    keep_copy(m - 2).wait()
                    back_copy(finished.at[chain, lax.rem(m, 2)], m - 2).wait_send()

                h_copy(m).wait()
                sum_copy(outgoing.at[chain, lax.rem(m, 2)], m).wait_recv()
                total = landed[chain, lax.rem(m, slots)] + own_part(chain, m)[...]
                finished[chain, lax.rem(m, 2)] = (residual[chain, lax.rem(m, 2)].astype(jnp.float32) + total).astype(jnp.bfloat16)

                @pl.when(m + slots < pieces)
                def _():
                    pl.semaphore_signal(credit.at[chain], inc=1, device_id={'tp': farther}, device_id_type=pl.DeviceIdType.MESH)

                keep_copy(m).start()
                back_copy(finished.at[chain, lax.rem(m, 2)], m).start()

        for chain in range(2):
            place = me if chain == 0 else last - me
            farther = me + 1 if chain == 0 else me - 1

            def relay_copy(m):
                return pltpu.make_async_remote_copy(
                    src_ref=out_ref.at[out_rows(chain, m)], dst_ref=out_ref.at[out_rows(chain, m)], send_sem=ag_send.at[chain, lax.rem(m, 4)],
                    recv_sem=ag_recv.at[chain, lax.rem(m, 8)], device_id={'tp': farther}, device_id_type=pl.DeviceIdType.MESH)

            for hops in range(1, size):
                m = slot - last - 2 * hops

                @pl.when((place == hops) & (m >= 0) & (m < pieces))
                def _():
                    relay_copy(m).wait_recv()
                    if hops < last:
                        @pl.when(m >= 4)
                        def _():
                            relay_copy(m - 4).wait_send()

                        relay_copy(m).start()

    def extra_copy(d):
        return pltpu.make_async_remote_copy(
            src_ref=acc.at[(chunks - 1) % 3, pl.ds(chunk_rows, others.shape[1])], dst_ref=others.at[d], send_sem=x_send.at[d - 1],
            recv_sem=x_recv.at[d - 1], device_id={'tp': lax.rem(me + d, size)}, device_id_type=pl.DeviceIdType.MESH)

    @pl.when(step == chunks * ff_steps)
    def _():
        others[0] = acc[(chunks - 1) % 3, chunk_rows:chunk_rows + others.shape[1]]
        for d in range(1, size):
            extra_copy(d).start()

    @pl.when(step == chunks * ff_steps + 4)
    def _():
        for d in range(1, size):
            extra_copy(d).wait()
        total = others[lax.rem(me, size)]
        for j in range(1, size):
            total = total + others[lax.rem(me + size - j, size)]
        y_ref[...] = (hextra_ref[:others.shape[1]].astype(jnp.float32) + total).astype(jnp.bfloat16)

    chunk = lax.div(step, ff_steps)
    block = min(1024, depth)

    def compute_gate():
        rows_in = normed_ref[0]
        dims = (((1,), (1,)), ((), ()))
        gate = lax.dot_general(rows_in, wgu_ref[0], dims, preferred_element_type=jnp.float32)
        up = lax.dot_general(rows_in, wgu_ref[1], dims, preferred_element_type=jnp.float32)
        activated[...] = (gate * jax.nn.sigmoid(gate) * up).astype(jnp.bfloat16)

    def compute_down():
        first = lax.rem(step, ff_steps) == 0
        for start in range(0, depth, block):
            part = jnp.dot(activated[...], wd_ref[:, start:start + block], preferred_element_type=jnp.float32)

            @pl.when(first)
            def _():
                acc[lax.rem(chunk, 3), :, start:start + block] = part

            @pl.when(jnp.logical_not(first))
            def _():
                acc[lax.rem(chunk, 3), :, start:start + block] += part

    for sub in range(subs):
        exchange((step - ff_steps) * subs + sub)
        for part in range(2):
            if part * subs // 2 == sub:
                pl.when(step < chunks * ff_steps)((compute_gate, compute_down)[part])

    @pl.when(step == pl.num_programs(0) - 1)
    def _():
        for chain in range(2):
            place = me if chain == 0 else last - me
            nearer = me - 1 if chain == 0 else me + 1
            farther = me + 1 if chain == 0 else me - 1

            def sent(m):
                return pltpu.make_async_remote_copy(
                    src_ref=outgoing.at[chain, m % 2], dst_ref=landed.at[chain, m % slots], send_sem=rs_send.at[chain, m % 4],
                    recv_sem=rs_recv.at[chain, m % slots], device_id={'tp': nearer}, device_id_type=pl.DeviceIdType.MESH)

            def returned(m):
                return pltpu.make_async_remote_copy(
                    src_ref=finished.at[chain, m % 2], dst_ref=out_ref.at[pl.ds(0, piece)], send_sem=ag_send.at[chain, m % 4],
                    recv_sem=ag_recv.at[chain, m % 8], device_id={'tp': farther}, device_id_type=pl.DeviceIdType.MESH)

            @pl.when(place == last)
            def _():
                for m in range(pieces - 4, pieces):
                    sent(m).wait_send()

            @pl.when((place > 0) & (place < last))
            def _():
                for m in range(pieces - 2, pieces):
                    sent(m).wait_send()
                for m in range(pieces - 4, pieces):
                    returned(m).wait_send()

            @pl.when(place == 0)
            def _():
                for m in range(pieces - 2, pieces):
                    pltpu.make_async_copy(finished.at[chain, m % 2], out_ref.at[pl.ds(0, piece)], keep_sem.at[chain, m % 2]).wait()
                    returned(m).wait_send()


SUBSLOTS = 2


def mlp(token, normed, hextra, w_gate_up, w_down, hidden, size):
    chunks, lines, depth = normed.shape
    rows = hidden.shape[0]
    chunk_rows = rows // chunks
    ff = w_down.shape[0]
    ff_steps = 4
    piece = chunk_rows // (8 * SUBSLOTS)
    slots = 4
    pieces = chunks * 4 * SUBSLOTS
    extra = lines - chunk_rows
    seen = min(8, extra)
    steps = chunks * ff_steps
    total_steps = ff_steps + -(-(pieces + 3 * (size - 1)) // SUBSLOTS)
    ff_block = ff // ff_steps
    at_ff = lambda g: lax.select(g < steps, lax.rem(g, ff_steps), ff_steps - 1)
    at_chunk = lambda g: lax.min(lax.div(g, ff_steps), chunks - 1)
    f32, bf16 = jnp.float32, jnp.bfloat16
    return pl.pallas_call(
        functools.partial(mlp_kernel, size, chunk_rows, ff_steps, slots),
        out_shape=[jax.ShapeDtypeStruct((rows, depth), bf16), jax.ShapeDtypeStruct((seen, depth), bf16)],
        grid=(total_steps,),
        in_specs=[
            pl.BlockSpec(memory_space=pl.ANY),
            pl.BlockSpec((1, lines, depth), lambda g: (at_chunk(g), 0, 0)),
            pl.BlockSpec((extra, depth), lambda g: (0, 0), pipeline_mode=pl.Buffered(1)),
            pl.BlockSpec((2, ff_block, depth), lambda g: (0, at_ff(g), 0)),
            pl.BlockSpec((ff_block, depth), lambda g: (at_ff(g), 0)),
            pl.BlockSpec(memory_space=pl.ANY),
        ],
        out_specs=[pl.BlockSpec(memory_space=pl.ANY), pl.BlockSpec((seen, depth), lambda g: (0, 0), pipeline_mode=pl.Buffered(1))],
        scratch_shapes=[
            pltpu.VMEM((3, lines, depth), f32),
            pltpu.VMEM((2, slots, piece, depth), f32),
            pltpu.VMEM((2, 2, piece, depth), f32),
            pltpu.VMEM((2, 2, piece, depth), bf16),
            pltpu.VMEM((2, 2, piece, depth), bf16),
            pltpu.VMEM((size, seen, depth), f32),
            pltpu.VMEM((lines, ff_block), bf16),
            pltpu.SemaphoreType.DMA((2, 4)),
            pltpu.SemaphoreType.DMA((2, slots)),
            pltpu.SemaphoreType.DMA((2, 4)),
            pltpu.SemaphoreType.DMA((2, 8)),
            pltpu.SemaphoreType.DMA((2, 2)),
            pltpu.SemaphoreType.DMA((2, 2)),
            pltpu.SemaphoreType.DMA((size - 1,)),
            pltpu.SemaphoreType.DMA((size - 1,)),
            pltpu.SemaphoreType.REGULAR((2,)),
        ],
        compiler_params=pltpu.CompilerParams(dimension_semantics=("arbitrary",), vmem_limit_bytes=63 << 20, collective_id=0, has_side_effects=True),
        cost_estimate=pl.CostEstimate(flops=6 * rows * depth * ff, bytes_accessed=6 * chunks * depth * ff, transcendentals=rows * ff),
        name="mlp",
    )(token, normed, hextra, w_gate_up, w_down, hidden)


def pick_by(index, options):
    result = options[0]
    for place in range(1, len(options)):
        result = jnp.where(index == place, options[place], result)
    return result


def solution(mesh):
    side_size = mesh.shape['side']
    tp_size = mesh.shape['tp']
    seats = mesh.shape['pair'] * side_size
    group_axes = ('pair', 'side')
    last = tp_size - 1

    def cyclic(value, d):
        return lax.ppermute(value, 'tp', [(t, (t + d) % tp_size) for t in range(tp_size)])

    def swap(value, mask):
        return lax.ppermute(value, group_axes, [(q, q ^ mask) for q in range(seats)])

    def in_order(me, copies):
        return [pick_by(me, [copies[(t - j) % tp_size] for t in range(tp_size)]) for j in range(tp_size)]

    def device_fn(x_prompt, s_len, y_tok, c_len, k_cache, v_cache, attn_gain, w_qkv, w_out, mlp_gain, w_gate_up, w_down):
        me = lax.axis_index('tp')
        seat = lax.axis_index('pair') * side_size + lax.axis_index('side')
        where = seat.reshape(1).astype(jnp.int32)
        seq_len, depth = x_prompt.shape[1:]
        heads_local = w_qkv.shape[2]
        head_dim = w_qkv.shape[4]
        width = heads_local * head_dim
        rows = seq_len // tp_size
        decodes = y_tok.shape[0]
        pad = 16
        cache_local = k_cache.shape[2]
        val = {}

        def tie(keys):
            keys = list(dict.fromkeys(keys))
            for key, value in zip(keys, lax.optimization_barrier(tuple(val[key] for key in keys))):
                val[key] = value

        val['w', 0] = lax.all_gather(lax.dynamic_index_in_dim(w_out[0, :, 0], seat, 0, keepdims=False), 'tp', axis=0, tiled=False)

        val['w_all'] = jnp.swapaxes(w_qkv[0], 1, 2).reshape(depth, 3 * width)
        tables = rope_tables(jnp.arange(seq_len, dtype=jnp.int32), head_dim)
        extra_tables = rope_tables(jnp.concatenate([c_len, jnp.zeros((pad - decodes,), jnp.int32)]), head_dim)
        y_pad = jnp.concatenate([y_tok, jnp.zeros((pad - decodes, depth), y_tok.dtype)])
        val['gain'], val['s_len'], val['mlp_gain'] = attn_gain, s_len, mlp_gain
        val['valid'] = (jnp.arange(seq_len) < s_len[0]).astype(jnp.bfloat16)
        for which in range(2):
            val['cache', which] = jnp.zeros((rows, tp_size, heads_local, head_dim), jnp.bfloat16)
        buffers = []
        qkv = []

        def compute(name):
            kind = name[0]
            c = int(name[1:]) if name[1:].isdigit() else 0
            if kind == 'Q':
                tie(thread + ['gain'])
                made = project_qkv(c, rows, val['token'], x_prompt[0], y_pad if c == 0 else None, val['gain'], val['w_all'], tables, extra_tables, head_dim)
                val['token'] = made[3]
                qkv.append(made[:3])
                if c == 0:
                    val['dq', 0] = jnp.stack([part[:decodes].reshape(decodes, heads_local, head_dim) for part in made[4:]])
                    for d in range(1, tp_size):
                        val['dq', d] = cyclic(val['dq', 0], d)
                return ['token']
            if kind == 'T':
                tie(thread + ['s_len'])
                val['context', c], val['token'] = attend(c, tp_size, rows, val['token'], val['s_len'], *zip(*qkv), head_dim)
                return ['token']
            if kind == 'G':
                val['gathered', name[1:]] = lax.all_gather(jnp.stack([val['context', int(digit)] for digit in name[1:]]), 'tp', axis=0, tiled=False)
                return ['token']
            if kind == 'K':
                tie(thread + ['valid'])
                for d in range(tp_size):
                    made = []
                    keep = pick_by(me, [val['valid'][((t + d) % tp_size) * rows:((t + d) % tp_size + 1) * rows] for t in range(tp_size)])
                    for which in (1, 2):
                        rows_d = pick_by(me, [qkv[(t + d) % tp_size // 2][which][(t + d) % tp_size % 2 * rows:][:rows].reshape(rows, heads_local, head_dim) for t in range(tp_size)])
                        made.append(rows_d * keep[:, None, None])
                    val['kv', d] = jnp.stack(made)
                return []
            if name == 'D1':
                tie(thread + [('dq', d) for d in range(tp_size)])
                dec_full = jnp.concatenate(in_order(me, [val['dq', d] for d in range(tp_size)]), axis=2)
                cache_pos = me * cache_local + jnp.arange(cache_local)
                write_mask = (cache_pos[None, :] == c_len[:, None])[:, :, None, None]
                allowed = (cache_pos[None, :] <= c_len[:, None])[:, None, :]
                key_now = jnp.where(write_mask, dec_full[1][:, None], k_cache[0])
                value_now = jnp.where(write_mask, dec_full[2][:, None], v_cache[0])
                val['key_now'], val['value_now'] = key_now, value_now
                scores = jnp.einsum('bkh,btkh->bkt', dec_full[0], key_now, preferred_element_type=jnp.float32) * head_dim ** -0.5
                scores = jnp.where(allowed, scores, -1e30)
                peak = jnp.max(scores, axis=-1, keepdims=True)
                weights = jnp.exp(scores - peak)
                total = jnp.sum(weights, axis=-1, keepdims=True)
                mixed = jnp.einsum('bkt,btkh->bkh', weights.astype(jnp.bfloat16), value_now, preferred_element_type=jnp.float32)
                packed = jnp.stack([mixed, jnp.broadcast_to(peak, mixed.shape), jnp.broadcast_to(total, mixed.shape)])
                packed = packed.reshape(3, decodes, tp_size, heads_local, head_dim)
                for d in range(tp_size):
                    share = lax.dynamic_index_in_dim(packed, lax.rem(me + d, tp_size), 2, keepdims=False)
                    val['ds', d] = share if d == 0 else cyclic(share, d)
                return [('ds', 0)]
            if name == 'D2':
                tie(thread + [('ds', d) for d in range(tp_size)])
                shares = [val['ds', d] for d in range(tp_size)]
                top = functools.reduce(jnp.maximum, [share[1] for share in shares])
                factors = [jnp.exp(share[1] - top) for share in shares]
                dec_mixed = sum(share[0] * factor for share, factor in zip(shares, factors))
                dec_total = sum(share[2] * factor for share, factor in zip(shares, factors))
                val['dc', 0] = (dec_mixed / dec_total).astype(jnp.bfloat16).reshape(decodes, width)
                for d in range(1, tp_size):
                    val['dc', d] = cyclic(val['dc', 0], d)
                return [('dc', 0)]
            if kind == 'O':
                w_keys = [('w', r) for r in range(seats)]
                final = c == last
                parts = [('gathered', '3')] if final else [('gathered', '0'), ('gathered', '12')]
                extra_keys = [('dc', d) for d in range(tp_size)] if final else []
                tie(thread + ['mlp_gain'] + parts + extra_keys + ([] if final else w_keys))
                extras = []
                if final:
                    extras = [jnp.pad(jnp.stack(in_order(me, [val[key] for key in extra_keys])), ((0, 0), (0, pad - decodes), (0, 0))), y_pad]
                made = project_out(last if final else 0, 1 if final else last, tp_size, pad, val['token'], where, [val[key] for key in parts], [val[key] for key in w_keys], x_prompt[0], val['mlp_gain'], extras, [val[key] for key in buffers])
                buffers[:] = ['normed', 'h']
                val['normed'], val['h'], val['token'] = made[0], made[1], made[-1]
                if final:
                    val['hx'] = made[2]
                return ['token']
            val['out'], val['y'] = mlp(val['token'], val['normed'], val['hx'], jnp.transpose(w_gate_up[0], (1, 2, 0)), w_down[0], val['h'], tp_size)
            return ['y']

        def transfer(name):
            if name[0] == 'k':
                d = int(name[1])
                tie(thread + [('kv', d)])
                route = [(t * side_size + s, ((t + d) % tp_size) * side_size + (s + 1) % side_size) for t in range(tp_size) for s in range(side_size)]
                val['landed', d] = lax.ppermute(val['kv', d], ('tp', 'side'), route)
                return
            if name[0] == 'l':
                d = int(name[1])
                tie(thread + [('landed', d)])
                for which in range(2):
                    val['cache', which] = lax.dynamic_update_slice(val['cache', which], val['landed', d][which][:, None], (0, lax.rem(me - d + tp_size, tp_size), 0, 0))
                return
            bases = [0] if name == 'w2' else list(range(0, seats, 2))
            kept = [] if name == 'w2' else [('kv', d) for d in range(tp_size)]
            tie(thread + kept + [('w', base) for base in bases])
            for mask in (range(2, seats, 2) if name == 'w2' else [1]):
                for base in bases:
                    val['w', base ^ mask] = swap(val['w', base], mask)

        val['token'] = jnp.zeros(TOKEN.shape, TOKEN.dtype)
        thread = ['token']
        for name in ORDER:
            if name[0] in 'QTGKDOB':
                made = compute(name)
                thread = thread + made if name in ('K', 'D1', 'D2') else made
            else:
                transfer(name)

        caches = [val['cache', which].reshape(1, 1, rows, tp_size * heads_local, head_dim) for which in range(2)]
        return (val['out'][None], val['y'][:decodes], caches[0], caches[1], val['key_now'][None], val['value_now'][None])

    cache_spec = P(None, group_axes, 'tp', None, None)
    in_specs = (P(group_axes, None, None), P(group_axes), P(group_axes, None), P(group_axes), cache_spec, cache_spec, P(), P(None, None, 'tp', None, None), P(None, 'tp', None, None, None), P(), P(None, None, None, 'tp'), P(None, 'tp', None))
    out_specs = (P(group_axes, None, None), P(group_axes, None), cache_spec, cache_spec, cache_spec, cache_spec)
    return jax.shard_map(device_fn, mesh=mesh, in_specs=in_specs, out_specs=out_specs, check_vma=False)
```

```python
import functools

import jax
import jax.numpy as jnp
from jax import lax
from jax.experimental import pallas as pl
from jax.experimental.pallas import tpu as pltpu
from jax.sharding import PartitionSpec as P


ROPE_BASE = 10000.0
NORM_EPS = 1e-5

ORDER = (
    'Q0', 'T0', 'G0', 'T1', 'w2', 'Q1', 'T2', 'G12', 'T3', 'G3', 'D1', 'K', 'D2', 'w3', 'O012', 'k0', 'k2', 'k1', 'k3',
    'O3', 'B', 'P',
)


def rms_scale(values_f32, gain_f32):
    inv_rms = lax.rsqrt(jnp.mean(values_f32 * values_f32, axis=-1, keepdims=True) + NORM_EPS)
    return (values_f32 * inv_rms * gain_f32).astype(jnp.bfloat16)


def rope_frequencies(head_dim):
    half_dim = head_dim // 2
    inv_freq = ROPE_BASE ** (-2.0 * jnp.arange(half_dim, dtype=jnp.float32) / head_dim)
    return jnp.concatenate([inv_freq, inv_freq])[None]


def rope_tables(positions, head_dim):
    angles = positions.astype(jnp.float32)[:, None] * rope_frequencies(head_dim)
    sign = jnp.where(jnp.arange(head_dim) < head_dim // 2, -1.0, 1.0)
    return jnp.cos(angles), jnp.sin(angles) * sign[None]


def rope_kernel(freq_ref, cos_ref, sin_ref):
    rows, head_dim = cos_ref.shape
    positions = lax.broadcasted_iota(jnp.int32, (rows, head_dim), 0) + pl.program_id(0) * rows
    angles = positions.astype(jnp.float32) * freq_ref[...]
    turns = jnp.floor(angles * 0.15915494309189535 + 0.5)
    angles = (angles - turns * 6.28125) - turns * 0.0019353071795864769
    sine = jnp.sin(angles)
    cos_ref[...] = jnp.cos(angles)
    sin_ref[...] = jnp.where(lax.broadcasted_iota(jnp.int32, (rows, head_dim), 1) < head_dim // 2, -sine, sine)


def rope_tables_upto(count, head_dim):
    rows = min(64, count)
    table = pl.BlockSpec((rows, head_dim), lambda n: (n, 0))
    return pl.pallas_call(
        rope_kernel,
        out_shape=[jax.ShapeDtypeStruct((count, head_dim), jnp.float32)] * 2,
        grid=(count // rows,),
        in_specs=[pl.BlockSpec((1, head_dim), lambda n: (0, 0))],
        out_specs=[table, table],
        name="rope_tables",
    )(rope_frequencies(head_dim))


def qkv_kernel(head_dim, extra, *refs):
    x_ref, gain_ref, wq_ref, wk_ref, wv_ref, cos_ref, sin_ref = refs[:7]
    extra_refs = refs[7:10] if extra else None
    normed_ref = refs[-1]
    q_ref, k_ref, v_ref, token_ref = refs[-5 - 3 * extra:-1 - 3 * extra]
    extra_outs = refs[-4:-1] if extra else (None,) * 3
    rows = x_ref.shape[0]
    chunk = pl.program_id(1)

    @pl.when(pl.program_id(0) == 0)
    def _():
        gain = gain_ref[...].astype(jnp.float32)
        block = min(64, rows)

        @pl.loop(0, rows // block)
        def _(number):
            lines = pl.ds(pl.multiple_of(number * block, block), block)
            normed_ref[chunk, lines] = rms_scale(x_ref[lines].astype(jnp.float32), gain)

        if extra:
            normed_ref[chunk, rows:] = rms_scale(extra_refs[0][...].astype(jnp.float32), gain)
        token_ref[...] = jnp.zeros_like(token_ref)

    cos, sin = cos_ref[...], sin_ref[...]
    if extra:
        cos = jnp.concatenate([cos, extra_refs[1][...]], axis=0)
        sin = jnp.concatenate([sin, extra_refs[2][...]], axis=0)
    for w_ref, out_ref, extra_out in zip((wq_ref, wk_ref, wv_ref), (q_ref, k_ref, v_ref), extra_outs):
        acc = jnp.dot(normed_ref[chunk], w_ref[...], preferred_element_type=jnp.float32)
        for start in range(0, acc.shape[1], head_dim):
            vals = acc[:, start:start + head_dim]
            if out_ref is not v_ref:
                vals = vals * cos + pltpu.roll(vals, head_dim // 2, 1) * sin
            out_ref[:, start:start + head_dim] = vals[:rows].astype(out_ref.dtype)
            if extra:
                extra_out[:, start:start + head_dim] = vals[rows:].astype(out_ref.dtype)


TOKEN = jax.ShapeDtypeStruct((8, 128), jnp.float32)


def project_qkv(half, rows, token, x, extra_rows, gain, w_all, tables, extra_tables, head_dim):
    depth = x.shape[1]
    width = w_all.shape[1] // 3
    block = 2 * head_dim
    steps = width // block
    extra = extra_rows is not None
    extras = [extra_rows, *extra_tables] if extra else []
    pad = extra_rows.shape[0] if extra else 0
    bf16 = jnp.bfloat16
    whole = lambda shape: pl.BlockSpec(shape, lambda n, c: (0, 0), pipeline_mode=pl.Buffered(1))
    columns = lambda part: pl.BlockSpec((depth, block), lambda n, c: (0, part * steps + n))
    table = pl.BlockSpec((rows, head_dim), lambda n, c: (2 * half + c, 0))
    extra_outs = [jax.ShapeDtypeStruct((pad, width), bf16)] * 3 if extra else []
    return pl.pallas_call(
        functools.partial(qkv_kernel, head_dim, extra),
        out_shape=[jax.ShapeDtypeStruct((2 * rows, width), bf16)] * 3 + [TOKEN] + extra_outs,
        grid=(steps, 2),
        in_specs=[
            pl.BlockSpec((rows, depth), lambda n, c: (2 * half + lax.select(n == 0, c, 1), 0)),
            whole((1, depth)),
            columns(0),
            columns(1),
            columns(2),
            table,
            table,
        ] + [whole(e.shape) for e in extras] + [pl.BlockSpec(memory_space=pl.ANY)],
        out_specs=[pl.BlockSpec((rows, block), lambda n, c: (c, n))] * 3 + [whole(TOKEN.shape)] + [pl.BlockSpec((pad, block), lambda n, c: (0, n))] * len(extra_outs),
        scratch_shapes=[pltpu.VMEM((2, rows + pad, depth), bf16)],
        compiler_params=pltpu.CompilerParams(dimension_semantics=("arbitrary", "arbitrary"), vmem_limit_bytes=56 << 20),
        cost_estimate=pl.CostEstimate(flops=12 * rows * depth * width, bytes_accessed=2 * (2 * rows * depth + 3 * depth * width + 6 * rows * width), transcendentals=0),
        name="project_qkv",
    )(x, gain, w_all, w_all, w_all, *tables, *extras, token)


def attend_kernel(chunk, first_checked, q_rows, slen_ref, *refs):
    q_ref = refs[0]
    k_refs = refs[1:chunk + 2]
    v_refs = refs[chunk + 2:2 * chunk + 3]
    out_ref, token_ref = refs[-2:]
    token_ref[...] = jnp.zeros_like(token_ref)
    rows, head_dim = q_ref.shape
    scale = head_dim ** -0.5
    limit = slen_ref[0]

    @pl.loop(0, rows // q_rows)
    def _(number):
        start = pl.multiple_of(number * q_rows, q_rows)
        query = q_ref[pl.ds(start, q_rows), :]
        scores = []
        for part in range(chunk + 1):
            score = lax.dot_general(query, k_refs[part][...], (((1,), (1,)), ((), ())), preferred_element_type=jnp.float32) * scale
            key_pos = lax.broadcasted_iota(jnp.int32, score.shape, 1)
            if part == chunk:
                allowed = key_pos <= lax.broadcasted_iota(jnp.int32, score.shape, 0) + start
                if part >= first_checked:
                    allowed = allowed & (key_pos < limit - part * rows)
                score = jnp.where(allowed, score, -1e30)
            elif part >= first_checked:
                score = jnp.where(key_pos < limit - part * rows, score, -1e30)
            scores.append(score)
        peak = functools.reduce(jnp.maximum, [jnp.max(score, axis=-1, keepdims=True) for score in scores])
        total = jnp.zeros((q_rows, 1), jnp.float32)
        mixed = jnp.zeros((q_rows, head_dim), jnp.float32)
        for score, v_ref in zip(scores, v_refs):
            weight = jnp.exp(score - peak)
            total = total + jnp.sum(weight, axis=-1, keepdims=True)
            mixed = mixed + jnp.dot(weight.astype(jnp.bfloat16), v_ref[...], preferred_element_type=jnp.float32)
        out_ref[pl.ds(start, q_rows), :] = (mixed / total).astype(out_ref.dtype)


def attend(chunk, chunks, rows, token, s_len, queries, keys, values, head_dim):
    width = queries[0].shape[1]
    heads = width // head_dim

    pick = lambda c: pl.BlockSpec((rows, head_dim), lambda h, slen: (c % 2, h))
    every = range(chunk + 1)
    total_keys = rows * (chunk + 1)
    return pl.pallas_call(
        functools.partial(attend_kernel, chunk, chunks // 2, min(256, rows)),
        out_shape=[jax.ShapeDtypeStruct((rows, width), jnp.bfloat16), TOKEN],
        grid_spec=pltpu.PrefetchScalarGridSpec(
            num_scalar_prefetch=1,
            grid=(heads,),
            in_specs=[pick(c) for c in (chunk, *every, *every)] + [pl.BlockSpec(memory_space=pl.ANY)],
            out_specs=[pick(0), pl.BlockSpec(TOKEN.shape, lambda h, slen: (0, 0))],
        ),
        compiler_params=pltpu.CompilerParams(dimension_semantics=("arbitrary",), vmem_limit_bytes=48 << 20),
        cost_estimate=pl.CostEstimate(flops=8 * heads * rows * total_keys * head_dim, bytes_accessed=2 * width * (2 * total_keys + 2 * rows), transcendentals=heads * rows * total_keys),
    )(s_len, queries[chunk // 2], *[keys[c // 2] for c in every], *[values[c // 2] for c in every], token)


def output_kernel(size, heads, contexts, extra, aliased, where_ref, *refs):
    context_refs, refs = refs[:contexts], refs[contexts:]
    w_refs, refs = refs[:heads], refs[heads:]
    x_ref, gain_ref, refs = refs[0], refs[1], refs[2:]
    if extra:
        context_x_ref, x_x_ref, refs = refs[0], refs[1], refs[2:]
    refs = refs[1:]
    if aliased:
        refs = refs[2:]
    normed_ref, hidden_ref, refs = refs[0], refs[1], refs[2:]
    if extra:
        hidden_x_ref, refs = refs[0], refs[1:]
    token_ref, full_ref, square_ref = refs
    rows, depth = hidden_ref.shape
    head_dim, block = w_refs[0].shape[1:]
    chunk, step = pl.program_id(0), pl.program_id(1)

    @pl.when(step == 0)
    def _():
        square_ref[...] = jnp.zeros_like(square_ref)
        token_ref[...] = jnp.zeros_like(token_ref)
        for number, context_ref in enumerate(context_refs):
            @pl.when((chunk == 0) if number == 0 else (chunk > 0))
            def _():
                @pl.loop(0, heads)
                def _(r):
                    columns = pl.ds(pl.multiple_of(lax.bitwise_xor(where_ref[0], r) * head_dim, head_dim), head_dim)
                    for t in range(size):
                        there = pl.ds(pl.multiple_of((r * size + t) * head_dim, head_dim), head_dim)
                        full_ref[:rows, there] = context_ref[t, 0, :, columns]
                        if extra:
                            full_ref[rows:, there] = context_x_ref[t, :, columns]

    w_block = jnp.concatenate([w_ref[...].reshape(size * head_dim, block) for w_ref in w_refs], axis=0)
    acc = jnp.dot(full_ref[...], w_block, preferred_element_type=jnp.float32)
    columns = pl.ds(pl.multiple_of(step * block, block), block)
    hidden = (x_ref[...].astype(jnp.float32) + acc[:rows]).astype(jnp.bfloat16)
    hidden_ref[:, columns] = hidden
    hidden_f32 = hidden.astype(jnp.float32)
    square_ref[:rows] += jnp.sum(hidden_f32 * hidden_f32, axis=-1, keepdims=True)
    if extra:
        hidden = (x_x_ref[...].astype(jnp.float32) + acc[rows:]).astype(jnp.bfloat16)
        hidden_x_ref[:, columns] = hidden
        hidden_f32 = hidden.astype(jnp.float32)
        square_ref[rows:] += jnp.sum(hidden_f32 * hidden_f32, axis=-1, keepdims=True)

    @pl.when(step == pl.num_programs(1) - 1)
    def _():
        half = rows // 2
        inv_rms = lax.rsqrt(square_ref[...] / depth + NORM_EPS)

        @pl.loop(0, depth // block)
        def _(number):
            columns = pl.ds(pl.multiple_of(number * block, block), block)
            gain = gain_ref[:, columns].astype(jnp.float32)
            for part in range(2):
                lo, hi = part * half, (part + 1) * half
                normed_ref[part, :half, columns] = (hidden_ref[lo:hi, columns].astype(jnp.float32) * inv_rms[lo:hi] * gain).astype(jnp.bfloat16)
                if extra and part == 1:
                    normed_ref[part, half:, columns] = (hidden_x_ref[:, columns].astype(jnp.float32) * inv_rms[rows:] * gain).astype(jnp.bfloat16)
                else:
                    normed_ref[part, half:, columns] = jnp.zeros((normed_ref.shape[1] - half, block), jnp.bfloat16)


def project_out(first, count, chunks, pad, token, where, contexts, w_heads, x, gain, extras, buffers):
    rows, width = contexts[0].shape[2:]
    depth = x.shape[1]
    heads = len(w_heads)
    size, head_dim = w_heads[0].shape[:2]
    block = min(512, depth)
    total = rows + (pad if extras else 0)
    whole = lambda shape: pl.BlockSpec(shape, lambda c, n, where: (0,) * len(shape), pipeline_mode=pl.Buffered(1))
    in_specs = [whole(contexts[0].shape)]
    if count > 1:
        in_specs.append(pl.BlockSpec((size, 1, rows, width), lambda c, n, where: (0, lax.max(c - 1, 0), 0, 0)))
    in_specs += [pl.BlockSpec((size, head_dim, block), lambda c, n, where: (0, 0, n))] * heads
    in_specs += [pl.BlockSpec((rows, block), lambda c, n, where: (first + c, n)), whole((1, depth))]
    out_shape = [jax.ShapeDtypeStruct((2 * chunks, rows // 2 + pad, depth), jnp.bfloat16), jax.ShapeDtypeStruct((rows * chunks, depth), jnp.bfloat16)]
    mode = {} if count > 1 else dict(pipeline_mode=pl.Buffered(1))
    out_specs = [
        pl.BlockSpec((2, rows // 2 + pad, depth), lambda c, n, where: (first + c, 0, 0), **mode),
        pl.BlockSpec((rows, depth), lambda c, n, where: (first + c, 0), **mode),
    ]
    if extras:
        in_specs += [whole(extras[0].shape), pl.BlockSpec((pad, block), lambda c, n, where: (0, n))]
        out_shape.append(jax.ShapeDtypeStruct((pad, depth), jnp.bfloat16))
        out_specs.append(whole((pad, depth)))
    in_specs.append(pl.BlockSpec(memory_space=pl.ANY))
    out_shape.append(TOKEN)
    out_specs.append(whole(TOKEN.shape))
    aliases = {}
    if buffers:
        aliases = {1 + len(in_specs): 0, 2 + len(in_specs): 1}
        in_specs += [pl.BlockSpec(memory_space=pl.ANY)] * 2
    return pl.pallas_call(
        functools.partial(output_kernel, size, heads, len(contexts), bool(extras), bool(buffers)),
        out_shape=out_shape,
        grid_spec=pltpu.PrefetchScalarGridSpec(
            num_scalar_prefetch=1,
            grid=(count, depth // block),
            in_specs=in_specs,
            out_specs=out_specs,
            scratch_shapes=[pltpu.VMEM((total, size * width), jnp.bfloat16), pltpu.VMEM((total, 1), jnp.float32)],
        ),
        input_output_aliases=aliases,
        compiler_params=pltpu.CompilerParams(dimension_semantics=("arbitrary", "arbitrary"), vmem_limit_bytes=60 << 20),
        cost_estimate=pl.CostEstimate(flops=2 * count * total * size * width * depth, bytes_accessed=2 * count * (size * width * depth + 4 * rows * width + 3 * total * depth), transcendentals=0),
        name="project_out",
    )(where, *contexts, *w_heads, x, gain, *extras, token, *buffers)


def mlp_kernel(size, chunk_rows, ff_steps, slots, token_ref, normed_ref, hextra_ref, wgu_ref, wd_ref, h_ref, out_ref, y_ref,
               acc, landed, outgoing, finished, residual, others, activated,
               rs_send, rs_recv, ag_send, ag_recv, keep_sem, h_sem, x_send, x_recv, credit):
    step = pl.program_id(0)
    me = lax.axis_index('tp')
    depth = wd_ref.shape[1]
    chunks = (out_ref.shape[0] // chunk_rows)
    piece = outgoing.shape[2]
    per_chunk = chunk_rows // (2 * piece)
    pieces = chunks * per_chunk
    subs = per_chunk // ff_steps
    last = size - 1

    @pl.when(step == 0)
    def _():
        barrier = pltpu.get_barrier_semaphore()
        for d in range(1, size):
            pl.semaphore_signal(barrier, inc=1, device_id={'tp': lax.rem(me + d, size)}, device_id_type=pl.DeviceIdType.MESH)
        pl.semaphore_wait(barrier, size - 1)

    def own_part(chain, m):
        start = pl.multiple_of(chain * (chunk_rows // 2) + lax.rem(m, per_chunk) * piece, piece)
        return acc.at[lax.rem(lax.div(m, per_chunk), 3), pl.ds(start, piece)]

    def out_rows(chain, m):
        start = pl.multiple_of(lax.div(m, per_chunk) * chunk_rows + chain * (chunk_rows // 2) + lax.rem(m, per_chunk) * piece, piece)
        return pl.ds(start, piece)

    def exchange(slot):
        for chain in range(2):
            place = me if chain == 0 else last - me
            nearer = me - 1 if chain == 0 else me + 1
            farther = me + 1 if chain == 0 else me - 1

            def sum_copy(source, m):
                return pltpu.make_async_remote_copy(
                    src_ref=source, dst_ref=landed.at[chain, lax.rem(m, slots)], send_sem=rs_send.at[chain, lax.rem(m, 4)],
                    recv_sem=rs_recv.at[chain, lax.rem(m, slots)], device_id={'tp': nearer}, device_id_type=pl.DeviceIdType.MESH)

            def keep_copy(m):
                return pltpu.make_async_copy(finished.at[chain, lax.rem(m, 2)], out_ref.at[out_rows(chain, m)], keep_sem.at[chain, lax.rem(m, 2)])

            def h_copy(m):
                return pltpu.make_async_copy(h_ref.at[out_rows(chain, m)], residual.at[chain, lax.rem(m, 2)], h_sem.at[chain, lax.rem(m, 2)])

            def back_copy(source, m):
                return pltpu.make_async_remote_copy(
                    src_ref=source, dst_ref=out_ref.at[out_rows(chain, m)], send_sem=ag_send.at[chain, lax.rem(m, 4)],
                    recv_sem=ag_recv.at[chain, lax.rem(m, 8)], device_id={'tp': farther}, device_id_type=pl.DeviceIdType.MESH)

            @pl.when((place == last) & (slot >= 0) & (slot < pieces))
            def _():
                @pl.when(slot >= 4)
                def _():
                    sum_copy(own_part(chain, slot - 4), slot - 4).wait_send()

                @pl.when(slot >= slots)
                def _():
                    pl.semaphore_wait(credit.at[chain], 1)

                sum_copy(own_part(chain, slot), slot).start()

            m = slot - (last - place)

            @pl.when((place > 0) & (place < last) & (m >= 0) & (m < pieces))
            def _():
                @pl.when(m >= 2)
                def _():
                    sum_copy(outgoing.at[chain, lax.rem(m, 2)], m - 2).wait_send()

                sum_copy(outgoing.at[chain, lax.rem(m, 2)], m).wait_recv()
                outgoing[chain, lax.rem(m, 2)] = landed[chain, lax.rem(m, slots)] + own_part(chain, m)[...]

                @pl.when(m + slots < pieces)
                def _():
                    pl.semaphore_signal(credit.at[chain], inc=1, device_id={'tp': farther}, device_id_type=pl.DeviceIdType.MESH)

                @pl.when(m >= slots)
                def _():
                    pl.semaphore_wait(credit.at[chain], 1)

                sum_copy(outgoing.at[chain, lax.rem(m, 2)], m).start()

            m = slot - last

            @pl.when((place == 0) & (slot == 0))
            def _():
                h_copy(0).start()

            @pl.when((place == 0) & (m >= 0) & (m < pieces))
            def _():
                @pl.when(m + 1 < pieces)
                def _():
                    h_copy(m + 1).start()

                @pl.when(m >= 2)
                def _():
                    keep_copy(m - 2).wait()
                    back_copy(finished.at[chain, lax.rem(m, 2)], m - 2).wait_send()

                h_copy(m).wait()
                sum_copy(outgoing.at[chain, lax.rem(m, 2)], m).wait_recv()
                total = landed[chain, lax.rem(m, slots)] + own_part(chain, m)[...]
                finished[chain, lax.rem(m, 2)] = (residual[chain, lax.rem(m, 2)].astype(jnp.float32) + total).astype(jnp.bfloat16)

                @pl.when(m + slots < pieces)
                def _():
                    pl.semaphore_signal(credit.at[chain], inc=1, device_id={'tp': farther}, device_id_type=pl.DeviceIdType.MESH)

                keep_copy(m).start()
                back_copy(finished.at[chain, lax.rem(m, 2)], m).start()

        for chain in range(2):
            place = me if chain == 0 else last - me
            farther = me + 1 if chain == 0 else me - 1

            def relay_copy(m):
                return pltpu.make_async_remote_copy(
                    src_ref=out_ref.at[out_rows(chain, m)], dst_ref=out_ref.at[out_rows(chain, m)], send_sem=ag_send.at[chain, lax.rem(m, 4)],
                    recv_sem=ag_recv.at[chain, lax.rem(m, 8)], device_id={'tp': farther}, device_id_type=pl.DeviceIdType.MESH)

            m = slot - last - 2 * place

            @pl.when((place > 0) & (m >= 0) & (m < pieces))
            def _():
                relay_copy(m).wait_recv()

                @pl.when((place < last) & (m >= 4))
                def _():
                    relay_copy(m - 4).wait_send()

                @pl.when(place < last)
                def _():
                    relay_copy(m).start()

    def extra_copy(d):
        return pltpu.make_async_remote_copy(
            src_ref=acc.at[(chunks - 1) % 3, pl.ds(chunk_rows, others.shape[1])], dst_ref=others.at[d], send_sem=x_send.at[d - 1],
            recv_sem=x_recv.at[d - 1], device_id={'tp': lax.rem(me + d, size)}, device_id_type=pl.DeviceIdType.MESH)

    @pl.when(step == chunks * ff_steps)
    def _():
        others[0] = acc[(chunks - 1) % 3, chunk_rows:chunk_rows + others.shape[1]]
        for d in range(1, size):
            extra_copy(d).start()

    @pl.when(step == chunks * ff_steps + 4)
    def _():
        for d in range(1, size):
            extra_copy(d).wait()
        total = others[lax.rem(me, size)]
        for j in range(1, size):
            total = total + others[lax.rem(me + size - j, size)]
        y_ref[...] = (hextra_ref[:others.shape[1]].astype(jnp.float32) + total).astype(jnp.bfloat16)

    chunk = lax.div(step, ff_steps)
    block = min(1024, depth)

    def compute_gate():
        rows_in = normed_ref[0]
        dims = (((1,), (1,)), ((), ()))
        gate = lax.dot_general(rows_in, wgu_ref[0], dims, preferred_element_type=jnp.float32)
        up = lax.dot_general(rows_in, wgu_ref[1], dims, preferred_element_type=jnp.float32)
        activated[...] = (gate * jax.nn.sigmoid(gate) * up).astype(jnp.bfloat16)

    def compute_down():
        first = lax.rem(step, ff_steps) == 0
        for start in range(0, depth, block):
            part = jnp.dot(activated[...], wd_ref[:, start:start + block], preferred_element_type=jnp.float32)

            @pl.when(first)
            def _():
                acc[lax.rem(chunk, 3), :, start:start + block] = part

            @pl.when(jnp.logical_not(first))
            def _():
                acc[lax.rem(chunk, 3), :, start:start + block] += part

    @pl.loop(0, subs)
    def _(sub):
        exchange((step - ff_steps) * subs + sub)
        for part in range(2):
            pl.when((step < chunks * ff_steps) & (sub == part * subs // 2))((compute_gate, compute_down)[part])

    @pl.when(step == pl.num_programs(0) - 1)
    def _():
        for chain in range(2):
            place = me if chain == 0 else last - me
            nearer = me - 1 if chain == 0 else me + 1
            farther = me + 1 if chain == 0 else me - 1

            def sent(m):
                return pltpu.make_async_remote_copy(
                    src_ref=outgoing.at[chain, m % 2], dst_ref=landed.at[chain, m % slots], send_sem=rs_send.at[chain, m % 4],
                    recv_sem=rs_recv.at[chain, m % slots], device_id={'tp': nearer}, device_id_type=pl.DeviceIdType.MESH)

            def returned(m):
                return pltpu.make_async_remote_copy(
                    src_ref=finished.at[chain, m % 2], dst_ref=out_ref.at[pl.ds(0, piece)], send_sem=ag_send.at[chain, m % 4],
                    recv_sem=ag_recv.at[chain, m % 8], device_id={'tp': farther}, device_id_type=pl.DeviceIdType.MESH)

            @pl.when(place == last)
            def _():
                for m in range(pieces - 4, pieces):
                    sent(m).wait_send()

            @pl.when((place > 0) & (place < last))
            def _():
                for m in range(pieces - 2, pieces):
                    sent(m).wait_send()
                for m in range(pieces - 4, pieces):
                    returned(m).wait_send()

            @pl.when(place == 0)
            def _():
                for m in range(pieces - 2, pieces):
                    pltpu.make_async_copy(finished.at[chain, m % 2], out_ref.at[pl.ds(0, piece)], keep_sem.at[chain, m % 2]).wait()
                    returned(m).wait_send()


SUBSLOTS = 2


def mlp(token, normed, hextra, w_gate_up, w_down, hidden, size):
    chunks, lines, depth = normed.shape
    rows = hidden.shape[0]
    chunk_rows = rows // chunks
    ff = w_down.shape[0]
    ff_steps = 4
    piece = chunk_rows // (8 * SUBSLOTS)
    slots = 4
    pieces = chunks * 4 * SUBSLOTS
    extra = lines - chunk_rows
    seen = min(8, extra)
    steps = chunks * ff_steps
    total_steps = ff_steps + -(-(pieces + 3 * (size - 1)) // SUBSLOTS)
    ff_block = ff // ff_steps
    at_ff = lambda g: lax.select(g < steps, lax.rem(g, ff_steps), ff_steps - 1)
    at_chunk = lambda g: lax.min(lax.div(g, ff_steps), chunks - 1)
    f32, bf16 = jnp.float32, jnp.bfloat16
    return pl.pallas_call(
        functools.partial(mlp_kernel, size, chunk_rows, ff_steps, slots),
        out_shape=[jax.ShapeDtypeStruct((rows, depth), bf16), jax.ShapeDtypeStruct((seen, depth), bf16)],
        grid=(total_steps,),
        in_specs=[
            pl.BlockSpec(memory_space=pl.ANY),
            pl.BlockSpec((1, lines, depth), lambda g: (at_chunk(g), 0, 0)),
            pl.BlockSpec((extra, depth), lambda g: (0, 0), pipeline_mode=pl.Buffered(1)),
            pl.BlockSpec((2, ff_block, depth), lambda g: (0, at_ff(g), 0)),
            pl.BlockSpec((ff_block, depth), lambda g: (at_ff(g), 0)),
            pl.BlockSpec(memory_space=pl.ANY),
        ],
        out_specs=[pl.BlockSpec(memory_space=pl.ANY), pl.BlockSpec((seen, depth), lambda g: (0, 0), pipeline_mode=pl.Buffered(1))],
        scratch_shapes=[
            pltpu.VMEM((3, lines, depth), f32),
            pltpu.VMEM((2, slots, piece, depth), f32),
            pltpu.VMEM((2, 2, piece, depth), f32),
            pltpu.VMEM((2, 2, piece, depth), bf16),
            pltpu.VMEM((2, 2, piece, depth), bf16),
            pltpu.VMEM((size, seen, depth), f32),
            pltpu.VMEM((lines, ff_block), bf16),
            pltpu.SemaphoreType.DMA((2, 4)),
            pltpu.SemaphoreType.DMA((2, slots)),
            pltpu.SemaphoreType.DMA((2, 4)),
            pltpu.SemaphoreType.DMA((2, 8)),
            pltpu.SemaphoreType.DMA((2, 2)),
            pltpu.SemaphoreType.DMA((2, 2)),
            pltpu.SemaphoreType.DMA((size - 1,)),
            pltpu.SemaphoreType.DMA((size - 1,)),
            pltpu.SemaphoreType.REGULAR((2,)),
        ],
        compiler_params=pltpu.CompilerParams(dimension_semantics=("arbitrary",), vmem_limit_bytes=63 << 20, collective_id=0, has_side_effects=True),
        cost_estimate=pl.CostEstimate(flops=6 * rows * depth * ff, bytes_accessed=6 * chunks * depth * ff, transcendentals=rows * ff),
        name="mlp",
    )(token, normed, hextra, w_gate_up, w_down, hidden)


def place_kernel(size, where_ref, *refs):
    k_ref, v_ref = refs[-2:]
    for d in range(size):
        @pl.when(pl.program_id(0) == d)
        def _():
            k_ref[:, 0] = refs[d][0]
            v_ref[:, 0] = refs[d][1]


def place_caches(where, landed):
    rows, heads, head_dim = landed[0].shape[1:]
    size = len(landed)
    block = rows // 4
    blocks = rows // block

    def turn(number):
        return lambda d, n, where: (0, lax.select(d == number, n, lax.select(d < number, 0, blocks - 1)), 0, 0)

    out = pl.BlockSpec((block, 1, heads, head_dim), lambda d, n, where: (n, lax.rem(where[0] - d + size, size), 0, 0))
    return pl.pallas_call(
        functools.partial(place_kernel, size),
        out_shape=[jax.ShapeDtypeStruct((rows, size, heads, head_dim), jnp.bfloat16)] * 2,
        grid_spec=pltpu.PrefetchScalarGridSpec(
            num_scalar_prefetch=1,
            grid=(size, blocks),
            in_specs=[pl.BlockSpec((2, block, heads, head_dim), turn(d)) for d in range(size)],
            out_specs=[out, out],
        ),
        compiler_params=pltpu.CompilerParams(dimension_semantics=("arbitrary", "arbitrary")),
        cost_estimate=pl.CostEstimate(flops=0, bytes_accessed=8 * size * rows * heads * head_dim, transcendentals=0),
        name="place_caches",
    )(where, *landed)


def pick_by(index, options):
    result = options[0]
    for place in range(1, len(options)):
        result = jnp.where(index == place, options[place], result)
    return result


def solution(mesh):
    side_size = mesh.shape['side']
    tp_size = mesh.shape['tp']
    seats = mesh.shape['pair'] * side_size
    group_axes = ('pair', 'side')
    last = tp_size - 1

    def cyclic(value, d):
        return lax.ppermute(value, 'tp', [(t, (t + d) % tp_size) for t in range(tp_size)])

    def swap(value, mask):
        return lax.ppermute(value, group_axes, [(q, q ^ mask) for q in range(seats)])

    def in_order(me, copies):
        return [pick_by(me, [copies[(t - j) % tp_size] for t in range(tp_size)]) for j in range(tp_size)]

    def device_fn(x_prompt, s_len, y_tok, c_len, k_cache, v_cache, attn_gain, w_qkv, w_out, mlp_gain, w_gate_up, w_down):
        me = lax.axis_index('tp')
        seat = lax.axis_index('pair') * side_size + lax.axis_index('side')
        where = seat.reshape(1).astype(jnp.int32)
        seq_len, depth = x_prompt.shape[1:]
        heads_local = w_qkv.shape[2]
        head_dim = w_qkv.shape[4]
        width = heads_local * head_dim
        rows = seq_len // tp_size
        decodes = y_tok.shape[0]
        pad = 16
        cache_local = k_cache.shape[2]
        val = {}

        def tie(keys):
            keys = list(dict.fromkeys(keys))
            for key, value in zip(keys, lax.optimization_barrier(tuple(val[key] for key in keys))):
                val[key] = value

        val['w', 0] = lax.all_gather(lax.dynamic_index_in_dim(w_out[0, :, 0], seat, 0, keepdims=False), 'tp', axis=0, tiled=False)

        val['w_all'] = jnp.swapaxes(w_qkv[0], 1, 2).reshape(depth, 3 * width)
        tables = rope_tables_upto(seq_len, head_dim)
        extra_tables = rope_tables(jnp.concatenate([c_len, jnp.zeros((pad - decodes,), jnp.int32)]), head_dim)
        y_pad = jnp.concatenate([y_tok, jnp.zeros((pad - decodes, depth), y_tok.dtype)])
        val['gain'], val['s_len'], val['mlp_gain'] = attn_gain, s_len, mlp_gain
        val['valid'] = (jnp.arange(seq_len) < s_len[0]).astype(jnp.bfloat16)
        buffers = []
        qkv = []

        def compute(name):
            kind = name[0]
            c = int(name[1:]) if name[1:].isdigit() else 0
            if kind == 'Q':
                tie(thread + ['gain'])
                made = project_qkv(c, rows, val['token'], x_prompt[0], y_pad if c == 0 else None, val['gain'], val['w_all'], tables, extra_tables, head_dim)
                val['token'] = made[3]
                qkv.append(made[:3])
                if c == 0:
                    val['dq', 0] = jnp.stack([part[:decodes].reshape(decodes, heads_local, head_dim) for part in made[4:]])
                    for d in range(1, tp_size):
                        val['dq', d] = cyclic(val['dq', 0], d)
                return ['token']
            if kind == 'T':
                tie(thread + ['s_len'])
                val['context', c], val['token'] = attend(c, tp_size, rows, val['token'], val['s_len'], *zip(*qkv), head_dim)
                return ['token']
            if kind == 'G':
                val['gathered', name[1:]] = lax.all_gather(jnp.stack([val['context', int(digit)] for digit in name[1:]]), 'tp', axis=0, tiled=False)
                return ['token']
            if kind == 'K':
                tie(thread + ['valid'])
                for d in range(tp_size):
                    made = []
                    keep = pick_by(me, [val['valid'][((t + d) % tp_size) * rows:((t + d) % tp_size + 1) * rows] for t in range(tp_size)])
                    for which in (1, 2):
                        rows_d = pick_by(me, [qkv[(t + d) % tp_size // 2][which][(t + d) % tp_size % 2 * rows:][:rows].reshape(rows, heads_local, head_dim) for t in range(tp_size)])
                        made.append(rows_d * keep[:, None, None])
                    val['kv', d] = jnp.stack(made)
                return []
            if name == 'D1':
                tie(thread + [('dq', d) for d in range(tp_size)])
                dec_full = jnp.concatenate(in_order(me, [val['dq', d] for d in range(tp_size)]), axis=2)
                cache_pos = me * cache_local + jnp.arange(cache_local)
                write_mask = (cache_pos[None, :] == c_len[:, None])[:, :, None, None]
                allowed = (cache_pos[None, :] <= c_len[:, None])[:, :, None]
                key_now = jnp.where(write_mask, dec_full[1][:, None], k_cache[0])
                value_now = jnp.where(write_mask, dec_full[2][:, None], v_cache[0])
                val['key_now'], val['value_now'] = key_now, value_now
                scores = jnp.sum(dec_full[0][:, None].astype(jnp.float32) * key_now.astype(jnp.float32), axis=-1) * head_dim ** -0.5
                scores = jnp.where(allowed, scores, -1e30)
                peak = jnp.max(scores, axis=1, keepdims=True)
                weights = jnp.exp(scores - peak)
                total = jnp.sum(weights, axis=1)[..., None]
                peak = peak[:, 0, :, None]
                mixed = jnp.sum(weights.astype(jnp.bfloat16).astype(jnp.float32)[..., None] * value_now.astype(jnp.float32), axis=1)
                packed = jnp.stack([mixed, jnp.broadcast_to(peak, mixed.shape), jnp.broadcast_to(total, mixed.shape)])
                packed = packed.reshape(3, decodes, tp_size, heads_local, head_dim)
                for d in range(tp_size):
                    share = lax.dynamic_index_in_dim(packed, lax.rem(me + d, tp_size), 2, keepdims=False)
                    val['ds', d] = share if d == 0 else cyclic(share, d)
                return [('ds', 0)]
            if name == 'D2':
                tie(thread + [('ds', d) for d in range(tp_size)])
                shares = [val['ds', d] for d in range(tp_size)]
                top = functools.reduce(jnp.maximum, [share[1] for share in shares])
                factors = [jnp.exp(share[1] - top) for share in shares]
                dec_mixed = sum(share[0] * factor for share, factor in zip(shares, factors))
                dec_total = sum(share[2] * factor for share, factor in zip(shares, factors))
                val['dc', 0] = (dec_mixed / dec_total).astype(jnp.bfloat16).reshape(decodes, width)
                for d in range(1, tp_size):
                    val['dc', d] = cyclic(val['dc', 0], d)
                return [('dc', 0)]
            if kind == 'O':
                w_keys = [('w', r) for r in range(seats)]
                final = c == last
                parts = [('gathered', '3')] if final else [('gathered', '0'), ('gathered', '12')]
                extra_keys = [('dc', d) for d in range(tp_size)] if final else []
                tie(thread + ['mlp_gain'] + parts + extra_keys + ([] if final else w_keys))
                extras = []
                if final:
                    extras = [jnp.pad(jnp.stack(in_order(me, [val[key] for key in extra_keys])), ((0, 0), (0, pad - decodes), (0, 0))), y_pad]
                made = project_out(last if final else 0, 1 if final else last, tp_size, pad, val['token'], where, [val[key] for key in parts], [val[key] for key in w_keys], x_prompt[0], val['mlp_gain'], extras, [val[key] for key in buffers])
                buffers[:] = ['normed', 'h']
                val['normed'], val['h'], val['token'] = made[0], made[1], made[-1]
                if final:
                    val['hx'] = made[2]
                return ['token']
            if kind == 'P':
                tie(thread + [('landed', d) for d in range(tp_size)])
                val['k'], val['v'] = place_caches(me.reshape(1).astype(jnp.int32), [val['landed', d] for d in range(tp_size)])
                return ['k']
            val['out'], val['y'] = mlp(val['token'], val['normed'], val['hx'], jnp.transpose(w_gate_up[0], (1, 2, 0)), w_down[0], val['h'], tp_size)
            return ['y']

        def transfer(name):
            if name[0] == 'k':
                d = int(name[1])
                tie(thread + [('kv', d)])
                route = [(t * side_size + s, ((t + d) % tp_size) * side_size + (s + 1) % side_size) for t in range(tp_size) for s in range(side_size)]
                val['landed', d] = lax.ppermute(val['kv', d], ('tp', 'side'), route)
                return
            bases = [0] if name == 'w2' else list(range(0, seats, 2))
            kept = [] if name == 'w2' else [('kv', d) for d in range(tp_size)]
            tie(thread + kept + [('w', base) for base in bases])
            for mask in (range(2, seats, 2) if name == 'w2' else [1]):
                for base in bases:
                    val['w', base ^ mask] = swap(val['w', base], mask)

        val['token'] = jnp.zeros(TOKEN.shape, TOKEN.dtype)
        thread = ['token']
        for name in ORDER:
            if name[0] in 'QTGKDOBP':
                made = compute(name)
                thread = thread + made if name in ('K', 'D1', 'D2') else made
            else:
                transfer(name)

        caches = [val[name].reshape(1, 1, rows, tp_size * heads_local, head_dim) for name in 'kv']
        return (val['out'][None], val['y'][:decodes], caches[0], caches[1], val['key_now'][None], val['value_now'][None])

    cache_spec = P(None, group_axes, 'tp', None, None)
    in_specs = (P(group_axes, None, None), P(group_axes), P(group_axes, None), P(group_axes), cache_spec, cache_spec, P(), P(None, None, 'tp', None, None), P(None, 'tp', None, None, None), P(), P(None, None, None, 'tp'), P(None, 'tp', None))
    out_specs = (P(group_axes, None, None), P(group_axes, None), cache_spec, cache_spec, cache_spec, cache_spec)
    return jax.shard_map(device_fn, mesh=mesh, in_specs=in_specs, out_specs=out_specs, check_vma=False)
```

```python
import functools

import jax
import jax.numpy as jnp
from jax import lax
from jax.experimental import pallas as pl
from jax.experimental.pallas import tpu as pltpu
from jax.sharding import PartitionSpec as P


ROPE_BASE = 10000.0
NORM_EPS = 1e-5

ORDER = (
    'Q0', 'T0', 'G0', 'T1', 'w2', 'Q1', 'T2', 'G12', 'T3', 'G3', 'K', 'k1', 'k3', 'D1', 'D2', 'w3', 'O012', 'k0', 'k2',
    'O3', 'B', 'P',
)


def rms_scale(values_f32, gain_f32):
    inv_rms = lax.rsqrt(jnp.mean(values_f32 * values_f32, axis=-1, keepdims=True) + NORM_EPS)
    return (values_f32 * inv_rms * gain_f32).astype(jnp.bfloat16)


def rope_frequencies(head_dim):
    half_dim = head_dim // 2
    inv_freq = ROPE_BASE ** (-2.0 * jnp.arange(half_dim, dtype=jnp.float32) / head_dim)
    return jnp.concatenate([inv_freq, inv_freq])[None]


def rope_tables(positions, head_dim):
    angles = positions.astype(jnp.float32)[:, None] * rope_frequencies(head_dim)
    sign = jnp.where(jnp.arange(head_dim) < head_dim // 2, -1.0, 1.0)
    return jnp.cos(angles), jnp.sin(angles) * sign[None]


def rope_rows(first, rows, freq):
    head_dim = freq.shape[1]
    positions = lax.broadcasted_iota(jnp.int32, (rows, head_dim), 0) + first
    angles = positions.astype(jnp.float32) * freq
    turns = jnp.floor(angles * 0.15915494309189535 + 0.5)
    angles = (angles - turns * 6.28125) - turns * 0.0019353071795864769
    sine = jnp.sin(angles)
    return jnp.cos(angles), jnp.where(lax.broadcasted_iota(jnp.int32, (rows, head_dim), 1) < head_dim // 2, -sine, sine)


def qkv_kernel(half, head_dim, extra, *refs):
    x_ref, gain_ref, wq_ref, wk_ref, wv_ref, freq_ref = refs[:6]
    extra_refs = refs[6:9] if extra else None
    normed_ref, cos_ref, sin_ref = refs[-3:]
    q_ref, k_ref, v_ref, token_ref = refs[-7 - 3 * extra:-3 - 3 * extra]
    extra_outs = refs[-6:-3] if extra else (None,) * 3
    rows = x_ref.shape[0]
    chunk = pl.program_id(1)

    @pl.when(pl.program_id(0) == 0)
    def _():
        gain = gain_ref[...].astype(jnp.float32)
        block = min(64, rows)

        @pl.loop(0, rows // block)
        def _(number):
            lines = pl.ds(pl.multiple_of(number * block, block), block)
            normed_ref[chunk, lines] = rms_scale(x_ref[lines].astype(jnp.float32), gain)
            cos_ref[chunk, lines], sin_ref[chunk, lines] = rope_rows((2 * half + chunk) * rows + number * block, block, freq_ref[...])

        if extra:
            normed_ref[chunk, rows:] = rms_scale(extra_refs[0][...].astype(jnp.float32), gain)
        token_ref[...] = jnp.zeros_like(token_ref)

    cos, sin = cos_ref[chunk], sin_ref[chunk]
    if extra:
        cos = jnp.concatenate([cos, extra_refs[1][...]], axis=0)
        sin = jnp.concatenate([sin, extra_refs[2][...]], axis=0)
    for w_ref, out_ref, extra_out in zip((wq_ref, wk_ref, wv_ref), (q_ref, k_ref, v_ref), extra_outs):
        acc = jnp.dot(normed_ref[chunk], w_ref[...], preferred_element_type=jnp.float32)
        for start in range(0, acc.shape[1], head_dim):
            vals = acc[:, start:start + head_dim]
            if out_ref is not v_ref:
                vals = vals * cos + pltpu.roll(vals, head_dim // 2, 1) * sin
            out_ref[:, start:start + head_dim] = vals[:rows].astype(out_ref.dtype)
            if extra:
                extra_out[:, start:start + head_dim] = vals[rows:].astype(out_ref.dtype)


TOKEN = jax.ShapeDtypeStruct((8, 128), jnp.float32)


def project_qkv(half, rows, token, x, extra_rows, gain, w_all, extra_tables, head_dim):
    depth = x.shape[1]
    width = w_all.shape[1] // 3
    block = 2 * head_dim
    steps = width // block
    extra = extra_rows is not None
    extras = [extra_rows, *extra_tables] if extra else []
    pad = extra_rows.shape[0] if extra else 0
    bf16 = jnp.bfloat16
    whole = lambda shape: pl.BlockSpec(shape, lambda n, c: (0, 0), pipeline_mode=pl.Buffered(1))
    columns = lambda part: pl.BlockSpec((depth, block), lambda n, c: (0, part * steps + n))
    extra_outs = [jax.ShapeDtypeStruct((pad, width), bf16)] * 3 if extra else []
    return pl.pallas_call(
        functools.partial(qkv_kernel, half, head_dim, extra),
        out_shape=[jax.ShapeDtypeStruct((2 * rows, width), bf16)] * 3 + [TOKEN] + extra_outs,
        grid=(steps, 2),
        in_specs=[
            pl.BlockSpec((rows, depth), lambda n, c: (2 * half + lax.select(n == 0, c, 1), 0)),
            whole((1, depth)),
            columns(0),
            columns(1),
            columns(2),
            whole((1, head_dim)),
        ] + [whole(e.shape) for e in extras] + [pl.BlockSpec(memory_space=pl.ANY)],
        out_specs=[pl.BlockSpec((rows, block), lambda n, c: (c, n))] * 3 + [whole(TOKEN.shape)] + [pl.BlockSpec((pad, block), lambda n, c: (0, n))] * len(extra_outs),
        scratch_shapes=[pltpu.VMEM((2, rows + pad, depth), bf16)] + [pltpu.VMEM((2, rows, head_dim), jnp.float32)] * 2,
        compiler_params=pltpu.CompilerParams(dimension_semantics=("arbitrary", "arbitrary"), vmem_limit_bytes=56 << 20),
        cost_estimate=pl.CostEstimate(flops=12 * rows * depth * width, bytes_accessed=2 * (2 * rows * depth + 3 * depth * width + 6 * rows * width), transcendentals=0),
        name="project_qkv",
    )(x, gain, w_all, w_all, w_all, rope_frequencies(head_dim), *extras, token)


def attend_kernel(chunk, first_checked, q_rows, slen_ref, *refs):
    q_ref = refs[0]
    k_refs = refs[1:chunk + 2]
    v_refs = refs[chunk + 2:2 * chunk + 3]
    out_ref, token_ref = refs[-2:]
    token_ref[...] = jnp.zeros_like(token_ref)
    rows, head_dim = q_ref.shape
    scale = head_dim ** -0.5
    limit = slen_ref[0]

    @pl.loop(0, rows // q_rows)
    def _(number):
        start = pl.multiple_of(number * q_rows, q_rows)
        query = q_ref[pl.ds(start, q_rows), :]
        scores = []
        for part in range(chunk + 1):
            score = lax.dot_general(query, k_refs[part][...], (((1,), (1,)), ((), ())), preferred_element_type=jnp.float32) * scale
            key_pos = lax.broadcasted_iota(jnp.int32, score.shape, 1)
            if part == chunk:
                allowed = key_pos <= lax.broadcasted_iota(jnp.int32, score.shape, 0) + start
                if part >= first_checked:
                    allowed = allowed & (key_pos < limit - part * rows)
                score = jnp.where(allowed, score, -1e30)
            elif part >= first_checked:
                score = jnp.where(key_pos < limit - part * rows, score, -1e30)
            scores.append(score)
        peak = functools.reduce(jnp.maximum, [jnp.max(score, axis=-1, keepdims=True) for score in scores])
        total = jnp.zeros((q_rows, 1), jnp.float32)
        mixed = jnp.zeros((q_rows, head_dim), jnp.float32)
        for score, v_ref in zip(scores, v_refs):
            weight = jnp.exp(score - peak)
            total = total + jnp.sum(weight, axis=-1, keepdims=True)
            mixed = mixed + jnp.dot(weight.astype(jnp.bfloat16), v_ref[...], preferred_element_type=jnp.float32)
        out_ref[pl.ds(start, q_rows), :] = (mixed / total).astype(out_ref.dtype)


def attend(chunk, chunks, rows, token, s_len, queries, keys, values, head_dim):
    width = queries[0].shape[1]
    heads = width // head_dim

    pick = lambda c: pl.BlockSpec((rows, head_dim), lambda h, slen: (c % 2, h))
    every = range(chunk + 1)
    total_keys = rows * (chunk + 1)
    return pl.pallas_call(
        functools.partial(attend_kernel, chunk, chunks // 2, min(256, rows)),
        out_shape=[jax.ShapeDtypeStruct((rows, width), jnp.bfloat16), TOKEN],
        grid_spec=pltpu.PrefetchScalarGridSpec(
            num_scalar_prefetch=1,
            grid=(heads,),
            in_specs=[pick(c) for c in (chunk, *every, *every)] + [pl.BlockSpec(memory_space=pl.ANY)],
            out_specs=[pick(0), pl.BlockSpec(TOKEN.shape, lambda h, slen: (0, 0))],
        ),
        compiler_params=pltpu.CompilerParams(dimension_semantics=("arbitrary",), vmem_limit_bytes=48 << 20),
        cost_estimate=pl.CostEstimate(flops=8 * heads * rows * total_keys * head_dim, bytes_accessed=2 * width * (2 * total_keys + 2 * rows), transcendentals=heads * rows * total_keys),
    )(s_len, queries[chunk // 2], *[keys[c // 2] for c in every], *[values[c // 2] for c in every], token)


def output_kernel(size, heads, contexts, extra, aliased, where_ref, *refs):
    context_refs, refs = refs[:contexts], refs[contexts:]
    w_refs, refs = refs[:heads], refs[heads:]
    x_ref, gain_ref, refs = refs[0], refs[1], refs[2:]
    if extra:
        context_x_ref, x_x_ref, refs = refs[0], refs[1], refs[2:]
    refs = refs[1:]
    if aliased:
        refs = refs[2:]
    normed_ref, hidden_ref, refs = refs[0], refs[1], refs[2:]
    if extra:
        hidden_x_ref, refs = refs[0], refs[1:]
    token_ref, full_ref, square_ref = refs
    rows, depth = hidden_ref.shape
    head_dim, block = w_refs[0].shape[1:]
    chunk, step = pl.program_id(0), pl.program_id(1)

    @pl.when(step == 0)
    def _():
        square_ref[...] = jnp.zeros_like(square_ref)
        token_ref[...] = jnp.zeros_like(token_ref)
        for number, context_ref in enumerate(context_refs):
            @pl.when((chunk == 0) if number == 0 else (chunk > 0))
            def _():
                @pl.loop(0, heads)
                def _(r):
                    columns = pl.ds(pl.multiple_of(lax.bitwise_xor(where_ref[0], r) * head_dim, head_dim), head_dim)
                    for t in range(size):
                        there = pl.ds(pl.multiple_of((r * size + t) * head_dim, head_dim), head_dim)
                        full_ref[:rows, there] = context_ref[t, 0, :, columns]
                        if extra:
                            full_ref[rows:, there] = context_x_ref[t, :, columns]

    w_block = jnp.concatenate([w_ref[...].reshape(size * head_dim, block) for w_ref in w_refs], axis=0)
    acc = jnp.dot(full_ref[...], w_block, preferred_element_type=jnp.float32)
    columns = pl.ds(pl.multiple_of(step * block, block), block)
    hidden = (x_ref[...].astype(jnp.float32) + acc[:rows]).astype(jnp.bfloat16)
    hidden_ref[:, columns] = hidden
    hidden_f32 = hidden.astype(jnp.float32)
    square_ref[:rows] += jnp.sum(hidden_f32 * hidden_f32, axis=-1, keepdims=True)
    if extra:
        hidden = (x_x_ref[...].astype(jnp.float32) + acc[rows:]).astype(jnp.bfloat16)
        hidden_x_ref[:, columns] = hidden
        hidden_f32 = hidden.astype(jnp.float32)
        square_ref[rows:] += jnp.sum(hidden_f32 * hidden_f32, axis=-1, keepdims=True)

    @pl.when(step == pl.num_programs(1) - 1)
    def _():
        half = rows // 2
        inv_rms = lax.rsqrt(square_ref[...] / depth + NORM_EPS)

        @pl.loop(0, depth // block)
        def _(number):
            columns = pl.ds(pl.multiple_of(number * block, block), block)
            gain = gain_ref[:, columns].astype(jnp.float32)
            for part in range(2):
                lo, hi = part * half, (part + 1) * half
                normed_ref[part, :half, columns] = (hidden_ref[lo:hi, columns].astype(jnp.float32) * inv_rms[lo:hi] * gain).astype(jnp.bfloat16)
                if extra and part == 1:
                    normed_ref[part, half:, columns] = (hidden_x_ref[:, columns].astype(jnp.float32) * inv_rms[rows:] * gain).astype(jnp.bfloat16)
                else:
                    normed_ref[part, half:, columns] = jnp.zeros((normed_ref.shape[1] - half, block), jnp.bfloat16)


def project_out(first, count, chunks, pad, token, where, contexts, w_heads, x, gain, extras, buffers):
    rows, width = contexts[0].shape[2:]
    depth = x.shape[1]
    heads = len(w_heads)
    size, head_dim = w_heads[0].shape[:2]
    block = min(512, depth)
    total = rows + (pad if extras else 0)
    whole = lambda shape: pl.BlockSpec(shape, lambda c, n, where: (0,) * len(shape), pipeline_mode=pl.Buffered(1))
    in_specs = [whole(contexts[0].shape)]
    if count > 1:
        in_specs.append(pl.BlockSpec((size, 1, rows, width), lambda c, n, where: (0, lax.max(c - 1, 0), 0, 0)))
    in_specs += [pl.BlockSpec((size, head_dim, block), lambda c, n, where: (0, 0, n))] * heads
    in_specs += [pl.BlockSpec((rows, block), lambda c, n, where: (first + c, n)), whole((1, depth))]
    out_shape = [jax.ShapeDtypeStruct((2 * chunks, rows // 2 + pad, depth), jnp.bfloat16), jax.ShapeDtypeStruct((rows * chunks, depth), jnp.bfloat16)]
    mode = {} if count > 1 else dict(pipeline_mode=pl.Buffered(1))
    out_specs = [
        pl.BlockSpec((2, rows // 2 + pad, depth), lambda c, n, where: (first + c, 0, 0), **mode),
        pl.BlockSpec((rows, depth), lambda c, n, where: (first + c, 0), **mode),
    ]
    if extras:
        in_specs += [whole(extras[0].shape), pl.BlockSpec((pad, block), lambda c, n, where: (0, n))]
        out_shape.append(jax.ShapeDtypeStruct((pad, depth), jnp.bfloat16))
        out_specs.append(whole((pad, depth)))
    in_specs.append(pl.BlockSpec(memory_space=pl.ANY))
    out_shape.append(TOKEN)
    out_specs.append(whole(TOKEN.shape))
    aliases = {}
    if buffers:
        aliases = {1 + len(in_specs): 0, 2 + len(in_specs): 1}
        in_specs += [pl.BlockSpec(memory_space=pl.ANY)] * 2
    return pl.pallas_call(
        functools.partial(output_kernel, size, heads, len(contexts), bool(extras), bool(buffers)),
        out_shape=out_shape,
        grid_spec=pltpu.PrefetchScalarGridSpec(
            num_scalar_prefetch=1,
            grid=(count, depth // block),
            in_specs=in_specs,
            out_specs=out_specs,
            scratch_shapes=[pltpu.VMEM((total, size * width), jnp.bfloat16), pltpu.VMEM((total, 1), jnp.float32)],
        ),
        input_output_aliases=aliases,
        compiler_params=pltpu.CompilerParams(dimension_semantics=("arbitrary", "arbitrary"), vmem_limit_bytes=60 << 20),
        cost_estimate=pl.CostEstimate(flops=2 * count * total * size * width * depth, bytes_accessed=2 * count * (size * width * depth + 4 * rows * width + 3 * total * depth), transcendentals=0),
        name="project_out",
    )(where, *contexts, *w_heads, x, gain, *extras, token, *buffers)


def mlp_kernel(size, chunk_rows, ff_steps, slots, token_ref, normed_ref, hextra_ref, wgu_ref, wd_ref, h_ref, out_ref, y_ref,
               acc, landed, outgoing, finished, residual, others, activated,
               rs_send, rs_recv, ag_send, ag_recv, keep_sem, h_sem, x_send, x_recv, credit):
    step = pl.program_id(0)
    me = lax.axis_index('tp')
    depth = wd_ref.shape[1]
    chunks = (out_ref.shape[0] // chunk_rows)
    piece = outgoing.shape[2]
    per_chunk = chunk_rows // (2 * piece)
    pieces = chunks * per_chunk
    subs = per_chunk // ff_steps
    last = size - 1

    @pl.when(step == 0)
    def _():
        barrier = pltpu.get_barrier_semaphore()
        for d in range(1, size):
            pl.semaphore_signal(barrier, inc=1, device_id={'tp': lax.rem(me + d, size)}, device_id_type=pl.DeviceIdType.MESH)
        pl.semaphore_wait(barrier, size - 1)

    def own_part(chain, m):
        start = pl.multiple_of(chain * (chunk_rows // 2) + lax.rem(m, per_chunk) * piece, piece)
        return acc.at[lax.rem(lax.div(m, per_chunk), 3), pl.ds(start, piece)]

    def out_rows(chain, m):
        start = pl.multiple_of(lax.div(m, per_chunk) * chunk_rows + chain * (chunk_rows // 2) + lax.rem(m, per_chunk) * piece, piece)
        return pl.ds(start, piece)

    def exchange(slot):
        for chain in range(2):
            place = me if chain == 0 else last - me
            nearer = me - 1 if chain == 0 else me + 1
            farther = me + 1 if chain == 0 else me - 1

            def sum_copy(source, m):
                return pltpu.make_async_remote_copy(
                    src_ref=source, dst_ref=landed.at[chain, lax.rem(m, slots)], send_sem=rs_send.at[chain, lax.rem(m, 4)],
                    recv_sem=rs_recv.at[chain, lax.rem(m, slots)], device_id={'tp': nearer}, device_id_type=pl.DeviceIdType.MESH)

            def keep_copy(m):
                return pltpu.make_async_copy(finished.at[chain, lax.rem(m, 2)], out_ref.at[out_rows(chain, m)], keep_sem.at[chain, lax.rem(m, 2)])

            def h_copy(m):
                return pltpu.make_async_copy(h_ref.at[out_rows(chain, m)], residual.at[chain, lax.rem(m, 2)], h_sem.at[chain, lax.rem(m, 2)])

            def back_copy(source, m):
                return pltpu.make_async_remote_copy(
                    src_ref=source, dst_ref=out_ref.at[out_rows(chain, m)], send_sem=ag_send.at[chain, lax.rem(m, 4)],
                    recv_sem=ag_recv.at[chain, lax.rem(m, 8)], device_id={'tp': farther}, device_id_type=pl.DeviceIdType.MESH)

            @pl.when((place == last) & (slot >= 0) & (slot < pieces))
            def _():
                @pl.when(slot >= 4)
                def _():
                    sum_copy(own_part(chain, slot - 4), slot - 4).wait_send()

                @pl.when(slot >= slots)
                def _():
                    pl.semaphore_wait(credit.at[chain], 1)

                sum_copy(own_part(chain, slot), slot).start()

            m = slot - (last - place)

            @pl.when((place > 0) & (place < last) & (m >= 0) & (m < pieces))
            def _():
                @pl.when(m >= 2)
                def _():
                    sum_copy(outgoing.at[chain, lax.rem(m, 2)], m - 2).wait_send()

                sum_copy(outgoing.at[chain, lax.rem(m, 2)], m).wait_recv()
                outgoing[chain, lax.rem(m, 2)] = landed[chain, lax.rem(m, slots)] + own_part(chain, m)[...]

                @pl.when(m + slots < pieces)
                def _():
                    pl.semaphore_signal(credit.at[chain], inc=1, device_id={'tp': farther}, device_id_type=pl.DeviceIdType.MESH)

                @pl.when(m >= slots)
                def _():
                    pl.semaphore_wait(credit.at[chain], 1)

                sum_copy(outgoing.at[chain, lax.rem(m, 2)], m).start()

            m = slot - last

            @pl.when((place == 0) & (slot == 0))
            def _():
                h_copy(0).start()

            @pl.when((place == 0) & (m >= 0) & (m < pieces))
            def _():
                @pl.when(m + 1 < pieces)
                def _():
                    h_copy(m + 1).start()

                @pl.when(m >= 2)
                def _():
                    keep_copy(m - 2).wait()
                    back_copy(finished.at[chain, lax.rem(m, 2)], m - 2).wait_send()

                h_copy(m).wait()
                sum_copy(outgoing.at[chain, lax.rem(m, 2)], m).wait_recv()
                total = landed[chain, lax.rem(m, slots)] + own_part(chain, m)[...]
                finished[chain, lax.rem(m, 2)] = (residual[chain, lax.rem(m, 2)].astype(jnp.float32) + total).astype(jnp.bfloat16)

                @pl.when(m + slots < pieces)
                def _():
                    pl.semaphore_signal(credit.at[chain], inc=1, device_id={'tp': farther}, device_id_type=pl.DeviceIdType.MESH)

                keep_copy(m).start()
                back_copy(finished.at[chain, lax.rem(m, 2)], m).start()

        for chain in range(2):
            place = me if chain == 0 else last - me
            farther = me + 1 if chain == 0 else me - 1

            def relay_copy(m):
                return pltpu.make_async_remote_copy(
                    src_ref=out_ref.at[out_rows(chain, m)], dst_ref=out_ref.at[out_rows(chain, m)], send_sem=ag_send.at[chain, lax.rem(m, 4)],
                    recv_sem=ag_recv.at[chain, lax.rem(m, 8)], device_id={'tp': farther}, device_id_type=pl.DeviceIdType.MESH)

            m = slot - last - 2 * place

            @pl.when((place > 0) & (m >= 0) & (m < pieces))
            def _():
                relay_copy(m).wait_recv()

                @pl.when((place < last) & (m >= 4))
                def _():
                    relay_copy(m - 4).wait_send()

                @pl.when(place < last)
                def _():
                    relay_copy(m).start()

    def extra_copy(d):
        return pltpu.make_async_remote_copy(
            src_ref=acc.at[(chunks - 1) % 3, pl.ds(chunk_rows, others.shape[1])], dst_ref=others.at[d], send_sem=x_send.at[d - 1],
            recv_sem=x_recv.at[d - 1], device_id={'tp': lax.rem(me + d, size)}, device_id_type=pl.DeviceIdType.MESH)

    @pl.when(step == chunks * ff_steps)
    def _():
        others[0] = acc[(chunks - 1) % 3, chunk_rows:chunk_rows + others.shape[1]]
        for d in range(1, size):
            extra_copy(d).start()

    @pl.when(step == chunks * ff_steps + 4)
    def _():
        for d in range(1, size):
            extra_copy(d).wait()
        total = others[lax.rem(me, size)]
        for j in range(1, size):
            total = total + others[lax.rem(me + size - j, size)]
        y_ref[...] = (hextra_ref[:others.shape[1]].astype(jnp.float32) + total).astype(jnp.bfloat16)

    chunk = lax.div(step, ff_steps)
    block = min(1024, depth)

    def compute_gate():
        rows_in = normed_ref[0]
        dims = (((1,), (1,)), ((), ()))
        gate = lax.dot_general(rows_in, wgu_ref[0], dims, preferred_element_type=jnp.float32)
        up = lax.dot_general(rows_in, wgu_ref[1], dims, preferred_element_type=jnp.float32)
        activated[...] = (gate * jax.nn.sigmoid(gate) * up).astype(jnp.bfloat16)

    def compute_down():
        first = lax.rem(step, ff_steps) == 0
        for start in range(0, depth, block):
            part = jnp.dot(activated[...], wd_ref[:, start:start + block], preferred_element_type=jnp.float32)

            @pl.when(first)
            def _():
                acc[lax.rem(chunk, 3), :, start:start + block] = part

            @pl.when(jnp.logical_not(first))
            def _():
                acc[lax.rem(chunk, 3), :, start:start + block] += part

    @pl.loop(0, subs)
    def _(sub):
        exchange((step - ff_steps) * subs + sub)
        for part in range(2):
            pl.when((step < chunks * ff_steps) & (sub == part * subs // 2))((compute_gate, compute_down)[part])

    @pl.when(step == pl.num_programs(0) - 1)
    def _():
        for chain in range(2):
            place = me if chain == 0 else last - me
            nearer = me - 1 if chain == 0 else me + 1
            farther = me + 1 if chain == 0 else me - 1

            def sent(m):
                return pltpu.make_async_remote_copy(
                    src_ref=outgoing.at[chain, m % 2], dst_ref=landed.at[chain, m % slots], send_sem=rs_send.at[chain, m % 4],
                    recv_sem=rs_recv.at[chain, m % slots], device_id={'tp': nearer}, device_id_type=pl.DeviceIdType.MESH)

            def returned(m):
                return pltpu.make_async_remote_copy(
                    src_ref=finished.at[chain, m % 2], dst_ref=out_ref.at[pl.ds(0, piece)], send_sem=ag_send.at[chain, m % 4],
                    recv_sem=ag_recv.at[chain, m % 8], device_id={'tp': farther}, device_id_type=pl.DeviceIdType.MESH)

            @pl.when(place == last)
            def _():
                for m in range(pieces - 4, pieces):
                    sent(m).wait_send()

            @pl.when((place > 0) & (place < last))
            def _():
                for m in range(pieces - 2, pieces):
                    sent(m).wait_send()
                for m in range(pieces - 4, pieces):
                    returned(m).wait_send()

            @pl.when(place == 0)
            def _():
                for m in range(pieces - 2, pieces):
                    pltpu.make_async_copy(finished.at[chain, m % 2], out_ref.at[pl.ds(0, piece)], keep_sem.at[chain, m % 2]).wait()
                    returned(m).wait_send()


SUBSLOTS = 2


def mlp(token, normed, hextra, w_gate_up, w_down, hidden, size):
    chunks, lines, depth = normed.shape
    rows = hidden.shape[0]
    chunk_rows = rows // chunks
    ff = w_down.shape[0]
    ff_steps = 4
    piece = chunk_rows // (8 * SUBSLOTS)
    slots = 4
    pieces = chunks * 4 * SUBSLOTS
    extra = lines - chunk_rows
    seen = min(8, extra)
    steps = chunks * ff_steps
    total_steps = ff_steps + -(-(pieces + 3 * (size - 1)) // SUBSLOTS)
    ff_block = ff // ff_steps
    at_ff = lambda g: lax.select(g < steps, lax.rem(g, ff_steps), ff_steps - 1)
    at_chunk = lambda g: lax.min(lax.div(g, ff_steps), chunks - 1)
    f32, bf16 = jnp.float32, jnp.bfloat16
    return pl.pallas_call(
        functools.partial(mlp_kernel, size, chunk_rows, ff_steps, slots),
        out_shape=[jax.ShapeDtypeStruct((rows, depth), bf16), jax.ShapeDtypeStruct((seen, depth), bf16)],
        grid=(total_steps,),
        in_specs=[
            pl.BlockSpec(memory_space=pl.ANY),
            pl.BlockSpec((1, lines, depth), lambda g: (at_chunk(g), 0, 0)),
            pl.BlockSpec((extra, depth), lambda g: (0, 0), pipeline_mode=pl.Buffered(1)),
            pl.BlockSpec((2, ff_block, depth), lambda g: (0, at_ff(g), 0)),
            pl.BlockSpec((ff_block, depth), lambda g: (at_ff(g), 0)),
            pl.BlockSpec(memory_space=pl.ANY),
        ],
        out_specs=[pl.BlockSpec(memory_space=pl.ANY), pl.BlockSpec((seen, depth), lambda g: (0, 0), pipeline_mode=pl.Buffered(1))],
        scratch_shapes=[
            pltpu.VMEM((3, lines, depth), f32),
            pltpu.VMEM((2, slots, piece, depth), f32),
            pltpu.VMEM((2, 2, piece, depth), f32),
            pltpu.VMEM((2, 2, piece, depth), bf16),
            pltpu.VMEM((2, 2, piece, depth), bf16),
            pltpu.VMEM((size, seen, depth), f32),
            pltpu.VMEM((lines, ff_block), bf16),
            pltpu.SemaphoreType.DMA((2, 4)),
            pltpu.SemaphoreType.DMA((2, slots)),
            pltpu.SemaphoreType.DMA((2, 4)),
            pltpu.SemaphoreType.DMA((2, 8)),
            pltpu.SemaphoreType.DMA((2, 2)),
            pltpu.SemaphoreType.DMA((2, 2)),
            pltpu.SemaphoreType.DMA((size - 1,)),
            pltpu.SemaphoreType.DMA((size - 1,)),
            pltpu.SemaphoreType.REGULAR((2,)),
        ],
        compiler_params=pltpu.CompilerParams(dimension_semantics=("arbitrary",), vmem_limit_bytes=63 << 20, collective_id=0, has_side_effects=True),
        cost_estimate=pl.CostEstimate(flops=6 * rows * depth * ff, bytes_accessed=6 * chunks * depth * ff, transcendentals=rows * ff),
        name="mlp",
    )(token, normed, hextra, w_gate_up, w_down, hidden)


def place_kernel(size, where_ref, *refs):
    k_ref, v_ref = refs[-2:]
    for d in range(size):
        @pl.when(pl.program_id(0) == d)
        def _():
            k_ref[:, 0] = refs[d][0]
            v_ref[:, 0] = refs[d][1]


def place_caches(where, landed):
    rows, heads, head_dim = landed[0].shape[1:]
    size = len(landed)
    block = rows // 2
    blocks = rows // block

    def turn(number):
        return lambda d, n, where: (0, lax.select(d == number, n, lax.select(d < number, 0, blocks - 1)), 0, 0)

    out = pl.BlockSpec((block, 1, heads, head_dim), lambda d, n, where: (n, lax.rem(where[0] - d + size, size), 0, 0))
    return pl.pallas_call(
        functools.partial(place_kernel, size),
        out_shape=[jax.ShapeDtypeStruct((rows, size, heads, head_dim), jnp.bfloat16)] * 2,
        grid_spec=pltpu.PrefetchScalarGridSpec(
            num_scalar_prefetch=1,
            grid=(size, blocks),
            in_specs=[pl.BlockSpec((2, block, heads, head_dim), turn(d)) for d in range(size)],
            out_specs=[out, out],
        ),
        compiler_params=pltpu.CompilerParams(dimension_semantics=("arbitrary", "arbitrary"), vmem_limit_bytes=16 << 20),
        cost_estimate=pl.CostEstimate(flops=20 * rows * size * heads * head_dim, bytes_accessed=8 * size * rows * heads * head_dim, transcendentals=0),
        name="place_caches",
    )(where, *landed)


def pick_by(index, options):
    result = options[0]
    for place in range(1, len(options)):
        result = jnp.where(index == place, options[place], result)
    return result


def solution(mesh):
    side_size = mesh.shape['side']
    tp_size = mesh.shape['tp']
    seats = mesh.shape['pair'] * side_size
    group_axes = ('pair', 'side')
    last = tp_size - 1

    def cyclic(value, d):
        return lax.ppermute(value, 'tp', [(t, (t + d) % tp_size) for t in range(tp_size)])

    def swap(value, mask):
        return lax.ppermute(value, group_axes, [(q, q ^ mask) for q in range(seats)])

    def in_order(me, copies):
        return [pick_by(me, [copies[(t - j) % tp_size] for t in range(tp_size)]) for j in range(tp_size)]

    def device_fn(x_prompt, s_len, y_tok, c_len, k_cache, v_cache, attn_gain, w_qkv, w_out, mlp_gain, w_gate_up, w_down):
        me = lax.axis_index('tp')
        seat = lax.axis_index('pair') * side_size + lax.axis_index('side')
        where = seat.reshape(1).astype(jnp.int32)
        seq_len, depth = x_prompt.shape[1:]
        heads_local = w_qkv.shape[2]
        head_dim = w_qkv.shape[4]
        width = heads_local * head_dim
        rows = seq_len // tp_size
        decodes = y_tok.shape[0]
        pad = 16
        cache_local = k_cache.shape[2]
        val = {}

        def tie(keys):
            keys = list(dict.fromkeys(keys))
            for key, value in zip(keys, lax.optimization_barrier(tuple(val[key] for key in keys))):
                val[key] = value

        val['w', 0] = lax.all_gather(lax.dynamic_index_in_dim(w_out[0, :, 0], seat, 0, keepdims=False), 'tp', axis=0, tiled=False)

        val['w_all'] = jnp.swapaxes(w_qkv[0], 1, 2).reshape(depth, 3 * width)
        extra_tables = rope_tables(jnp.concatenate([c_len, jnp.zeros((pad - decodes,), jnp.int32)]), head_dim)
        y_pad = jnp.concatenate([y_tok, jnp.zeros((pad - decodes, depth), y_tok.dtype)])
        val['gain'], val['s_len'], val['mlp_gain'] = attn_gain, s_len, mlp_gain
        val['valid'] = (jnp.arange(seq_len) < s_len[0]).astype(jnp.bfloat16)
        buffers = []
        qkv = []

        def compute(name):
            kind = name[0]
            c = int(name[1:]) if name[1:].isdigit() else 0
            if kind == 'Q':
                tie(thread + ['gain'])
                made = project_qkv(c, rows, val['token'], x_prompt[0], y_pad if c == 0 else None, val['gain'], val['w_all'], extra_tables, head_dim)
                val['token'] = made[3]
                qkv.append(made[:3])
                if c == 0:
                    val['dq', 0] = jnp.stack([part[:decodes].reshape(decodes, heads_local, head_dim) for part in made[4:]])
                    for d in range(1, tp_size):
                        val['dq', d] = cyclic(val['dq', 0], d)
                return ['token']
            if kind == 'T':
                tie(thread + ['s_len'])
                val['context', c], val['token'] = attend(c, tp_size, rows, val['token'], val['s_len'], *zip(*qkv), head_dim)
                return ['token']
            if kind == 'G':
                val['gathered', name[1:]] = lax.all_gather(jnp.stack([val['context', int(digit)] for digit in name[1:]]), 'tp', axis=0, tiled=False)
                return ['token']
            if kind == 'K':
                tie(thread + ['valid'])
                for d in range(tp_size):
                    made = []
                    keep = pick_by(me, [val['valid'][((t + d) % tp_size) * rows:((t + d) % tp_size + 1) * rows] for t in range(tp_size)])
                    for which in (1, 2):
                        rows_d = pick_by(me, [qkv[(t + d) % tp_size // 2][which][(t + d) % tp_size % 2 * rows:][:rows].reshape(rows, heads_local, head_dim) for t in range(tp_size)])
                        made.append(rows_d * keep[:, None, None])
                    val['kv', d] = jnp.stack(made)
                return []
            if name == 'D1':
                tie(thread + [('dq', d) for d in range(tp_size)])
                dec_full = jnp.concatenate(in_order(me, [val['dq', d] for d in range(tp_size)]), axis=2)
                cache_pos = me * cache_local + jnp.arange(cache_local)
                write_mask = (cache_pos[None, :] == c_len[:, None])[:, :, None, None]
                allowed = (cache_pos[None, :] <= c_len[:, None])[:, :, None]
                key_now = jnp.where(write_mask, dec_full[1][:, None], k_cache[0])
                value_now = jnp.where(write_mask, dec_full[2][:, None], v_cache[0])
                val['key_now'], val['value_now'] = key_now, value_now
                scores = jnp.sum(dec_full[0][:, None].astype(jnp.float32) * key_now.astype(jnp.float32), axis=-1) * head_dim ** -0.5
                scores = jnp.where(allowed, scores, -1e30)
                peak = jnp.max(scores, axis=1, keepdims=True)
                weights = jnp.exp(scores - peak)
                total = jnp.sum(weights, axis=1)[..., None]
                peak = peak[:, 0, :, None]
                mixed = jnp.sum(weights.astype(jnp.bfloat16).astype(jnp.float32)[..., None] * value_now.astype(jnp.float32), axis=1)
                packed = jnp.stack([mixed, jnp.broadcast_to(peak, mixed.shape), jnp.broadcast_to(total, mixed.shape)])
                packed = packed.reshape(3, decodes, tp_size, heads_local, head_dim)
                for d in range(tp_size):
                    share = lax.dynamic_index_in_dim(packed, lax.rem(me + d, tp_size), 2, keepdims=False)
                    val['ds', d] = share if d == 0 else cyclic(share, d)
                return [('ds', 0)]
            if name == 'D2':
                tie(thread + [('ds', d) for d in range(tp_size)])
                shares = [val['ds', d] for d in range(tp_size)]
                top = functools.reduce(jnp.maximum, [share[1] for share in shares])
                factors = [jnp.exp(share[1] - top) for share in shares]
                dec_mixed = sum(share[0] * factor for share, factor in zip(shares, factors))
                dec_total = sum(share[2] * factor for share, factor in zip(shares, factors))
                val['dc', 0] = (dec_mixed / dec_total).astype(jnp.bfloat16).reshape(decodes, width)
                for d in range(1, tp_size):
                    val['dc', d] = cyclic(val['dc', 0], d)
                return [('dc', 0)]
            if kind == 'O':
                w_keys = [('w', r) for r in range(seats)]
                final = c == last
                parts = [('gathered', '3')] if final else [('gathered', '0'), ('gathered', '12')]
                extra_keys = [('dc', d) for d in range(tp_size)] if final else []
                tie(thread + ['mlp_gain'] + parts + extra_keys + ([] if final else w_keys))
                extras = []
                if final:
                    extras = [jnp.pad(jnp.stack(in_order(me, [val[key] for key in extra_keys])), ((0, 0), (0, pad - decodes), (0, 0))), y_pad]
                made = project_out(last if final else 0, 1 if final else last, tp_size, pad, val['token'], where, [val[key] for key in parts], [val[key] for key in w_keys], x_prompt[0], val['mlp_gain'], extras, [val[key] for key in buffers])
                buffers[:] = ['normed', 'h']
                val['normed'], val['h'], val['token'] = made[0], made[1], made[-1]
                if final:
                    val['hx'] = made[2]
                return ['token']
            if kind == 'P':
                tie(thread + [('landed', d) for d in range(tp_size)])
                val['k'], val['v'] = place_caches(me.reshape(1).astype(jnp.int32), [val['landed', d] for d in range(tp_size)])
                return ['k']
            val['out'], val['y'] = mlp(val['token'], val['normed'], val['hx'], jnp.transpose(w_gate_up[0], (1, 2, 0)), w_down[0], val['h'], tp_size)
            return ['y']

        def transfer(name):
            if name[0] == 'k':
                d = int(name[1])
                tie(thread + [('kv', d)])
                route = [(t * side_size + s, ((t + d) % tp_size) * side_size + (s + 1) % side_size) for t in range(tp_size) for s in range(side_size)]
                val['landed', d] = lax.ppermute(val['kv', d], ('tp', 'side'), route)
                return
            bases = [0] if name == 'w2' else list(range(0, seats, 2))
            kept = [] if name == 'w2' else [('kv', 0), ('kv', 2)]
            tie(thread + kept + [('w', base) for base in bases])
            for mask in (range(2, seats, 2) if name == 'w2' else [1]):
                for base in bases:
                    val['w', base ^ mask] = swap(val['w', base], mask)

        val['token'] = jnp.zeros(TOKEN.shape, TOKEN.dtype)
        thread = ['token']
        for name in ORDER:
            if name[0] in 'QTGKDOBP':
                made = compute(name)
                thread = thread + made if name in ('K', 'D1', 'D2') else made
            else:
                transfer(name)

        caches = [val[name].reshape(1, 1, rows, tp_size * heads_local, head_dim) for name in 'kv']
        return (val['out'][None], val['y'][:decodes], caches[0], caches[1], val['key_now'][None], val['value_now'][None])

    cache_spec = P(None, group_axes, 'tp', None, None)
    in_specs = (P(group_axes, None, None), P(group_axes), P(group_axes, None), P(group_axes), cache_spec, cache_spec, P(), P(None, None, 'tp', None, None), P(None, 'tp', None, None, None), P(), P(None, None, None, 'tp'), P(None, 'tp', None))
    out_specs = (P(group_axes, None, None), P(group_axes, None), cache_spec, cache_spec, cache_spec, cache_spec)
    return jax.shard_map(device_fn, mesh=mesh, in_specs=in_specs, out_specs=out_specs, check_vma=False)
```

```python
import functools

import jax
import jax.numpy as jnp
from jax import lax
from jax.experimental import pallas as pl
from jax.experimental.pallas import tpu as pltpu
from jax.sharding import PartitionSpec as P


ROPE_BASE = 10000.0
NORM_EPS = 1e-5

ORDER = (
    'Q0', 'T0', 'G0', 'T1', 'w2', 'Q1', 'T2', 'G12', 'T3', 'G3', 'K', 'k1', 'k3', 'D1', 'w3', 'O012', 'D2', 'k0', 'k2',
    'O3', 'B', 'P',
)


def rms_scale(values_f32, gain_f32):
    inv_rms = lax.rsqrt(jnp.mean(values_f32 * values_f32, axis=-1, keepdims=True) + NORM_EPS)
    return (values_f32 * inv_rms * gain_f32).astype(jnp.bfloat16)


def rope_frequencies(head_dim):
    half_dim = head_dim // 2
    inv_freq = ROPE_BASE ** (-2.0 * jnp.arange(half_dim, dtype=jnp.float32) / head_dim)
    return jnp.concatenate([inv_freq, inv_freq])[None]


def rope_tables(positions, head_dim):
    angles = positions.astype(jnp.float32)[:, None] * rope_frequencies(head_dim)
    sign = jnp.where(jnp.arange(head_dim) < head_dim // 2, -1.0, 1.0)
    return jnp.cos(angles), jnp.sin(angles) * sign[None]


def rope_rows(first, rows, freq):
    head_dim = freq.shape[1]
    positions = lax.broadcasted_iota(jnp.int32, (rows, head_dim), 0) + first
    angles = positions.astype(jnp.float32) * freq
    turns = jnp.floor(angles * 0.15915494309189535 + 0.5)
    angles = (angles - turns * 6.28125) - turns * 0.0019353071795864769
    sine = jnp.sin(angles)
    return jnp.cos(angles), jnp.where(lax.broadcasted_iota(jnp.int32, (rows, head_dim), 1) < head_dim // 2, -sine, sine)


def qkv_kernel(half, head_dim, extra, *refs):
    x_ref, gain_ref, wq_ref, wk_ref, wv_ref, freq_ref = refs[:6]
    extra_refs = refs[6:9] if extra else None
    normed_ref, cos_ref, sin_ref = refs[-3:]
    q_ref, k_ref, v_ref, token_ref = refs[-7 - 3 * extra:-3 - 3 * extra]
    extra_outs = refs[-6:-3] if extra else (None,) * 3
    rows = x_ref.shape[0]
    chunk = pl.program_id(1)

    @pl.when(pl.program_id(0) == 0)
    def _():
        gain = gain_ref[...].astype(jnp.float32)
        block = min(64, rows)

        @pl.loop(0, rows // block)
        def _(number):
            lines = pl.ds(pl.multiple_of(number * block, block), block)
            normed_ref[chunk, lines] = rms_scale(x_ref[lines].astype(jnp.float32), gain)
            cos_ref[chunk, lines], sin_ref[chunk, lines] = rope_rows((2 * half + chunk) * rows + number * block, block, freq_ref[...])

        if extra:
            normed_ref[chunk, rows:] = rms_scale(extra_refs[0][...].astype(jnp.float32), gain)
        token_ref[...] = jnp.zeros_like(token_ref)

    cos, sin = cos_ref[chunk], sin_ref[chunk]
    if extra:
        cos = jnp.concatenate([cos, extra_refs[1][...]], axis=0)
        sin = jnp.concatenate([sin, extra_refs[2][...]], axis=0)
    for w_ref, out_ref, extra_out in zip((wq_ref, wk_ref, wv_ref), (q_ref, k_ref, v_ref), extra_outs):
        acc = jnp.dot(normed_ref[chunk], w_ref[...], preferred_element_type=jnp.float32)
        for start in range(0, acc.shape[1], head_dim):
            vals = acc[:, start:start + head_dim]
            if out_ref is not v_ref:
                vals = vals * cos + pltpu.roll(vals, head_dim // 2, 1) * sin
            out_ref[:, start:start + head_dim] = vals[:rows].astype(out_ref.dtype)
            if extra:
                extra_out[:, start:start + head_dim] = vals[rows:].astype(out_ref.dtype)


TOKEN = jax.ShapeDtypeStruct((8, 128), jnp.float32)


def project_qkv(half, rows, token, x, extra_rows, gain, w_all, extra_tables, head_dim):
    depth = x.shape[1]
    width = w_all.shape[1] // 3
    block = 2 * head_dim
    steps = width // block
    extra = extra_rows is not None
    extras = [extra_rows, *extra_tables] if extra else []
    pad = extra_rows.shape[0] if extra else 0
    bf16 = jnp.bfloat16
    whole = lambda shape: pl.BlockSpec(shape, lambda n, c: (0, 0), pipeline_mode=pl.Buffered(1))
    columns = lambda part: pl.BlockSpec((depth, block), lambda n, c: (0, part * steps + n))
    extra_outs = [jax.ShapeDtypeStruct((pad, width), bf16)] * 3 if extra else []
    return pl.pallas_call(
        functools.partial(qkv_kernel, half, head_dim, extra),
        out_shape=[jax.ShapeDtypeStruct((2 * rows, width), bf16)] * 3 + [TOKEN] + extra_outs,
        grid=(steps, 2),
        in_specs=[
            pl.BlockSpec((rows, depth), lambda n, c: (2 * half + lax.select(n == 0, c, 1), 0)),
            whole((1, depth)),
            columns(0),
            columns(1),
            columns(2),
            whole((1, head_dim)),
        ] + [whole(e.shape) for e in extras] + [pl.BlockSpec(memory_space=pl.ANY)],
        out_specs=[pl.BlockSpec((rows, block), lambda n, c: (c, n))] * 3 + [whole(TOKEN.shape)] + [pl.BlockSpec((pad, block), lambda n, c: (0, n))] * len(extra_outs),
        scratch_shapes=[pltpu.VMEM((2, rows + pad, depth), bf16)] + [pltpu.VMEM((2, rows, head_dim), jnp.float32)] * 2,
        compiler_params=pltpu.CompilerParams(dimension_semantics=("arbitrary", "arbitrary"), vmem_limit_bytes=56 << 20),
        cost_estimate=pl.CostEstimate(flops=12 * rows * depth * width, bytes_accessed=2 * (2 * rows * depth + 3 * depth * width + 6 * rows * width), transcendentals=0),
        name="project_qkv",
    )(x, gain, w_all, w_all, w_all, rope_frequencies(head_dim), *extras, token)


def attend_kernel(chunk, first_checked, q_rows, slen_ref, *refs):
    q_ref = refs[0]
    k_refs = refs[1:chunk + 2]
    v_refs = refs[chunk + 2:2 * chunk + 3]
    out_ref, token_ref = refs[-2:]
    token_ref[...] = jnp.zeros_like(token_ref)
    rows, head_dim = q_ref.shape
    scale = head_dim ** -0.5
    limit = slen_ref[0]

    @pl.loop(0, rows // q_rows)
    def _(number):
        start = pl.multiple_of(number * q_rows, q_rows)
        query = q_ref[pl.ds(start, q_rows), :]
        scores = []
        for part in range(chunk + 1):
            score = lax.dot_general(query, k_refs[part][...], (((1,), (1,)), ((), ())), preferred_element_type=jnp.float32) * scale
            key_pos = lax.broadcasted_iota(jnp.int32, score.shape, 1)
            if part == chunk:
                allowed = key_pos <= lax.broadcasted_iota(jnp.int32, score.shape, 0) + start
                if part >= first_checked:
                    allowed = allowed & (key_pos < limit - part * rows)
                score = jnp.where(allowed, score, -1e30)
            elif part >= first_checked:
                score = jnp.where(key_pos < limit - part * rows, score, -1e30)
            scores.append(score)
        peak = functools.reduce(jnp.maximum, [jnp.max(score, axis=-1, keepdims=True) for score in scores])
        total = jnp.zeros((q_rows, 1), jnp.float32)
        mixed = jnp.zeros((q_rows, head_dim), jnp.float32)
        for score, v_ref in zip(scores, v_refs):
            weight = jnp.exp(score - peak)
            total = total + jnp.sum(weight, axis=-1, keepdims=True)
            mixed = mixed + jnp.dot(weight.astype(jnp.bfloat16), v_ref[...], preferred_element_type=jnp.float32)
        out_ref[pl.ds(start, q_rows), :] = (mixed / total).astype(out_ref.dtype)


def attend(chunk, chunks, rows, token, s_len, queries, keys, values, head_dim):
    width = queries[0].shape[1]
    heads = width // head_dim

    pick = lambda c: pl.BlockSpec((rows, head_dim), lambda h, slen: (c % 2, h))
    every = range(chunk + 1)
    total_keys = rows * (chunk + 1)
    return pl.pallas_call(
        functools.partial(attend_kernel, chunk, chunks // 2, min(256, rows)),
        out_shape=[jax.ShapeDtypeStruct((rows, width), jnp.bfloat16), TOKEN],
        grid_spec=pltpu.PrefetchScalarGridSpec(
            num_scalar_prefetch=1,
            grid=(heads,),
            in_specs=[pick(c) for c in (chunk, *every, *every)] + [pl.BlockSpec(memory_space=pl.ANY)],
            out_specs=[pick(0), pl.BlockSpec(TOKEN.shape, lambda h, slen: (0, 0))],
        ),
        compiler_params=pltpu.CompilerParams(dimension_semantics=("arbitrary",), vmem_limit_bytes=48 << 20),
        cost_estimate=pl.CostEstimate(flops=8 * heads * rows * total_keys * head_dim, bytes_accessed=2 * width * (2 * total_keys + 2 * rows), transcendentals=heads * rows * total_keys),
    )(s_len, queries[chunk // 2], *[keys[c // 2] for c in every], *[values[c // 2] for c in every], token)


def output_kernel(size, heads, contexts, extra, aliased, where_ref, *refs):
    context_refs, refs = refs[:contexts], refs[contexts:]
    w_refs, refs = refs[:heads], refs[heads:]
    x_ref, gain_ref, refs = refs[0], refs[1], refs[2:]
    if extra:
        context_x_ref, x_x_ref, refs = refs[0], refs[1], refs[2:]
    refs = refs[1:]
    if aliased:
        refs = refs[2:]
    normed_ref, hidden_ref, refs = refs[0], refs[1], refs[2:]
    if extra:
        hidden_x_ref, refs = refs[0], refs[1:]
    token_ref, full_ref, square_ref = refs
    rows, depth = hidden_ref.shape
    head_dim, block = w_refs[0].shape[1:]
    chunk, step = pl.program_id(0), pl.program_id(1)

    @pl.when(step == 0)
    def _():
        square_ref[...] = jnp.zeros_like(square_ref)
        token_ref[...] = jnp.zeros_like(token_ref)
        for number, context_ref in enumerate(context_refs):
            @pl.when((chunk == 0) if number == 0 else (chunk > 0))
            def _():
                @pl.loop(0, heads)
                def _(r):
                    columns = pl.ds(pl.multiple_of(lax.bitwise_xor(where_ref[0], r) * head_dim, head_dim), head_dim)
                    for t in range(size):
                        there = pl.ds(pl.multiple_of((r * size + t) * head_dim, head_dim), head_dim)
                        full_ref[:rows, there] = context_ref[t, 0, :, columns]
                        if extra:
                            full_ref[rows:, there] = context_x_ref[t, :, columns]

    w_block = jnp.concatenate([w_ref[...].reshape(size * head_dim, block) for w_ref in w_refs], axis=0)
    acc = jnp.dot(full_ref[...], w_block, preferred_element_type=jnp.float32)
    columns = pl.ds(pl.multiple_of(step * block, block), block)
    hidden = (x_ref[...].astype(jnp.float32) + acc[:rows]).astype(jnp.bfloat16)
    hidden_ref[:, columns] = hidden
    hidden_f32 = hidden.astype(jnp.float32)
    square_ref[:rows] += jnp.sum(hidden_f32 * hidden_f32, axis=-1, keepdims=True)
    if extra:
        hidden = (x_x_ref[...].astype(jnp.float32) + acc[rows:]).astype(jnp.bfloat16)
        hidden_x_ref[:, columns] = hidden
        hidden_f32 = hidden.astype(jnp.float32)
        square_ref[rows:] += jnp.sum(hidden_f32 * hidden_f32, axis=-1, keepdims=True)

    @pl.when(step == pl.num_programs(1) - 1)
    def _():
        half = rows // 2
        inv_rms = lax.rsqrt(square_ref[...] / depth + NORM_EPS)

        @pl.loop(0, depth // block)
        def _(number):
            columns = pl.ds(pl.multiple_of(number * block, block), block)
            gain = gain_ref[:, columns].astype(jnp.float32)
            for part in range(2):
                lo, hi = part * half, (part + 1) * half
                normed_ref[part, :half, columns] = (hidden_ref[lo:hi, columns].astype(jnp.float32) * inv_rms[lo:hi] * gain).astype(jnp.bfloat16)
                if extra and part == 1:
                    normed_ref[part, half:, columns] = (hidden_x_ref[:, columns].astype(jnp.float32) * inv_rms[rows:] * gain).astype(jnp.bfloat16)
                else:
                    normed_ref[part, half:, columns] = jnp.zeros((normed_ref.shape[1] - half, block), jnp.bfloat16)


def project_out(first, count, chunks, pad, token, where, contexts, w_heads, x, gain, extras, buffers):
    rows, width = contexts[0].shape[2:]
    depth = x.shape[1]
    heads = len(w_heads)
    size, head_dim = w_heads[0].shape[:2]
    block = min(512, depth)
    total = rows + (pad if extras else 0)
    whole = lambda shape: pl.BlockSpec(shape, lambda c, n, where: (0,) * len(shape), pipeline_mode=pl.Buffered(1))
    in_specs = [whole(contexts[0].shape)]
    if count > 1:
        in_specs.append(pl.BlockSpec((size, 1, rows, width), lambda c, n, where: (0, lax.max(c - 1, 0), 0, 0)))
    in_specs += [pl.BlockSpec((size, head_dim, block), lambda c, n, where: (0, 0, n))] * heads
    in_specs += [pl.BlockSpec((rows, block), lambda c, n, where: (first + c, n)), whole((1, depth))]
    out_shape = [jax.ShapeDtypeStruct((2 * chunks, rows // 2 + pad, depth), jnp.bfloat16), jax.ShapeDtypeStruct((rows * chunks, depth), jnp.bfloat16)]
    mode = {} if count > 1 else dict(pipeline_mode=pl.Buffered(1))
    out_specs = [
        pl.BlockSpec((2, rows // 2 + pad, depth), lambda c, n, where: (first + c, 0, 0), **mode),
        pl.BlockSpec((rows, depth), lambda c, n, where: (first + c, 0), **mode),
    ]
    if extras:
        in_specs += [whole(extras[0].shape), pl.BlockSpec((pad, block), lambda c, n, where: (0, n))]
        out_shape.append(jax.ShapeDtypeStruct((pad, depth), jnp.bfloat16))
        out_specs.append(whole((pad, depth)))
    in_specs.append(pl.BlockSpec(memory_space=pl.ANY))
    out_shape.append(TOKEN)
    out_specs.append(whole(TOKEN.shape))
    aliases = {}
    if buffers:
        aliases = {1 + len(in_specs): 0, 2 + len(in_specs): 1}
        in_specs += [pl.BlockSpec(memory_space=pl.ANY)] * 2
    return pl.pallas_call(
        functools.partial(output_kernel, size, heads, len(contexts), bool(extras), bool(buffers)),
        out_shape=out_shape,
        grid_spec=pltpu.PrefetchScalarGridSpec(
            num_scalar_prefetch=1,
            grid=(count, depth // block),
            in_specs=in_specs,
            out_specs=out_specs,
            scratch_shapes=[pltpu.VMEM((total, size * width), jnp.bfloat16), pltpu.VMEM((total, 1), jnp.float32)],
        ),
        input_output_aliases=aliases,
        compiler_params=pltpu.CompilerParams(dimension_semantics=("arbitrary", "arbitrary"), vmem_limit_bytes=60 << 20),
        cost_estimate=pl.CostEstimate(flops=2 * count * total * size * width * depth, bytes_accessed=2 * count * (size * width * depth + 4 * rows * width + 3 * total * depth), transcendentals=0),
        name="project_out",
    )(where, *contexts, *w_heads, x, gain, *extras, token, *buffers)


def mlp_kernel(size, chunk_rows, ff_steps, slots, token_ref, normed_ref, hextra_ref, wgu_ref, wd_ref, h_ref, out_ref, y_ref,
               acc, landed, outgoing, finished, residual, others, activated,
               rs_send, rs_recv, ag_send, ag_recv, keep_sem, h_sem, x_send, x_recv, credit):
    step = pl.program_id(0)
    me = lax.axis_index('tp')
    depth = wd_ref.shape[1]
    chunks = (out_ref.shape[0] // chunk_rows)
    piece = outgoing.shape[2]
    per_chunk = chunk_rows // (2 * piece)
    pieces = chunks * per_chunk
    subs = per_chunk // ff_steps
    last = size - 1

    @pl.when(step == 0)
    def _():
        barrier = pltpu.get_barrier_semaphore()
        for d in range(1, size):
            pl.semaphore_signal(barrier, inc=1, device_id={'tp': lax.rem(me + d, size)}, device_id_type=pl.DeviceIdType.MESH)
        pl.semaphore_wait(barrier, size - 1)

    def own_part(chain, m):
        start = pl.multiple_of(chain * (chunk_rows // 2) + lax.rem(m, per_chunk) * piece, piece)
        return acc.at[lax.rem(lax.div(m, per_chunk), 3), pl.ds(start, piece)]

    def out_rows(chain, m):
        start = pl.multiple_of(lax.div(m, per_chunk) * chunk_rows + chain * (chunk_rows // 2) + lax.rem(m, per_chunk) * piece, piece)
        return pl.ds(start, piece)

    def exchange(slot):
        for chain in range(2):
            place = me if chain == 0 else last - me
            nearer = me - 1 if chain == 0 else me + 1
            farther = me + 1 if chain == 0 else me - 1

            def sum_copy(source, m):
                return pltpu.make_async_remote_copy(
                    src_ref=source, dst_ref=landed.at[chain, lax.rem(m, slots)], send_sem=rs_send.at[chain, lax.rem(m, 4)],
                    recv_sem=rs_recv.at[chain, lax.rem(m, slots)], device_id={'tp': nearer}, device_id_type=pl.DeviceIdType.MESH)

            def keep_copy(m):
                return pltpu.make_async_copy(finished.at[chain, lax.rem(m, 2)], out_ref.at[out_rows(chain, m)], keep_sem.at[chain, lax.rem(m, 2)])

            def h_copy(m):
                return pltpu.make_async_copy(h_ref.at[out_rows(chain, m)], residual.at[chain, lax.rem(m, 2)], h_sem.at[chain, lax.rem(m, 2)])

            def back_copy(source, m):
                return pltpu.make_async_remote_copy(
                    src_ref=source, dst_ref=out_ref.at[out_rows(chain, m)], send_sem=ag_send.at[chain, lax.rem(m, 4)],
                    recv_sem=ag_recv.at[chain, lax.rem(m, 8)], device_id={'tp': farther}, device_id_type=pl.DeviceIdType.MESH)

            @pl.when((place == last) & (slot >= 0) & (slot < pieces))
            def _():
                @pl.when(slot >= 4)
                def _():
                    sum_copy(own_part(chain, slot - 4), slot - 4).wait_send()

                @pl.when(slot >= slots)
                def _():
                    pl.semaphore_wait(credit.at[chain], 1)

                sum_copy(own_part(chain, slot), slot).start()

            m = slot - (last - place)

            @pl.when((place > 0) & (place < last) & (m >= 0) & (m < pieces))
            def _():
                @pl.when(m >= 2)
                def _():
                    sum_copy(outgoing.at[chain, lax.rem(m, 2)], m - 2).wait_send()

                sum_copy(outgoing.at[chain, lax.rem(m, 2)], m).wait_recv()
                outgoing[chain, lax.rem(m, 2)] = landed[chain, lax.rem(m, slots)] + own_part(chain, m)[...]

                @pl.when(m + slots < pieces)
                def _():
                    pl.semaphore_signal(credit.at[chain], inc=1, device_id={'tp': farther}, device_id_type=pl.DeviceIdType.MESH)

                @pl.when(m >= slots)
                def _():
                    pl.semaphore_wait(credit.at[chain], 1)

                sum_copy(outgoing.at[chain, lax.rem(m, 2)], m).start()

            m = slot - last

            @pl.when((place == 0) & (slot == 0))
            def _():
                h_copy(0).start()

            @pl.when((place == 0) & (m >= 0) & (m < pieces))
            def _():
                @pl.when(m + 1 < pieces)
                def _():
                    h_copy(m + 1).start()

                @pl.when(m >= 2)
                def _():
                    keep_copy(m - 2).wait()
                    back_copy(finished.at[chain, lax.rem(m, 2)], m - 2).wait_send()

                h_copy(m).wait()
                sum_copy(outgoing.at[chain, lax.rem(m, 2)], m).wait_recv()
                total = landed[chain, lax.rem(m, slots)] + own_part(chain, m)[...]
                finished[chain, lax.rem(m, 2)] = (residual[chain, lax.rem(m, 2)].astype(jnp.float32) + total).astype(jnp.bfloat16)

                @pl.when(m + slots < pieces)
                def _():
                    pl.semaphore_signal(credit.at[chain], inc=1, device_id={'tp': farther}, device_id_type=pl.DeviceIdType.MESH)

                keep_copy(m).start()
                back_copy(finished.at[chain, lax.rem(m, 2)], m).start()

        for chain in range(2):
            place = me if chain == 0 else last - me
            farther = me + 1 if chain == 0 else me - 1

            def relay_copy(m):
                return pltpu.make_async_remote_copy(
                    src_ref=out_ref.at[out_rows(chain, m)], dst_ref=out_ref.at[out_rows(chain, m)], send_sem=ag_send.at[chain, lax.rem(m, 4)],
                    recv_sem=ag_recv.at[chain, lax.rem(m, 8)], device_id={'tp': farther}, device_id_type=pl.DeviceIdType.MESH)

            m = slot - last - 2 * place

            @pl.when((place > 0) & (m >= 0) & (m < pieces))
            def _():
                relay_copy(m).wait_recv()

                @pl.when((place < last) & (m >= 4))
                def _():
                    relay_copy(m - 4).wait_send()

                @pl.when(place < last)
                def _():
                    relay_copy(m).start()

    def extra_copy(d):
        return pltpu.make_async_remote_copy(
            src_ref=acc.at[(chunks - 1) % 3, pl.ds(chunk_rows, others.shape[1])], dst_ref=others.at[d], send_sem=x_send.at[d - 1],
            recv_sem=x_recv.at[d - 1], device_id={'tp': lax.rem(me + d, size)}, device_id_type=pl.DeviceIdType.MESH)

    @pl.when(step == chunks * ff_steps)
    def _():
        others[0] = acc[(chunks - 1) % 3, chunk_rows:chunk_rows + others.shape[1]]
        for d in range(1, size):
            extra_copy(d).start()

    @pl.when(step == chunks * ff_steps + 4)
    def _():
        for d in range(1, size):
            extra_copy(d).wait()
        total = others[lax.rem(me, size)]
        for j in range(1, size):
            total = total + others[lax.rem(me + size - j, size)]
        y_ref[...] = (hextra_ref[:others.shape[1]].astype(jnp.float32) + total).astype(jnp.bfloat16)

    chunk = lax.div(step, ff_steps)
    block = min(1024, depth)

    def compute_gate():
        rows_in = normed_ref[0]
        dims = (((1,), (1,)), ((), ()))
        gate = lax.dot_general(rows_in, wgu_ref[0], dims, preferred_element_type=jnp.float32)
        up = lax.dot_general(rows_in, wgu_ref[1], dims, preferred_element_type=jnp.float32)
        activated[...] = (gate * jax.nn.sigmoid(gate) * up).astype(jnp.bfloat16)

    def compute_down():
        first = lax.rem(step, ff_steps) == 0
        for start in range(0, depth, block):
            part = jnp.dot(activated[...], wd_ref[:, start:start + block], preferred_element_type=jnp.float32)

            @pl.when(first)
            def _():
                acc[lax.rem(chunk, 3), :, start:start + block] = part

            @pl.when(jnp.logical_not(first))
            def _():
                acc[lax.rem(chunk, 3), :, start:start + block] += part

    @pl.loop(0, subs)
    def _(sub):
        exchange((step - ff_steps) * subs + sub)
        for part in range(2):
            pl.when((step < chunks * ff_steps) & (sub == part * subs // 2))((compute_gate, compute_down)[part])

    @pl.when(step == pl.num_programs(0) - 1)
    def _():
        for chain in range(2):
            place = me if chain == 0 else last - me
            nearer = me - 1 if chain == 0 else me + 1
            farther = me + 1 if chain == 0 else me - 1

            def sent(m):
                return pltpu.make_async_remote_copy(
                    src_ref=outgoing.at[chain, m % 2], dst_ref=landed.at[chain, m % slots], send_sem=rs_send.at[chain, m % 4],
                    recv_sem=rs_recv.at[chain, m % slots], device_id={'tp': nearer}, device_id_type=pl.DeviceIdType.MESH)

            def returned(m):
                return pltpu.make_async_remote_copy(
                    src_ref=finished.at[chain, m % 2], dst_ref=out_ref.at[pl.ds(0, piece)], send_sem=ag_send.at[chain, m % 4],
                    recv_sem=ag_recv.at[chain, m % 8], device_id={'tp': farther}, device_id_type=pl.DeviceIdType.MESH)

            @pl.when(place == last)
            def _():
                for m in range(pieces - 4, pieces):
                    sent(m).wait_send()

            @pl.when((place > 0) & (place < last))
            def _():
                for m in range(pieces - 2, pieces):
                    sent(m).wait_send()
                for m in range(pieces - 4, pieces):
                    returned(m).wait_send()

            @pl.when(place == 0)
            def _():
                for m in range(pieces - 2, pieces):
                    pltpu.make_async_copy(finished.at[chain, m % 2], out_ref.at[pl.ds(0, piece)], keep_sem.at[chain, m % 2]).wait()
                    returned(m).wait_send()


SUBSLOTS = 2


def mlp(token, normed, hextra, w_gate_up, w_down, hidden, size):
    chunks, lines, depth = normed.shape
    rows = hidden.shape[0]
    chunk_rows = rows // chunks
    ff = w_down.shape[0]
    ff_steps = 4
    piece = chunk_rows // (8 * SUBSLOTS)
    slots = 4
    pieces = chunks * 4 * SUBSLOTS
    extra = lines - chunk_rows
    seen = min(8, extra)
    steps = chunks * ff_steps
    total_steps = ff_steps + -(-(pieces + 3 * (size - 1)) // SUBSLOTS)
    ff_block = ff // ff_steps
    at_ff = lambda g: lax.select(g < steps, lax.rem(g, ff_steps), ff_steps - 1)
    at_chunk = lambda g: lax.min(lax.div(g, ff_steps), chunks - 1)
    f32, bf16 = jnp.float32, jnp.bfloat16
    return pl.pallas_call(
        functools.partial(mlp_kernel, size, chunk_rows, ff_steps, slots),
        out_shape=[jax.ShapeDtypeStruct((rows, depth), bf16), jax.ShapeDtypeStruct((seen, depth), bf16)],
        grid=(total_steps,),
        in_specs=[
            pl.BlockSpec(memory_space=pl.ANY),
            pl.BlockSpec((1, lines, depth), lambda g: (at_chunk(g), 0, 0)),
            pl.BlockSpec((extra, depth), lambda g: (0, 0), pipeline_mode=pl.Buffered(1)),
            pl.BlockSpec((2, ff_block, depth), lambda g: (0, at_ff(g), 0)),
            pl.BlockSpec((ff_block, depth), lambda g: (at_ff(g), 0)),
            pl.BlockSpec(memory_space=pl.ANY),
        ],
        out_specs=[pl.BlockSpec(memory_space=pl.ANY), pl.BlockSpec((seen, depth), lambda g: (0, 0), pipeline_mode=pl.Buffered(1))],
        scratch_shapes=[
            pltpu.VMEM((3, lines, depth), f32),
            pltpu.VMEM((2, slots, piece, depth), f32),
            pltpu.VMEM((2, 2, piece, depth), f32),
            pltpu.VMEM((2, 2, piece, depth), bf16),
            pltpu.VMEM((2, 2, piece, depth), bf16),
            pltpu.VMEM((size, seen, depth), f32),
            pltpu.VMEM((lines, ff_block), bf16),
            pltpu.SemaphoreType.DMA((2, 4)),
            pltpu.SemaphoreType.DMA((2, slots)),
            pltpu.SemaphoreType.DMA((2, 4)),
            pltpu.SemaphoreType.DMA((2, 8)),
            pltpu.SemaphoreType.DMA((2, 2)),
            pltpu.SemaphoreType.DMA((2, 2)),
            pltpu.SemaphoreType.DMA((size - 1,)),
            pltpu.SemaphoreType.DMA((size - 1,)),
            pltpu.SemaphoreType.REGULAR((2,)),
        ],
        compiler_params=pltpu.CompilerParams(dimension_semantics=("arbitrary",), vmem_limit_bytes=63 << 20, collective_id=0, has_side_effects=True),
        cost_estimate=pl.CostEstimate(flops=6 * rows * depth * ff, bytes_accessed=6 * chunks * depth * ff, transcendentals=rows * ff),
        name="mlp",
    )(token, normed, hextra, w_gate_up, w_down, hidden)


def place_kernel(size, where_ref, *refs):
    k_ref, v_ref = refs[-2:]
    for d in range(size):
        @pl.when(pl.program_id(0) == d)
        def _():
            k_ref[:, 0] = refs[d][0]
            v_ref[:, 0] = refs[d][1]


def place_caches(where, landed):
    rows, heads, head_dim = landed[0].shape[1:]
    size = len(landed)
    block = rows // 2
    blocks = rows // block

    def turn(number):
        return lambda d, n, where: (0, lax.select(d == number, n, lax.select(d < number, 0, blocks - 1)), 0, 0)

    out = pl.BlockSpec((block, 1, heads, head_dim), lambda d, n, where: (n, lax.rem(where[0] - d + size, size), 0, 0))
    return pl.pallas_call(
        functools.partial(place_kernel, size),
        out_shape=[jax.ShapeDtypeStruct((rows, size, heads, head_dim), jnp.bfloat16)] * 2,
        grid_spec=pltpu.PrefetchScalarGridSpec(
            num_scalar_prefetch=1,
            grid=(size, blocks),
            in_specs=[pl.BlockSpec((2, block, heads, head_dim), turn(d)) for d in range(size)],
            out_specs=[out, out],
        ),
        compiler_params=pltpu.CompilerParams(dimension_semantics=("arbitrary", "arbitrary"), vmem_limit_bytes=16 << 20),
        cost_estimate=pl.CostEstimate(flops=4000 * rows * size * heads * head_dim, bytes_accessed=8 * size * rows * heads * head_dim, transcendentals=0),
        name="place_caches",
    )(where, *landed)


def pick_by(index, options):
    result = options[0]
    for place in range(1, len(options)):
        result = jnp.where(index == place, options[place], result)
    return result


def solution(mesh):
    side_size = mesh.shape['side']
    tp_size = mesh.shape['tp']
    seats = mesh.shape['pair'] * side_size
    group_axes = ('pair', 'side')
    last = tp_size - 1

    def cyclic(value, d):
        return lax.ppermute(value, 'tp', [(t, (t + d) % tp_size) for t in range(tp_size)])

    def swap(value, mask):
        return lax.ppermute(value, group_axes, [(q, q ^ mask) for q in range(seats)])

    def in_order(me, copies):
        return [pick_by(me, [copies[(t - j) % tp_size] for t in range(tp_size)]) for j in range(tp_size)]

    def device_fn(x_prompt, s_len, y_tok, c_len, k_cache, v_cache, attn_gain, w_qkv, w_out, mlp_gain, w_gate_up, w_down):
        me = lax.axis_index('tp')
        seat = lax.axis_index('pair') * side_size + lax.axis_index('side')
        where = seat.reshape(1).astype(jnp.int32)
        seq_len, depth = x_prompt.shape[1:]
        heads_local = w_qkv.shape[2]
        head_dim = w_qkv.shape[4]
        width = heads_local * head_dim
        rows = seq_len // tp_size
        decodes = y_tok.shape[0]
        pad = 16
        cache_local = k_cache.shape[2]
        val = {}

        def tie(keys):
            keys = list(dict.fromkeys(keys))
            for key, value in zip(keys, lax.optimization_barrier(tuple(val[key] for key in keys))):
                val[key] = value

        val['w', 0] = lax.all_gather(lax.dynamic_index_in_dim(w_out[0, :, 0], seat, 0, keepdims=False), 'tp', axis=0, tiled=False)

        val['w_all'] = jnp.swapaxes(w_qkv[0], 1, 2).reshape(depth, 3 * width)
        extra_tables = rope_tables(jnp.concatenate([c_len, jnp.zeros((pad - decodes,), jnp.int32)]), head_dim)
        y_pad = jnp.concatenate([y_tok, jnp.zeros((pad - decodes, depth), y_tok.dtype)])
        val['gain'], val['s_len'], val['mlp_gain'] = attn_gain, s_len, mlp_gain
        val['valid'] = (jnp.arange(seq_len) < s_len[0]).astype(jnp.bfloat16)
        buffers = []
        qkv = []

        def compute(name):
            kind = name[0]
            c = int(name[1:]) if name[1:].isdigit() else 0
            if kind == 'Q':
                tie(thread + ['gain'])
                made = project_qkv(c, rows, val['token'], x_prompt[0], y_pad if c == 0 else None, val['gain'], val['w_all'], extra_tables, head_dim)
                val['token'] = made[3]
                qkv.append(made[:3])
                if c == 0:
                    val['dq', 0] = jnp.stack([part[:decodes].reshape(decodes, heads_local, head_dim) for part in made[4:]])
                    for d in range(1, tp_size):
                        val['dq', d] = cyclic(val['dq', 0], d)
                return ['token']
            if kind == 'T':
                tie(thread + ['s_len'])
                val['context', c], val['token'] = attend(c, tp_size, rows, val['token'], val['s_len'], *zip(*qkv), head_dim)
                return ['token']
            if kind == 'G':
                val['gathered', name[1:]] = lax.all_gather(jnp.stack([val['context', int(digit)] for digit in name[1:]]), 'tp', axis=0, tiled=False)
                return ['token']
            if kind == 'K':
                tie(thread + ['valid'])
                for d in range(tp_size):
                    made = []
                    keep = pick_by(me, [val['valid'][((t + d) % tp_size) * rows:((t + d) % tp_size + 1) * rows] for t in range(tp_size)])
                    for which in (1, 2):
                        rows_d = pick_by(me, [qkv[(t + d) % tp_size // 2][which][(t + d) % tp_size % 2 * rows:][:rows].reshape(rows, heads_local, head_dim) for t in range(tp_size)])
                        made.append(rows_d * keep[:, None, None])
                    val['kv', d] = jnp.stack(made)
                return []
            if name == 'D1':
                tie(thread + [('dq', d) for d in range(tp_size)])
                dec_full = jnp.concatenate(in_order(me, [val['dq', d] for d in range(tp_size)]), axis=2)
                cache_pos = me * cache_local + jnp.arange(cache_local)
                write_mask = (cache_pos[None, :] == c_len[:, None])[:, :, None, None]
                allowed = (cache_pos[None, :] <= c_len[:, None])[:, :, None]
                key_now = jnp.where(write_mask, dec_full[1][:, None], k_cache[0])
                value_now = jnp.where(write_mask, dec_full[2][:, None], v_cache[0])
                val['key_now'], val['value_now'] = key_now, value_now
                scores = jnp.sum(dec_full[0][:, None].astype(jnp.float32) * key_now.astype(jnp.float32), axis=-1)
                scores = scores * head_dim ** -0.5
                scores = jnp.where(allowed, scores, -1e30)
                peak = jnp.max(scores, axis=1, keepdims=True)
                weights = jnp.exp(scores - peak)
                total = jnp.sum(weights, axis=1)[..., None]
                peak = peak[:, 0, :, None]
                mixed = jnp.sum(weights.astype(jnp.bfloat16).astype(jnp.float32)[..., None] * value_now.astype(jnp.float32), axis=1)
                packed = jnp.stack([mixed, jnp.broadcast_to(peak, mixed.shape), jnp.broadcast_to(total, mixed.shape)])
                packed = packed.reshape(3, decodes, tp_size, heads_local, head_dim)
                for d in range(tp_size):
                    share = lax.dynamic_index_in_dim(packed, lax.rem(me + d, tp_size), 2, keepdims=False)
                    val['ds', d] = share if d == 0 else cyclic(share, d)
                return [('ds', 0)]
            if name == 'D2':
                tie(thread + [('ds', d) for d in range(tp_size)])
                shares = [val['ds', d] for d in range(tp_size)]
                top = functools.reduce(jnp.maximum, [share[1] for share in shares])
                factors = [jnp.exp(share[1] - top) for share in shares]
                dec_mixed = sum(share[0] * factor for share, factor in zip(shares, factors))
                dec_total = sum(share[2] * factor for share, factor in zip(shares, factors))
                val['dc', 0] = (dec_mixed / dec_total).astype(jnp.bfloat16).reshape(decodes, width)
                for d in range(1, tp_size):
                    val['dc', d] = cyclic(val['dc', 0], d)
                return [('dc', 0)]
            if kind == 'O':
                w_keys = [('w', r) for r in range(seats)]
                final = c == last
                parts = [('gathered', '3')] if final else [('gathered', '0'), ('gathered', '12')]
                extra_keys = [('dc', d) for d in range(tp_size)] if final else []
                tie(thread + ['mlp_gain'] + parts + extra_keys + ([] if final else w_keys))
                extras = []
                if final:
                    extras = [jnp.pad(jnp.stack(in_order(me, [val[key] for key in extra_keys])), ((0, 0), (0, pad - decodes), (0, 0))), y_pad]
                made = project_out(last if final else 0, 1 if final else last, tp_size, pad, val['token'], where, [val[key] for key in parts], [val[key] for key in w_keys], x_prompt[0], val['mlp_gain'], extras, [val[key] for key in buffers])
                buffers[:] = ['normed', 'h']
                val['normed'], val['h'], val['token'] = made[0], made[1], made[-1]
                if final:
                    val['hx'] = made[2]
                return ['token']
            if kind == 'P':
                tie(thread + [('landed', d) for d in range(tp_size)])
                val['k'], val['v'] = place_caches(me.reshape(1).astype(jnp.int32), [val['landed', d] for d in range(tp_size)])
                return ['k']
            val['out'], val['y'] = mlp(val['token'], val['normed'], val['hx'], jnp.transpose(w_gate_up[0], (1, 2, 0)), w_down[0], val['h'], tp_size)
            return ['y']

        def transfer(name):
            if name[0] == 'k':
                d = int(name[1])
                tie(thread + [('kv', d)] + ([('gathered', '3')] if d in (0, 2) else []))
                route = [(t * side_size + s, ((t + d) % tp_size) * side_size + (s + 1) % side_size) for t in range(tp_size) for s in range(side_size)]
                val['landed', d] = lax.ppermute(val['kv', d], ('tp', 'side'), route)
                return
            bases = [0] if name == 'w2' else list(range(0, seats, 2))
            kept = [] if name == 'w2' else [('kv', 0), ('kv', 2)]
            tie(thread + kept + [('w', base) for base in bases])
            for mask in (range(2, seats, 2) if name == 'w2' else [1]):
                for base in bases:
                    val['w', base ^ mask] = swap(val['w', base], mask)

        val['token'] = jnp.zeros(TOKEN.shape, TOKEN.dtype)
        thread = ['token']
        for name in ORDER:
            if name[0] in 'QTGKDOBP':
                made = compute(name)
                thread = thread + made if name in ('K', 'D1', 'D2') else made
            else:
                transfer(name)

        caches = [val[name].reshape(1, 1, rows, tp_size * heads_local, head_dim) for name in 'kv']
        return (val['out'][None], val['y'][:decodes], caches[0], caches[1], val['key_now'][None], val['value_now'][None])

    cache_spec = P(None, group_axes, 'tp', None, None)
    in_specs = (P(group_axes, None, None), P(group_axes), P(group_axes, None), P(group_axes), cache_spec, cache_spec, P(), P(None, None, 'tp', None, None), P(None, 'tp', None, None, None), P(), P(None, None, None, 'tp'), P(None, 'tp', None))
    out_specs = (P(group_axes, None, None), P(group_axes, None), cache_spec, cache_spec, cache_spec, cache_spec)
    return jax.shard_map(device_fn, mesh=mesh, in_specs=in_specs, out_specs=out_specs, check_vma=False)
```

```python
import functools

import jax
import jax.numpy as jnp
from jax import lax
from jax.experimental import pallas as pl
from jax.experimental.pallas import tpu as pltpu
from jax.sharding import PartitionSpec as P


ROPE_BASE = 10000.0
NORM_EPS = 1e-5

ORDER = (
    'Q0', 'T0', 'G0', 'T1', 'w2', 'Q1', 'T2', 'G12', 'T3', 'G3', 'K', 'k1', 'k3', 'k0', 'D1', 'D2', 'w3', 'O012', 'k2',
    'O3', 'B', 'P',
)


def rms_scale(values_f32, gain_f32):
    inv_rms = lax.rsqrt(jnp.mean(values_f32 * values_f32, axis=-1, keepdims=True) + NORM_EPS)
    return (values_f32 * inv_rms * gain_f32).astype(jnp.bfloat16)


def rope_frequencies(head_dim):
    half_dim = head_dim // 2
    inv_freq = ROPE_BASE ** (-2.0 * jnp.arange(half_dim, dtype=jnp.float32) / head_dim)
    return jnp.concatenate([inv_freq, inv_freq])[None]


def rope_tables(positions, head_dim):
    angles = positions.astype(jnp.float32)[:, None] * rope_frequencies(head_dim)
    sign = jnp.where(jnp.arange(head_dim) < head_dim // 2, -1.0, 1.0)
    return jnp.cos(angles), jnp.sin(angles) * sign[None]


def rope_rows(first, rows, freq):
    head_dim = freq.shape[1]
    positions = lax.broadcasted_iota(jnp.int32, (rows, head_dim), 0) + first
    angles = positions.astype(jnp.float32) * freq
    turns = jnp.floor(angles * 0.15915494309189535 + 0.5)
    angles = (angles - turns * 6.28125) - turns * 0.0019353071795864769
    sine = jnp.sin(angles)
    return jnp.cos(angles), jnp.where(lax.broadcasted_iota(jnp.int32, (rows, head_dim), 1) < head_dim // 2, -sine, sine)


def qkv_kernel(half, head_dim, extra, *refs):
    x_ref, gain_ref, wq_ref, wk_ref, wv_ref, freq_ref = refs[:6]
    extra_refs = refs[6:9] if extra else None
    normed_ref, cos_ref, sin_ref = refs[-3:]
    q_ref, k_ref, v_ref, token_ref = refs[-7 - 3 * extra:-3 - 3 * extra]
    extra_outs = refs[-6:-3] if extra else (None,) * 3
    rows = x_ref.shape[0]
    chunk = pl.program_id(1)

    @pl.when(pl.program_id(0) == 0)
    def _():
        gain = gain_ref[...].astype(jnp.float32)
        block = min(64, rows)

        @pl.loop(0, rows // block)
        def _(number):
            lines = pl.ds(pl.multiple_of(number * block, block), block)
            normed_ref[chunk, lines] = rms_scale(x_ref[lines].astype(jnp.float32), gain)
            cos_ref[chunk, lines], sin_ref[chunk, lines] = rope_rows((2 * half + chunk) * rows + number * block, block, freq_ref[...])

        if extra:
            normed_ref[chunk, rows:] = rms_scale(extra_refs[0][...].astype(jnp.float32), gain)
        token_ref[...] = jnp.zeros_like(token_ref)

    cos, sin = cos_ref[chunk], sin_ref[chunk]
    if extra:
        cos = jnp.concatenate([cos, extra_refs[1][...]], axis=0)
        sin = jnp.concatenate([sin, extra_refs[2][...]], axis=0)
    for w_ref, out_ref, extra_out in zip((wq_ref, wk_ref, wv_ref), (q_ref, k_ref, v_ref), extra_outs):
        acc = jnp.dot(normed_ref[chunk], w_ref[...], preferred_element_type=jnp.float32)
        for start in range(0, acc.shape[1], head_dim):
            vals = acc[:, start:start + head_dim]
            if out_ref is not v_ref:
                vals = vals * cos + pltpu.roll(vals, head_dim // 2, 1) * sin
            out_ref[:, start:start + head_dim] = vals[:rows].astype(out_ref.dtype)
            if extra:
                extra_out[:, start:start + head_dim] = vals[rows:].astype(out_ref.dtype)


TOKEN = jax.ShapeDtypeStruct((8, 128), jnp.float32)


def project_qkv(half, rows, token, x, extra_rows, gain, w_all, extra_tables, head_dim):
    depth = x.shape[1]
    width = w_all.shape[1] // 3
    block = 2 * head_dim
    steps = width // block
    extra = extra_rows is not None
    extras = [extra_rows, *extra_tables] if extra else []
    pad = extra_rows.shape[0] if extra else 0
    bf16 = jnp.bfloat16
    whole = lambda shape: pl.BlockSpec(shape, lambda n, c: (0, 0), pipeline_mode=pl.Buffered(1))
    columns = lambda part: pl.BlockSpec((depth, block), lambda n, c: (0, part * steps + n))
    extra_outs = [jax.ShapeDtypeStruct((pad, width), bf16)] * 3 if extra else []
    return pl.pallas_call(
        functools.partial(qkv_kernel, half, head_dim, extra),
        out_shape=[jax.ShapeDtypeStruct((2 * rows, width), bf16)] * 3 + [TOKEN] + extra_outs,
        grid=(steps, 2),
        in_specs=[
            pl.BlockSpec((rows, depth), lambda n, c: (2 * half + lax.select(n == 0, c, 1), 0)),
            whole((1, depth)),
            columns(0),
            columns(1),
            columns(2),
            whole((1, head_dim)),
        ] + [whole(e.shape) for e in extras] + [pl.BlockSpec(memory_space=pl.ANY)],
        out_specs=[pl.BlockSpec((rows, block), lambda n, c: (c, n))] * 3 + [whole(TOKEN.shape)] + [pl.BlockSpec((pad, block), lambda n, c: (0, n))] * len(extra_outs),
        scratch_shapes=[pltpu.VMEM((2, rows + pad, depth), bf16)] + [pltpu.VMEM((2, rows, head_dim), jnp.float32)] * 2,
        compiler_params=pltpu.CompilerParams(dimension_semantics=("arbitrary", "arbitrary"), vmem_limit_bytes=56 << 20),
        cost_estimate=pl.CostEstimate(flops=12 * rows * depth * width, bytes_accessed=2 * (2 * rows * depth + 3 * depth * width + 6 * rows * width), transcendentals=0),
        name="project_qkv",
    )(x, gain, w_all, w_all, w_all, rope_frequencies(head_dim), *extras, token)


def attend_kernel(chunk, first_checked, q_rows, slen_ref, *refs):
    q_ref = refs[0]
    k_refs = refs[1:chunk + 2]
    v_refs = refs[chunk + 2:2 * chunk + 3]
    out_ref, token_ref = refs[-2:]
    token_ref[...] = jnp.zeros_like(token_ref)
    rows, head_dim = q_ref.shape
    scale = head_dim ** -0.5
    limit = slen_ref[0]

    @pl.loop(0, rows // q_rows)
    def _(number):
        start = pl.multiple_of(number * q_rows, q_rows)
        query = q_ref[pl.ds(start, q_rows), :]
        scores = []
        for part in range(chunk + 1):
            score = lax.dot_general(query, k_refs[part][...], (((1,), (1,)), ((), ())), preferred_element_type=jnp.float32) * scale
            key_pos = lax.broadcasted_iota(jnp.int32, score.shape, 1)
            if part == chunk:
                allowed = key_pos <= lax.broadcasted_iota(jnp.int32, score.shape, 0) + start
                if part >= first_checked:
                    allowed = allowed & (key_pos < limit - part * rows)
                score = jnp.where(allowed, score, -1e30)
            elif part >= first_checked:
                score = jnp.where(key_pos < limit - part * rows, score, -1e30)
            scores.append(score)
        peak = functools.reduce(jnp.maximum, [jnp.max(score, axis=-1, keepdims=True) for score in scores])
        total = jnp.zeros((q_rows, 1), jnp.float32)
        mixed = jnp.zeros((q_rows, head_dim), jnp.float32)
        for score, v_ref in zip(scores, v_refs):
            weight = jnp.exp(score - peak)
            total = total + jnp.sum(weight, axis=-1, keepdims=True)
            mixed = mixed + jnp.dot(weight.astype(jnp.bfloat16), v_ref[...], preferred_element_type=jnp.float32)
        out_ref[pl.ds(start, q_rows), :] = (mixed / total).astype(out_ref.dtype)


def attend(chunk, chunks, rows, token, s_len, queries, keys, values, head_dim):
    width = queries[0].shape[1]
    heads = width // head_dim

    pick = lambda c: pl.BlockSpec((rows, head_dim), lambda h, slen: (c % 2, h))
    every = range(chunk + 1)
    total_keys = rows * (chunk + 1)
    return pl.pallas_call(
        functools.partial(attend_kernel, chunk, chunks // 2, min(256, rows)),
        out_shape=[jax.ShapeDtypeStruct((rows, width), jnp.bfloat16), TOKEN],
        grid_spec=pltpu.PrefetchScalarGridSpec(
            num_scalar_prefetch=1,
            grid=(heads,),
            in_specs=[pick(c) for c in (chunk, *every, *every)] + [pl.BlockSpec(memory_space=pl.ANY)],
            out_specs=[pick(0), pl.BlockSpec(TOKEN.shape, lambda h, slen: (0, 0))],
        ),
        compiler_params=pltpu.CompilerParams(dimension_semantics=("arbitrary",), vmem_limit_bytes=48 << 20),
        cost_estimate=pl.CostEstimate(flops=8 * heads * rows * total_keys * head_dim, bytes_accessed=2 * width * (2 * total_keys + 2 * rows), transcendentals=heads * rows * total_keys),
    )(s_len, queries[chunk // 2], *[keys[c // 2] for c in every], *[values[c // 2] for c in every], token)


def output_kernel(size, heads, contexts, extra, aliased, where_ref, *refs):
    context_refs, refs = refs[:contexts], refs[contexts:]
    w_refs, refs = refs[:heads], refs[heads:]
    x_ref, gain_ref, refs = refs[0], refs[1], refs[2:]
    if extra:
        context_x_ref, x_x_ref, refs = refs[0], refs[1], refs[2:]
    refs = refs[1:]
    if aliased:
        refs = refs[2:]
    normed_ref, hidden_ref, refs = refs[0], refs[1], refs[2:]
    if extra:
        hidden_x_ref, refs = refs[0], refs[1:]
    token_ref, full_ref, square_ref = refs
    rows, depth = hidden_ref.shape
    head_dim, block = w_refs[0].shape[1:]
    chunk, step = pl.program_id(0), pl.program_id(1)

    @pl.when(step == 0)
    def _():
        square_ref[...] = jnp.zeros_like(square_ref)
        token_ref[...] = jnp.zeros_like(token_ref)
        for number, context_ref in enumerate(context_refs):
            @pl.when((chunk == 0) if number == 0 else (chunk > 0))
            def _():
                @pl.loop(0, heads)
                def _(r):
                    columns = pl.ds(pl.multiple_of(lax.bitwise_xor(where_ref[0], r) * head_dim, head_dim), head_dim)
                    for t in range(size):
                        there = pl.ds(pl.multiple_of((r * size + t) * head_dim, head_dim), head_dim)
                        full_ref[:rows, there] = context_ref[t, 0, :, columns]
                        if extra:
                            full_ref[rows:, there] = context_x_ref[t, :, columns]

    w_block = jnp.concatenate([w_ref[...].reshape(size * head_dim, block) for w_ref in w_refs], axis=0)
    acc = jnp.dot(full_ref[...], w_block, preferred_element_type=jnp.float32)
    columns = pl.ds(pl.multiple_of(step * block, block), block)
    hidden = (x_ref[...].astype(jnp.float32) + acc[:rows]).astype(jnp.bfloat16)
    hidden_ref[:, columns] = hidden
    hidden_f32 = hidden.astype(jnp.float32)
    square_ref[:rows] += jnp.sum(hidden_f32 * hidden_f32, axis=-1, keepdims=True)
    if extra:
        hidden = (x_x_ref[...].astype(jnp.float32) + acc[rows:]).astype(jnp.bfloat16)
        hidden_x_ref[:, columns] = hidden
        hidden_f32 = hidden.astype(jnp.float32)
        square_ref[rows:] += jnp.sum(hidden_f32 * hidden_f32, axis=-1, keepdims=True)

    @pl.when(step == pl.num_programs(1) - 1)
    def _():
        half = rows // 2
        inv_rms = lax.rsqrt(square_ref[...] / depth + NORM_EPS)

        @pl.loop(0, depth // block)
        def _(number):
            columns = pl.ds(pl.multiple_of(number * block, block), block)
            gain = gain_ref[:, columns].astype(jnp.float32)
            for part in range(2):
                lo, hi = part * half, (part + 1) * half
                normed_ref[part, :half, columns] = (hidden_ref[lo:hi, columns].astype(jnp.float32) * inv_rms[lo:hi] * gain).astype(jnp.bfloat16)
                if extra and part == 1:
                    normed_ref[part, half:, columns] = (hidden_x_ref[:, columns].astype(jnp.float32) * inv_rms[rows:] * gain).astype(jnp.bfloat16)
                else:
                    normed_ref[part, half:, columns] = jnp.zeros((normed_ref.shape[1] - half, block), jnp.bfloat16)


def project_out(first, count, chunks, pad, token, where, contexts, w_heads, x, gain, extras, buffers):
    rows, width = contexts[0].shape[2:]
    depth = x.shape[1]
    heads = len(w_heads)
    size, head_dim = w_heads[0].shape[:2]
    block = min(512, depth)
    total = rows + (pad if extras else 0)
    whole = lambda shape: pl.BlockSpec(shape, lambda c, n, where: (0,) * len(shape), pipeline_mode=pl.Buffered(1))
    in_specs = [whole(contexts[0].shape)]
    if count > 1:
        in_specs.append(pl.BlockSpec((size, 1, rows, width), lambda c, n, where: (0, lax.max(c - 1, 0), 0, 0)))
    in_specs += [pl.BlockSpec((size, head_dim, block), lambda c, n, where: (0, 0, n))] * heads
    in_specs += [pl.BlockSpec((rows, block), lambda c, n, where: (first + c, n)), whole((1, depth))]
    out_shape = [jax.ShapeDtypeStruct((2 * chunks, rows // 2 + pad, depth), jnp.bfloat16), jax.ShapeDtypeStruct((rows * chunks, depth), jnp.bfloat16)]
    mode = {} if count > 1 else dict(pipeline_mode=pl.Buffered(1))
    out_specs = [
        pl.BlockSpec((2, rows // 2 + pad, depth), lambda c, n, where: (first + c, 0, 0), **mode),
        pl.BlockSpec((rows, depth), lambda c, n, where: (first + c, 0), **mode),
    ]
    if extras:
        in_specs += [whole(extras[0].shape), pl.BlockSpec((pad, block), lambda c, n, where: (0, n))]
        out_shape.append(jax.ShapeDtypeStruct((pad, depth), jnp.bfloat16))
        out_specs.append(whole((pad, depth)))
    in_specs.append(pl.BlockSpec(memory_space=pl.ANY))
    out_shape.append(TOKEN)
    out_specs.append(whole(TOKEN.shape))
    aliases = {}
    if buffers:
        aliases = {1 + len(in_specs): 0, 2 + len(in_specs): 1}
        in_specs += [pl.BlockSpec(memory_space=pl.ANY)] * 2
    return pl.pallas_call(
        functools.partial(output_kernel, size, heads, len(contexts), bool(extras), bool(buffers)),
        out_shape=out_shape,
        grid_spec=pltpu.PrefetchScalarGridSpec(
            num_scalar_prefetch=1,
            grid=(count, depth // block),
            in_specs=in_specs,
            out_specs=out_specs,
            scratch_shapes=[pltpu.VMEM((total, size * width), jnp.bfloat16), pltpu.VMEM((total, 1), jnp.float32)],
        ),
        input_output_aliases=aliases,
        compiler_params=pltpu.CompilerParams(dimension_semantics=("arbitrary", "arbitrary"), vmem_limit_bytes=60 << 20),
        cost_estimate=pl.CostEstimate(flops=2 * count * total * size * width * depth, bytes_accessed=2 * count * (size * width * depth + 4 * rows * width + 3 * total * depth), transcendentals=0),
        name="project_out",
    )(where, *contexts, *w_heads, x, gain, *extras, token, *buffers)


def mlp_kernel(size, chunk_rows, ff_steps, slots, token_ref, normed_ref, hextra_ref, wgu_ref, wd_ref, h_ref, out_ref, y_ref,
               acc, landed, outgoing, finished, residual, others, activated,
               rs_send, rs_recv, ag_send, ag_recv, keep_sem, h_sem, x_send, x_recv, credit):
    step = pl.program_id(0)
    me = lax.axis_index('tp')
    depth = wd_ref.shape[1]
    chunks = (out_ref.shape[0] // chunk_rows)
    piece = outgoing.shape[2]
    per_chunk = chunk_rows // (2 * piece)
    pieces = chunks * per_chunk
    subs = per_chunk // ff_steps
    last = size - 1

    @pl.when(step == 0)
    def _():
        barrier = pltpu.get_barrier_semaphore()
        for d in range(1, size):
            pl.semaphore_signal(barrier, inc=1, device_id={'tp': lax.rem(me + d, size)}, device_id_type=pl.DeviceIdType.MESH)
        pl.semaphore_wait(barrier, size - 1)

    def own_part(chain, m):
        start = pl.multiple_of(chain * (chunk_rows // 2) + lax.rem(m, per_chunk) * piece, piece)
        return acc.at[lax.rem(lax.div(m, per_chunk), 3), pl.ds(start, piece)]

    def out_rows(chain, m):
        start = pl.multiple_of(lax.div(m, per_chunk) * chunk_rows + chain * (chunk_rows // 2) + lax.rem(m, per_chunk) * piece, piece)
        return pl.ds(start, piece)

    def exchange(slot):
        for chain in range(2):
            place = me if chain == 0 else last - me
            nearer = me - 1 if chain == 0 else me + 1
            farther = me + 1 if chain == 0 else me - 1

            def sum_copy(source, m):
                return pltpu.make_async_remote_copy(
                    src_ref=source, dst_ref=landed.at[chain, lax.rem(m, slots)], send_sem=rs_send.at[chain, lax.rem(m, 4)],
                    recv_sem=rs_recv.at[chain, lax.rem(m, slots)], device_id={'tp': nearer}, device_id_type=pl.DeviceIdType.MESH)

            def keep_copy(m):
                return pltpu.make_async_copy(finished.at[chain, lax.rem(m, 2)], out_ref.at[out_rows(chain, m)], keep_sem.at[chain, lax.rem(m, 2)])

            def h_copy(m):
                return pltpu.make_async_copy(h_ref.at[out_rows(chain, m)], residual.at[chain, lax.rem(m, 2)], h_sem.at[chain, lax.rem(m, 2)])

            def back_copy(source, m):
                return pltpu.make_async_remote_copy(
                    src_ref=source, dst_ref=out_ref.at[out_rows(chain, m)], send_sem=ag_send.at[chain, lax.rem(m, 4)],
                    recv_sem=ag_recv.at[chain, lax.rem(m, 8)], device_id={'tp': farther}, device_id_type=pl.DeviceIdType.MESH)

            @pl.when((place == last) & (slot >= 0) & (slot < pieces))
            def _():
                @pl.when(slot >= 4)
                def _():
                    sum_copy(own_part(chain, slot - 4), slot - 4).wait_send()

                @pl.when(slot >= slots)
                def _():
                    pl.semaphore_wait(credit.at[chain], 1)

                sum_copy(own_part(chain, slot), slot).start()

            m = slot - (last - place)

            @pl.when((place > 0) & (place < last) & (m >= 0) & (m < pieces))
            def _():
                @pl.when(m >= 2)
                def _():
                    sum_copy(outgoing.at[chain, lax.rem(m, 2)], m - 2).wait_send()

                sum_copy(outgoing.at[chain, lax.rem(m, 2)], m).wait_recv()
                outgoing[chain, lax.rem(m, 2)] = landed[chain, lax.rem(m, slots)] + own_part(chain, m)[...]

                @pl.when(m + slots < pieces)
                def _():
                    pl.semaphore_signal(credit.at[chain], inc=1, device_id={'tp': farther}, device_id_type=pl.DeviceIdType.MESH)

                @pl.when(m >= slots)
                def _():
                    pl.semaphore_wait(credit.at[chain], 1)

                sum_copy(outgoing.at[chain, lax.rem(m, 2)], m).start()

            m = slot - last

            @pl.when((place == 0) & (slot == 0))
            def _():
                h_copy(0).start()

            @pl.when((place == 0) & (m >= 0) & (m < pieces))
            def _():
                @pl.when(m + 1 < pieces)
                def _():
                    h_copy(m + 1).start()

                @pl.when(m >= 2)
                def _():
                    keep_copy(m - 2).wait()
                    back_copy(finished.at[chain, lax.rem(m, 2)], m - 2).wait_send()

                h_copy(m).wait()
                sum_copy(outgoing.at[chain, lax.rem(m, 2)], m).wait_recv()
                total = landed[chain, lax.rem(m, slots)] + own_part(chain, m)[...]
                finished[chain, lax.rem(m, 2)] = (residual[chain, lax.rem(m, 2)].astype(jnp.float32) + total).astype(jnp.bfloat16)

                @pl.when(m + slots < pieces)
                def _():
                    pl.semaphore_signal(credit.at[chain], inc=1, device_id={'tp': farther}, device_id_type=pl.DeviceIdType.MESH)

                keep_copy(m).start()
                back_copy(finished.at[chain, lax.rem(m, 2)], m).start()

        for chain in range(2):
            place = me if chain == 0 else last - me
            farther = me + 1 if chain == 0 else me - 1

            def relay_copy(m):
                return pltpu.make_async_remote_copy(
                    src_ref=out_ref.at[out_rows(chain, m)], dst_ref=out_ref.at[out_rows(chain, m)], send_sem=ag_send.at[chain, lax.rem(m, 4)],
                    recv_sem=ag_recv.at[chain, lax.rem(m, 8)], device_id={'tp': farther}, device_id_type=pl.DeviceIdType.MESH)

            m = slot - last - 2 * place

            @pl.when((place > 0) & (m >= 0) & (m < pieces))
            def _():
                relay_copy(m).wait_recv()

                @pl.when((place < last) & (m >= 4))
                def _():
                    relay_copy(m - 4).wait_send()

                @pl.when(place < last)
                def _():
                    relay_copy(m).start()

    def extra_copy(d):
        return pltpu.make_async_remote_copy(
            src_ref=acc.at[(chunks - 1) % 3, pl.ds(chunk_rows, others.shape[1])], dst_ref=others.at[d], send_sem=x_send.at[d - 1],
            recv_sem=x_recv.at[d - 1], device_id={'tp': lax.rem(me + d, size)}, device_id_type=pl.DeviceIdType.MESH)

    @pl.when(step == chunks * ff_steps)
    def _():
        others[0] = acc[(chunks - 1) % 3, chunk_rows:chunk_rows + others.shape[1]]
        for d in range(1, size):
            extra_copy(d).start()

    @pl.when(step == chunks * ff_steps + 4)
    def _():
        for d in range(1, size):
            extra_copy(d).wait()
        total = others[lax.rem(me, size)]
        for j in range(1, size):
            total = total + others[lax.rem(me + size - j, size)]
        y_ref[...] = (hextra_ref[:others.shape[1]].astype(jnp.float32) + total).astype(jnp.bfloat16)

    chunk = lax.div(step, ff_steps)
    block = min(1024, depth)

    def compute_gate():
        rows_in = normed_ref[0]
        dims = (((1,), (1,)), ((), ()))
        gate = lax.dot_general(rows_in, wgu_ref[0], dims, preferred_element_type=jnp.float32)
        up = lax.dot_general(rows_in, wgu_ref[1], dims, preferred_element_type=jnp.float32)
        activated[...] = (gate * jax.nn.sigmoid(gate) * up).astype(jnp.bfloat16)

    def compute_down():
        first = lax.rem(step, ff_steps) == 0
        for start in range(0, depth, block):
            part = jnp.dot(activated[...], wd_ref[:, start:start + block], preferred_element_type=jnp.float32)

            @pl.when(first)
            def _():
                acc[lax.rem(chunk, 3), :, start:start + block] = part

            @pl.when(jnp.logical_not(first))
            def _():
                acc[lax.rem(chunk, 3), :, start:start + block] += part

    @pl.loop(0, subs)
    def _(sub):
        exchange((step - ff_steps) * subs + sub)
        for part in range(2):
            pl.when((step < chunks * ff_steps) & (sub == part * subs // 2))((compute_gate, compute_down)[part])

    @pl.when(step == pl.num_programs(0) - 1)
    def _():
        for chain in range(2):
            place = me if chain == 0 else last - me
            nearer = me - 1 if chain == 0 else me + 1
            farther = me + 1 if chain == 0 else me - 1

            def sent(m):
                return pltpu.make_async_remote_copy(
                    src_ref=outgoing.at[chain, m % 2], dst_ref=landed.at[chain, m % slots], send_sem=rs_send.at[chain, m % 4],
                    recv_sem=rs_recv.at[chain, m % slots], device_id={'tp': nearer}, device_id_type=pl.DeviceIdType.MESH)

            def returned(m):
                return pltpu.make_async_remote_copy(
                    src_ref=finished.at[chain, m % 2], dst_ref=out_ref.at[pl.ds(0, piece)], send_sem=ag_send.at[chain, m % 4],
                    recv_sem=ag_recv.at[chain, m % 8], device_id={'tp': farther}, device_id_type=pl.DeviceIdType.MESH)

            @pl.when(place == last)
            def _():
                for m in range(pieces - 4, pieces):
                    sent(m).wait_send()

            @pl.when((place > 0) & (place < last))
            def _():
                for m in range(pieces - 2, pieces):
                    sent(m).wait_send()
                for m in range(pieces - 4, pieces):
                    returned(m).wait_send()

            @pl.when(place == 0)
            def _():
                for m in range(pieces - 2, pieces):
                    pltpu.make_async_copy(finished.at[chain, m % 2], out_ref.at[pl.ds(0, piece)], keep_sem.at[chain, m % 2]).wait()
                    returned(m).wait_send()


SUBSLOTS = 2


def mlp(token, normed, hextra, w_gate_up, w_down, hidden, size):
    chunks, lines, depth = normed.shape
    rows = hidden.shape[0]
    chunk_rows = rows // chunks
    ff = w_down.shape[0]
    ff_steps = 4
    piece = chunk_rows // (8 * SUBSLOTS)
    slots = 4
    pieces = chunks * 4 * SUBSLOTS
    extra = lines - chunk_rows
    seen = min(8, extra)
    steps = chunks * ff_steps
    total_steps = ff_steps + -(-(pieces + 3 * (size - 1)) // SUBSLOTS)
    ff_block = ff // ff_steps
    at_ff = lambda g: lax.select(g < steps, lax.rem(g, ff_steps), ff_steps - 1)
    at_chunk = lambda g: lax.min(lax.div(g, ff_steps), chunks - 1)
    f32, bf16 = jnp.float32, jnp.bfloat16
    return pl.pallas_call(
        functools.partial(mlp_kernel, size, chunk_rows, ff_steps, slots),
        out_shape=[jax.ShapeDtypeStruct((rows, depth), bf16), jax.ShapeDtypeStruct((seen, depth), bf16)],
        grid=(total_steps,),
        in_specs=[
            pl.BlockSpec(memory_space=pl.ANY),
            pl.BlockSpec((1, lines, depth), lambda g: (at_chunk(g), 0, 0)),
            pl.BlockSpec((extra, depth), lambda g: (0, 0), pipeline_mode=pl.Buffered(1)),
            pl.BlockSpec((2, ff_block, depth), lambda g: (0, at_ff(g), 0)),
            pl.BlockSpec((ff_block, depth), lambda g: (at_ff(g), 0)),
            pl.BlockSpec(memory_space=pl.ANY),
        ],
        out_specs=[pl.BlockSpec(memory_space=pl.ANY), pl.BlockSpec((seen, depth), lambda g: (0, 0), pipeline_mode=pl.Buffered(1))],
        scratch_shapes=[
            pltpu.VMEM((3, lines, depth), f32),
            pltpu.VMEM((2, slots, piece, depth), f32),
            pltpu.VMEM((2, 2, piece, depth), f32),
            pltpu.VMEM((2, 2, piece, depth), bf16),
            pltpu.VMEM((2, 2, piece, depth), bf16),
            pltpu.VMEM((size, seen, depth), f32),
            pltpu.VMEM((lines, ff_block), bf16),
            pltpu.SemaphoreType.DMA((2, 4)),
            pltpu.SemaphoreType.DMA((2, slots)),
            pltpu.SemaphoreType.DMA((2, 4)),
            pltpu.SemaphoreType.DMA((2, 8)),
            pltpu.SemaphoreType.DMA((2, 2)),
            pltpu.SemaphoreType.DMA((2, 2)),
            pltpu.SemaphoreType.DMA((size - 1,)),
            pltpu.SemaphoreType.DMA((size - 1,)),
            pltpu.SemaphoreType.REGULAR((2,)),
        ],
        compiler_params=pltpu.CompilerParams(dimension_semantics=("arbitrary",), vmem_limit_bytes=63 << 20, collective_id=0, has_side_effects=True),
        cost_estimate=pl.CostEstimate(flops=6 * rows * depth * ff, bytes_accessed=6 * chunks * depth * ff, transcendentals=rows * ff),
        name="mlp",
    )(token, normed, hextra, w_gate_up, w_down, hidden)


def place_kernel(size, where_ref, *refs):
    k_ref, v_ref = refs[-2:]
    for d in range(size):
        @pl.when(pl.program_id(0) == d)
        def _():
            k_ref[:, 0] = refs[d][0]
            v_ref[:, 0] = refs[d][1]


def place_caches(where, landed):
    rows, heads, head_dim = landed[0].shape[1:]
    size = len(landed)
    block = rows // 2
    blocks = rows // block

    def turn(number):
        return lambda d, n, where: (0, lax.select(d == number, n, lax.select(d < number, 0, blocks - 1)), 0, 0)

    out = pl.BlockSpec((block, 1, heads, head_dim), lambda d, n, where: (n, lax.rem(where[0] - d + size, size), 0, 0))
    return pl.pallas_call(
        functools.partial(place_kernel, size),
        out_shape=[jax.ShapeDtypeStruct((rows, size, heads, head_dim), jnp.bfloat16)] * 2,
        grid_spec=pltpu.PrefetchScalarGridSpec(
            num_scalar_prefetch=1,
            grid=(size, blocks),
            in_specs=[pl.BlockSpec((2, block, heads, head_dim), turn(d)) for d in range(size)],
            out_specs=[out, out],
        ),
        compiler_params=pltpu.CompilerParams(dimension_semantics=("arbitrary", "arbitrary"), vmem_limit_bytes=16 << 20),
        cost_estimate=pl.CostEstimate(flops=4000 * rows * size * heads * head_dim, bytes_accessed=8 * size * rows * heads * head_dim, transcendentals=0),
        name="place_caches",
    )(where, *landed)


def pick_by(index, options):
    result = options[0]
    for place in range(1, len(options)):
        result = jnp.where(index == place, options[place], result)
    return result


def solution(mesh):
    side_size = mesh.shape['side']
    tp_size = mesh.shape['tp']
    seats = mesh.shape['pair'] * side_size
    group_axes = ('pair', 'side')
    last = tp_size - 1

    def cyclic(value, d):
        return lax.ppermute(value, 'tp', [(t, (t + d) % tp_size) for t in range(tp_size)])

    def swap(value, mask):
        return lax.ppermute(value, group_axes, [(q, q ^ mask) for q in range(seats)])

    def in_order(me, copies):
        return [pick_by(me, [copies[(t - j) % tp_size] for t in range(tp_size)]) for j in range(tp_size)]

    def device_fn(x_prompt, s_len, y_tok, c_len, k_cache, v_cache, attn_gain, w_qkv, w_out, mlp_gain, w_gate_up, w_down):
        me = lax.axis_index('tp')
        seat = lax.axis_index('pair') * side_size + lax.axis_index('side')
        where = seat.reshape(1).astype(jnp.int32)
        seq_len, depth = x_prompt.shape[1:]
        heads_local = w_qkv.shape[2]
        head_dim = w_qkv.shape[4]
        width = heads_local * head_dim
        rows = seq_len // tp_size
        decodes = y_tok.shape[0]
        pad = 16
        cache_local = k_cache.shape[2]
        val = {}

        def tie(keys):
            keys = list(dict.fromkeys(keys))
            for key, value in zip(keys, lax.optimization_barrier(tuple(val[key] for key in keys))):
                val[key] = value

        val['w', 0] = lax.all_gather(lax.dynamic_index_in_dim(w_out[0, :, 0], seat, 0, keepdims=False), 'tp', axis=0, tiled=False)

        val['w_all'] = jnp.swapaxes(w_qkv[0], 1, 2).reshape(depth, 3 * width)
        extra_tables = rope_tables(jnp.concatenate([c_len, jnp.zeros((pad - decodes,), jnp.int32)]), head_dim)
        y_pad = jnp.concatenate([y_tok, jnp.zeros((pad - decodes, depth), y_tok.dtype)])
        val['gain'], val['s_len'], val['mlp_gain'] = attn_gain, s_len, mlp_gain
        val['valid'] = (jnp.arange(seq_len) < s_len[0]).astype(jnp.bfloat16)
        buffers = []
        qkv = []

        def compute(name):
            kind = name[0]
            c = int(name[1:]) if name[1:].isdigit() else 0
            if kind == 'Q':
                tie(thread + ['gain'])
                made = project_qkv(c, rows, val['token'], x_prompt[0], y_pad if c == 0 else None, val['gain'], val['w_all'], extra_tables, head_dim)
                val['token'] = made[3]
                qkv.append(made[:3])
                if c == 0:
                    val['dq', 0] = jnp.stack([part[:decodes].reshape(decodes, heads_local, head_dim) for part in made[4:]])
                    for d in range(1, tp_size):
                        val['dq', d] = cyclic(val['dq', 0], d)
                return ['token']
            if kind == 'T':
                tie(thread + ['s_len'])
                val['context', c], val['token'] = attend(c, tp_size, rows, val['token'], val['s_len'], *zip(*qkv), head_dim)
                return ['token']
            if kind == 'G':
                val['gathered', name[1:]] = lax.all_gather(jnp.stack([val['context', int(digit)] for digit in name[1:]]), 'tp', axis=0, tiled=False)
                return ['token']
            if kind == 'K':
                tie(thread + ['valid'])
                for d in range(tp_size):
                    made = []
                    keep = pick_by(me, [val['valid'][((t + d) % tp_size) * rows:((t + d) % tp_size + 1) * rows] for t in range(tp_size)])
                    for which in (1, 2):
                        rows_d = pick_by(me, [qkv[(t + d) % tp_size // 2][which][(t + d) % tp_size % 2 * rows:][:rows].reshape(rows, heads_local, head_dim) for t in range(tp_size)])
                        made.append(rows_d * keep[:, None, None])
                    val['kv', d] = jnp.stack(made)
                return []
            if name == 'D1':
                tie(thread + [('dq', d) for d in range(tp_size)])
                dec_full = jnp.concatenate(in_order(me, [val['dq', d] for d in range(tp_size)]), axis=2)
                cache_pos = me * cache_local + jnp.arange(cache_local)
                write_mask = (cache_pos[None, :] == c_len[:, None])[:, :, None, None]
                allowed = (cache_pos[None, :] <= c_len[:, None])[:, :, None]
                key_now = jnp.where(write_mask, dec_full[1][:, None], k_cache[0])
                value_now = jnp.where(write_mask, dec_full[2][:, None], v_cache[0])
                val['key_now'], val['value_now'] = key_now, value_now
                scores = jnp.sum(dec_full[0][:, None].astype(jnp.float32) * key_now.astype(jnp.float32), axis=-1) * head_dim ** -0.5
                scores = jnp.where(allowed, scores, -1e30)
                peak = jnp.max(scores, axis=1, keepdims=True)
                weights = jnp.exp(scores - peak)
                total = jnp.sum(weights, axis=1)[..., None]
                peak = peak[:, 0, :, None]
                mixed = jnp.sum(weights.astype(jnp.bfloat16).astype(jnp.float32)[..., None] * value_now.astype(jnp.float32), axis=1)
                packed = jnp.stack([mixed, jnp.broadcast_to(peak, mixed.shape), jnp.broadcast_to(total, mixed.shape)])
                packed = packed.reshape(3, decodes, tp_size, heads_local, head_dim)
                for d in range(tp_size):
                    share = lax.dynamic_index_in_dim(packed, lax.rem(me + d, tp_size), 2, keepdims=False)
                    val['ds', d] = share if d == 0 else cyclic(share, d)
                return [('ds', 0)]
            if name == 'D2':
                tie(thread + [('ds', d) for d in range(tp_size)])
                shares = [val['ds', d] for d in range(tp_size)]
                top = functools.reduce(jnp.maximum, [share[1] for share in shares])
                factors = [jnp.exp(share[1] - top) for share in shares]
                dec_mixed = sum(share[0] * factor for share, factor in zip(shares, factors))
                dec_total = sum(share[2] * factor for share, factor in zip(shares, factors))
                val['dc', 0] = (dec_mixed / dec_total).astype(jnp.bfloat16).reshape(decodes, width)
                for d in range(1, tp_size):
                    val['dc', d] = cyclic(val['dc', 0], d)
                return [('dc', 0)]
            if kind == 'O':
                w_keys = [('w', r) for r in range(seats)]
                final = c == last
                parts = [('gathered', '3')] if final else [('gathered', '0'), ('gathered', '12')]
                extra_keys = [('dc', d) for d in range(tp_size)] if final else []
                tie(thread + ['mlp_gain'] + parts + extra_keys + ([] if final else w_keys))
                extras = []
                if final:
                    extras = [jnp.pad(jnp.stack(in_order(me, [val[key] for key in extra_keys])), ((0, 0), (0, pad - decodes), (0, 0))), y_pad]
                made = project_out(last if final else 0, 1 if final else last, tp_size, pad, val['token'], where, [val[key] for key in parts], [val[key] for key in w_keys], x_prompt[0], val['mlp_gain'], extras, [val[key] for key in buffers])
                buffers[:] = ['normed', 'h']
                val['normed'], val['h'], val['token'] = made[0], made[1], made[-1]
                if final:
                    val['hx'] = made[2]
                return ['token']
            if kind == 'P':
                tie(thread + [('landed', d) for d in range(tp_size)])
                val['k'], val['v'] = place_caches(me.reshape(1).astype(jnp.int32), [val['landed', d] for d in range(tp_size)])
                return ['k']
            val['out'], val['y'] = mlp(val['token'], val['normed'], val['hx'], jnp.transpose(w_gate_up[0], (1, 2, 0)), w_down[0], val['h'], tp_size)
            return ['y']

        def transfer(name):
            if name[0] == 'k':
                d = int(name[1])
                tie(thread + [('kv', d)] + ([('gathered', '3')] if d == 2 else []))
                route = [(t * side_size + s, ((t + d) % tp_size) * side_size + (s + 1) % side_size) for t in range(tp_size) for s in range(side_size)]
                val['landed', d] = lax.ppermute(val['kv', d], ('tp', 'side'), route)
                return
            bases = [0] if name == 'w2' else list(range(0, seats, 2))
            kept = [] if name == 'w2' else [('kv', 2)]
            tie(thread + kept + [('w', base) for base in bases])
            for mask in (range(2, seats, 2) if name == 'w2' else [1]):
                for base in bases:
                    val['w', base ^ mask] = swap(val['w', base], mask)

        val['token'] = jnp.zeros(TOKEN.shape, TOKEN.dtype)
        thread = ['token']
        for name in ORDER:
            if name[0] in 'QTGKDOBP':
                made = compute(name)
                thread = thread + made if name in ('K', 'D1', 'D2') else made
            else:
                transfer(name)

        caches = [val[name].reshape(1, 1, rows, tp_size * heads_local, head_dim) for name in 'kv']
        return (val['out'][None], val['y'][:decodes], caches[0], caches[1], val['key_now'][None], val['value_now'][None])

    cache_spec = P(None, group_axes, 'tp', None, None)
    in_specs = (P(group_axes, None, None), P(group_axes), P(group_axes, None), P(group_axes), cache_spec, cache_spec, P(), P(None, None, 'tp', None, None), P(None, 'tp', None, None, None), P(), P(None, None, None, 'tp'), P(None, 'tp', None))
    out_specs = (P(group_axes, None, None), P(group_axes, None), cache_spec, cache_spec, cache_spec, cache_spec)
    return jax.shard_map(device_fn, mesh=mesh, in_specs=in_specs, out_specs=out_specs, check_vma=False)
```
